64 devices in a mesh: data: 4 (over x, y), tensor: 16 (over z, core).
Axes of the slice: x: 2, y: 2, z: 8, core: 2. Of those that a mesh axis runs over, the one named last changes fastest.
The devices are a block of a 4x4x8 slice.
Arguments:
- token_ids: int32 [32768], P(('data', 'tensor')), parts along dimension 0
- emb_table: bfloat16 [49152, 960], P('tensor')
- norm_gain: bfloat16 [960], replicated
- w_up: bfloat16 [960, 2560], P(None, 'tensor')
- w_down: bfloat16 [2560, 960], P('tensor')
- grad_out: bfloat16 [32768, 960], P(('data', 'tensor')), parts along dimension 0
Outputs:
- output 1: bfloat16 [32768, 960], P(('data', 'tensor')), parts along dimension 0
- output 2: float32 [196608, 960], P(('data', 'tensor')), parts along dimension 0
- output 3: float32 [3840, 2560], P('data', 'tensor'), parts along dimension 0
- output 4: float32 [10240, 960], P(('data', 'tensor')), parts along dimension 0
There are 4 independent parts. The reference program is written for one: setup_inputs(seed, part) draws one part's arguments, and reference() takes and returns one part's arrays. A program takes and returns all parts, laid end to end along the dimension named above; an argument that names none is the same for every part.
All inputs are finite; a program needn't handle non-finite values.
Results may differ from the reference program's by a relative error of at most 0.00554385.
Values are sent between devices in bfloat16 or wider.
A program may use at most 768 MiB of HBM per device.

```python
import math
import jax
import jax.numpy as jnp
from jax import lax

VOCAB_SIZE = 49152
MODEL_DIM = 960
FFN_DIM = 2560
TOKENS = 8192
HOT_IDS = 64
EPS = 1e-6
ROW_BLOCK = math.gcd(TOKENS, 2048)
NUM_BLOCKS = TOKENS // ROW_BLOCK


def draw_ids(key):
    key_uni, key_table, key_pick, key_coin = jax.random.split(key, 4)
    uniform_ids = jax.random.randint(key_uni, (TOKENS,), 0, VOCAB_SIZE)
    hot_table = jax.random.randint(key_table, (HOT_IDS,), 0, VOCAB_SIZE)
    hot_ids = hot_table[jax.random.randint(key_pick, (TOKENS,), 0, HOT_IDS)]
    coin_flip = jax.random.randint(key_coin, (TOKENS,), 0, 2)
    token_ids = jnp.where(coin_flip == 0, uniform_ids, hot_ids)
    token_ids = token_ids.at[0].set(0).at[TOKENS - 1].set(VOCAB_SIZE - 1)
    return token_ids.astype(jnp.int32)


def setup_inputs(seed: int = 0, part: int = 0) -> dict:
    shared_key, part_root = jax.random.split(jax.random.key(seed))
    key_emb, key_gain, key_up, key_down = jax.random.split(shared_key, 4)
    key_ids, key_grad = jax.random.split(jax.random.fold_in(part_root, part))
    emb_table = jax.random.normal(key_emb, (VOCAB_SIZE, MODEL_DIM), jnp.float32)
    norm_gain = 1.0 + 0.4 * jax.random.normal(key_gain, (MODEL_DIM,), jnp.float32)
    w_up = jax.random.normal(key_up, (MODEL_DIM, FFN_DIM), jnp.float32) * MODEL_DIM ** -0.5
    w_down = jax.random.normal(key_down, (FFN_DIM, MODEL_DIM), jnp.float32) * FFN_DIM ** -0.5
    grad_out = jax.random.normal(key_grad, (TOKENS, MODEL_DIM), jnp.float32)
    return {
        'token_ids': draw_ids(key_ids),
        'emb_table': emb_table.astype(jnp.bfloat16),
        'norm_gain': norm_gain.astype(jnp.bfloat16),
        'w_up': w_up.astype(jnp.bfloat16),
        'w_down': w_down.astype(jnp.bfloat16),
        'grad_out': grad_out.astype(jnp.bfloat16),
    }


def rms_norm(x_rows, gain_f):
    inv_rms = lax.rsqrt(jnp.mean(x_rows * x_rows, axis=-1, keepdims=True) + EPS)
    return x_rows * inv_rms * gain_f


def gelu_tanh(values):
    return jax.nn.gelu(values, approximate=True)


def reference(token_ids, emb_table, norm_gain, w_up, w_down, grad_out):
    gain_f = norm_gain.astype(jnp.float32)
    x_rows = jnp.take(emb_table, token_ids, axis=0)
    x_blocks = x_rows.reshape(NUM_BLOCKS, ROW_BLOCK, MODEL_DIM)
    grad_blocks = grad_out.reshape(NUM_BLOCKS, ROW_BLOCK, MODEL_DIM)

    def block_step(acc_pair, block_in):
        acc_up, acc_down = acc_pair
        x_blk = block_in[0].astype(jnp.float32)
        grad_blk = block_in[1]
        normed_f, norm_back = jax.vjp(lambda x_in: rms_norm(x_in, gain_f), x_blk)
        normed = normed_f.astype(jnp.bfloat16)
        pre_act = jnp.dot(normed, w_up, preferred_element_type=jnp.float32).astype(jnp.bfloat16)
        act_f, gelu_back = jax.vjp(gelu_tanh, pre_act.astype(jnp.float32))
        hidden = act_f.astype(jnp.bfloat16)
        y_blk = jnp.dot(hidden, w_down, preferred_element_type=jnp.float32)
        out_blk = (x_blk + y_blk).astype(jnp.bfloat16)
        d_hidden = jnp.dot(grad_blk, w_down.T, preferred_element_type=jnp.float32)
        d_pre = gelu_back(d_hidden)[0].astype(jnp.bfloat16)
        acc_down = acc_down + jnp.dot(hidden.T, grad_blk, preferred_element_type=jnp.float32)
        acc_up = acc_up + jnp.dot(normed.T, d_pre, preferred_element_type=jnp.float32)
        d_norm = jnp.dot(d_pre, w_up.T, preferred_element_type=jnp.float32)
        dx_blk = (grad_blk.astype(jnp.float32) + norm_back(d_norm)[0]).astype(jnp.bfloat16)
        return (acc_up, acc_down), (out_blk, dx_blk)

    zero_acc = (jnp.zeros((MODEL_DIM, FFN_DIM), jnp.float32), jnp.zeros((FFN_DIM, MODEL_DIM), jnp.float32))
    grads, outs = lax.scan(block_step, zero_acc, (x_blocks, grad_blocks))
    out = outs[0].reshape(TOKENS, MODEL_DIM)
    d_x = outs[1].reshape(TOKENS, MODEL_DIM).astype(jnp.float32)
    d_emb = jax.ops.segment_sum(d_x, token_ids, num_segments=VOCAB_SIZE)
    return (out, d_emb, grads[0], grads[1])
```

```python
import jax
import jax.numpy as jnp
from jax import lax
from jax.sharding import PartitionSpec as P

EPS = 1e-6


def rms_norm(x_rows, gain_f):
    inv_rms = lax.rsqrt(jnp.mean(x_rows * x_rows, axis=-1, keepdims=True) + EPS)
    return x_rows * inv_rms * gain_f


def gelu_tanh(values):
    return jax.nn.gelu(values, approximate=True)


def contract_last(left_op, right_op):
    return lax.dot_general(left_op, right_op, (((1,), (1,)), ((), ())), preferred_element_type=jnp.float32)


def contract_first(left_op, right_op):
    return lax.dot_general(left_op, right_op, (((0,), (0,)), ((), ())), preferred_element_type=jnp.float32)


def solution(mesh):
    tok_spec = P(('data', 'tensor'))
    row_spec = P(('data', 'tensor'), None)

    def local_step(token_ids, emb_shard, norm_gain, w_up, w_down, grad_out):
        vocab_local = emb_shard.shape[0]
        offset = lax.axis_index('tensor') * vocab_local
        ids_all = lax.all_gather(token_ids, 'tensor', tiled=True)
        up_all = lax.all_gather(w_up.T, 'tensor', tiled=True)
        down_all = lax.all_gather(w_down, 'tensor', tiled=True)
        rel_ids = ids_all - offset
        vocab_row = lax.broadcasted_iota(jnp.int32, (ids_all.shape[0], vocab_local), 1)
        pick = (vocab_row == rel_ids[:, None]).astype(jnp.bfloat16)
        emb_part = jnp.dot(pick, emb_shard, preferred_element_type=jnp.float32).astype(jnp.bfloat16)
        x_local = lax.psum_scatter(emb_part, 'tensor', scatter_dimension=0, tiled=True)
        x_f = x_local.astype(jnp.float32)
        gain_f = norm_gain.astype(jnp.float32)
        normed_f, norm_back = jax.vjp(lambda x_in: rms_norm(x_in, gain_f), x_f)
        normed = normed_f.astype(jnp.bfloat16)
        pre_act = contract_last(normed, up_all).astype(jnp.bfloat16)
        act_f, gelu_back = jax.vjp(gelu_tanh, pre_act.astype(jnp.float32))
        hidden = act_f.astype(jnp.bfloat16)
        d_hidden = contract_last(grad_out, down_all)
        d_pre = gelu_back(d_hidden)[0].astype(jnp.bfloat16)
        d_norm = jnp.dot(d_pre, up_all, preferred_element_type=jnp.float32)
        dx_local = (grad_out.astype(jnp.float32) + norm_back(d_norm)[0]).astype(jnp.bfloat16)
        dx_all = lax.all_gather(dx_local, 'tensor', tiled=True)
        y_local = jnp.dot(hidden, down_all, preferred_element_type=jnp.float32)
        out_local = (x_f + y_local).astype(jnp.bfloat16)
        d_w_down = lax.psum_scatter(contract_first(hidden, grad_out), 'tensor', scatter_dimension=0, tiled=True)
        d_w_up = lax.psum_scatter(contract_first(d_pre, normed), 'tensor', scatter_dimension=0, tiled=True).T
        vocab_col = lax.broadcasted_iota(jnp.int32, (vocab_local, ids_all.shape[0]), 0)
        place = (vocab_col == rel_ids[None, :]).astype(jnp.bfloat16)
        d_emb = jnp.dot(place, dx_all, preferred_element_type=jnp.float32)
        return out_local, d_emb, d_w_up, d_w_down

    return jax.shard_map(
        local_step,
        mesh=mesh,
        in_specs=(tok_spec, P('tensor', None), P(None), P(None, 'tensor'), P('tensor', None), row_spec),
        out_specs=(row_spec, row_spec, P('data', 'tensor'), row_spec),
        check_vma=False,
    )
```

```python
import functools

import jax
import jax.numpy as jnp
from jax import lax
from jax.experimental import pallas as pl
from jax.experimental.pallas import tpu as pltpu
from jax.sharding import PartitionSpec as P

EPS = 1e-6
CAP = 64
LANES = 128
FCHUNK = 256
ROWS = 128
MESH = pl.DeviceIdType.MESH
VMEM_LIMIT = 66_000_000
F32 = jnp.float32
BF16 = jnp.bfloat16
SQRT_2_PI = 0.7978845608028654
CUBIC = 0.044715


def contract(left_op, right_op, left_dim, right_dim):
    dims = (((left_dim,), (right_dim,)), ((), ()))
    return lax.dot_general(left_op, right_op, dims, preferred_element_type=F32)


def iota(shape, dim):
    return lax.broadcasted_iota(jnp.int32, shape, dim)


class Ring:
    def __init__(self, n):
        self.n, self.nz, self.half = n, n // 2, n // 4
        self.me = lax.axis_index('tensor')
        self.c = lax.rem(self.me, 2)
        self.z = self.me // 2

    def chip(self, k):
        return lax.rem(self.z + (k + self.nz) % self.nz, self.nz)

    def dev(self, k):
        return {'tensor': 2 * self.chip(k) + self.c}

    @property
    def sibling(self):
        return {'tensor': self.me + 1 - 2 * self.c}

    def barrier(self):
        sem = pltpu.get_barrier_semaphore()
        for k in range(1, self.nz):
            pl.semaphore_signal(sem, inc=1, device_id=self.dev(k), device_id_type=MESH)
        pl.semaphore_signal(sem, inc=1, device_id=self.sibling, device_id_type=MESH)
        pl.semaphore_wait(sem, self.nz)


def slot_of(nz):
    half = nz // 2
    order = [half] + [s * k for k in range(half - 1, 0, -1) for s in (1, -1)] + [0]
    table = {k: i for i, k in enumerate(order)}
    table[-half] = table[half]
    return table


def gather_messages(half):
    right = [(w, k) for k in range(half) for w in (0, 1) if w == 0 or k < half - 1]
    return right, [(1 - w, k) for w, k in right]


def scatter_messages(half):
    right = [(0, half)]
    for k in range(half - 1, 0, -1):
        right += [(1, k), (0, k)]
    return right, [(1 - w, -k) for w, k in right]


def remote(src, dst, send_sem, recv_sem, device):
    return pltpu.make_async_remote_copy(
        src_ref=src, dst_ref=dst, send_sem=send_sem, recv_sem=recv_sem, device_id=device, device_id_type=MESH
    )


def gather_kernel(
    n, ids_ref, emb_ref, up_ref, down_ref, grad_ref,
    x_ref, pick_ref, names_ref, flag_ref, ws_ref, gsib_ref,
    emb_v, w_v, ids_v, tri_v, col_v, req_s, req_r, hot_v, xs_v, xr_v, xp_v, xq_v,
    emb_sem, out_sem, ws_sem, wr_sem, ps_sem, pr_sem, qs_sem, qr_sem, xs_sem, xr_sem,
):
    ring = Ring(n)
    nz, half, c, z = ring.nz, ring.half, ring.c, ring.z
    slot = slot_of(nz)
    vocab, _ = emb_ref.shape
    tl = ids_ref.shape[1]
    tp = 2 * tl
    own = (up_ref, down_ref)

    ring.barrier()
    load_emb = pltpu.make_async_copy(emb_ref, emb_v, emb_sem.at[0])
    load_emb.start()
    own_ids = pltpu.make_async_copy(ids_ref, ids_v.at[c], emb_sem.at[1])
    own_ids.start()
    send_ids = remote(ids_ref, ids_v.at[c], ps_sem.at[0], pr_sem.at[0], ring.sibling)
    send_ids.start()

    moves = [[], []]
    for side, (sign, order) in enumerate(zip((1, -1), gather_messages(half))):
        for i, (w, k) in enumerate(order):
            src = own[w] if k == 0 else w_v.at[w, slot[-k * sign]]
            dst = w_v.at[w, slot[-(k + 1) * sign]]
            moves[side].append(remote(src, dst, ws_sem.at[side, i], wr_sem.at[side, i], ring.dev(sign)))
    for i in range(2):
        moves[0][i].start()
        moves[1][i].start()
    outs = [pltpu.make_async_copy(own[w], ws_ref.at[w, slot[0]], out_sem.at[w, slot[0]]) for w in range(2)]
    for copy in outs:
        copy.start()
    send_grad = remote(grad_ref, gsib_ref, ps_sem.at[1], pr_sem.at[1], ring.sibling)
    send_grad.start()

    def forward(i):
        for side, (sign, order) in enumerate(zip((1, -1), gather_messages(half))):
            w, k = order[i]
            moves[side][i].wait_recv()
            if i + 2 < len(order):
                moves[side][i + 2].start()
            s = slot[-(k + 1) * sign]
            copy = pltpu.make_async_copy(w_v.at[w, s], ws_ref.at[w, s], out_sem.at[w, s])
            copy.start()
            outs.append(copy)

    own_ids.wait()
    send_ids.wait_recv()
    ids = jnp.concatenate([ids_v[0], ids_v[1]], axis=1)
    ids_t = jnp.transpose(jnp.broadcast_to(ids, (LANES, tp)))
    seen = jnp.zeros((1, tp), F32)
    for i in range(tp // LANES):
        earlier = iota((LANES, tp), 0) + i * LANES < iota((LANES, tp), 1)
        tri_v[i * LANES:(i + 1) * LANES, :] = jnp.where(earlier, 1.0, 0.0).astype(BF16)
        same = ids_t[i * LANES:(i + 1) * LANES, 0:1] == ids
        hit = jnp.where(earlier & same, 1.0, 0.0)
        seen = jnp.maximum(seen, jnp.max(hit, axis=0, keepdims=True))
    row = iota((n, 1), 0)
    owner = jnp.where(row < nz, 2 * row + c, 2 * (row - nz) + 1 - c)
    base = (owner * vocab).astype(F32)
    member = jnp.where((seen < 0.5) & (ids >= base) & (ids < base + vocab), 1.0, 0.0)
    rank = jnp.dot(member.astype(BF16), tri_v[...], preferred_element_type=F32)
    count = jnp.max(jnp.sum(member, axis=1, keepdims=True), axis=0, keepdims=True)
    over = jnp.where(count > CAP, 1.0, 0.0)
    for k in range(nz):
        hit = (rank[k:k + 1, :] == iota((CAP, 1), 0).astype(F32)) & (member[k:k + 1, :] > 0.5)
        col = jnp.max(jnp.where(hit, ids, -1.0), axis=1, keepdims=True)
        col_v[k * CAP:(k + 1) * CAP, :] = jnp.broadcast_to(col, (CAP, LANES))
    cols_t = jnp.transpose(col_v[...])
    lane = iota((8, LANES), 1)
    per = LANES // CAP
    for k in range(nz):
        at = (k // per) * LANES
        tile = cols_t[0:8, at:at + LANES]
        if k % per:
            tile = pltpu.roll(tile, LANES - (k % per) * CAP, 1)
        req_s[k] = jnp.where(lane < CAP, tile, over)
    asks = []
    for d in range(1, nz):
        kk = ring.chip(d)
        asks.append(remote(req_s.at[kk], req_r.at[z], qs_sem.at[d], qr_sem.at[d], ring.dev(d)))
        asks[-1].start()
    req_r[z] = req_s[z]
    forward(0)
    pick_ref[...] = jnp.where(col_v[:, 0:1] == ids, 1.0, 0.0).astype(BF16)

    for copy in asks:
        copy.wait_recv()
    flag = req_r[0]
    for k in range(1, nz):
        flag = jnp.maximum(flag, req_r[k])
    flag_ref[...] = flag
    tiles = []
    for p in range(nz // per):
        tile = req_r[p * per]
        for j in range(1, per):
            part = pltpu.roll(req_r[p * per + j], j * CAP, 1)
            tile = jnp.where(lane < j * CAP, tile, part)
        tiles.append(tile)
    names = jnp.concatenate(tiles, axis=1) - (ring.me * vocab).astype(F32)
    names_ref[...] = names
    load_emb.wait()
    step = 512
    for i in range(vocab // step):
        here = (iota((step, 1), 0) + i * step).astype(F32) == names[0:1, :]
        hot_v[i * step:(i + 1) * step, :] = jnp.where(here, 1.0, 0.0).astype(BF16)
    for k in range(nz // 2):
        found = contract(hot_v[:, 2 * k * CAP:2 * (k + 1) * CAP], emb_v[...], 0, 0)
        xs_v[2 * k] = found[:CAP].astype(BF16)
        xs_v[2 * k + 1] = found[CAP:].astype(BF16)
    gives = []
    for d in range(1, nz):
        kk = ring.chip(d)
        gives.append(remote(xs_v.at[kk], xr_v.at[z], xs_sem.at[d], xr_sem.at[d], ring.dev(d)))
        gives[-1].start()
    xr_v[z] = xs_v[z]
    for i in range(1, len(moves[0])):
        forward(i)

    for copy in gives:
        copy.wait_recv()
    got = xr_v[...].reshape(nz * CAP, xr_v.shape[2])
    for b in range(0, tp, 256):
        xp_v[b:b + 256, :] = contract(pick_ref[:, b:b + 256], got, 0, 0).astype(BF16)
    swap = remote(xp_v, xq_v, ps_sem.at[2], pr_sem.at[2], ring.sibling)
    swap.start()
    swap.wait_recv()
    x_ref[...] = xp_v[...] + xq_v[...]

    send_grad.wait_recv()
    for copy in [send_ids, send_grad, swap] + asks + gives + moves[0] + moves[1]:
        copy.wait_send()
    for copy in outs:
        copy.wait()


def gather(n, ids, emb, up, down, grad):
    nz = n // 2
    vocab, dm = emb.shape
    tl, fl = ids.shape[1], up.shape[0]
    tp = 2 * tl
    vmem, hbm = pl.BlockSpec(memory_space=pltpu.VMEM), pl.BlockSpec(memory_space=pl.ANY)
    hops = n // 2 - 1
    return pl.pallas_call(
        functools.partial(gather_kernel, n),
        name='gather',
        out_shape=(
            jax.ShapeDtypeStruct((tp, dm), BF16),
            jax.ShapeDtypeStruct((nz * CAP, tp), BF16),
            jax.ShapeDtypeStruct((8, nz * CAP), F32),
            jax.ShapeDtypeStruct((8, LANES), F32),
            jax.ShapeDtypeStruct((2, nz, fl, dm), BF16),
            jax.ShapeDtypeStruct((tl, dm), BF16),
        ),
        in_specs=[vmem, hbm, vmem, vmem, hbm],
        out_specs=(vmem, vmem, vmem, vmem, hbm, hbm),
        scratch_shapes=[
            pltpu.VMEM((vocab, dm), BF16),
            pltpu.VMEM((2, nz, fl, dm), BF16),
            pltpu.VMEM((2, 1, tl), F32),
            pltpu.VMEM((tp, tp), BF16),
            pltpu.VMEM((nz * CAP, LANES), F32),
            pltpu.VMEM((nz, 8, LANES), F32),
            pltpu.VMEM((nz, 8, LANES), F32),
            pltpu.VMEM((vocab, nz * CAP), BF16),
            pltpu.VMEM((nz, CAP, dm), BF16),
            pltpu.VMEM((nz, CAP, dm), BF16),
            pltpu.VMEM((tp, dm), BF16),
            pltpu.VMEM((tp, dm), BF16),
            pltpu.SemaphoreType.DMA((2,)),
            pltpu.SemaphoreType.DMA((2, nz)),
            pltpu.SemaphoreType.DMA((2, hops)),
            pltpu.SemaphoreType.DMA((2, hops)),
            pltpu.SemaphoreType.DMA((3,)),
            pltpu.SemaphoreType.DMA((3,)),
            pltpu.SemaphoreType.DMA((nz,)),
            pltpu.SemaphoreType.DMA((nz,)),
            pltpu.SemaphoreType.DMA((nz,)),
            pltpu.SemaphoreType.DMA((nz,)),
        ],
        compiler_params=pltpu.CompilerParams(
            collective_id=0, has_side_effects=True, vmem_limit_bytes=VMEM_LIMIT
        ),
    )(ids, emb, up, down, grad)


def mlp_kernel(
    n, x_ref, grad_ref, gsib_ref, ws_ref, gain_ref, pick_ref,
    out_ref, dup_ref, ddown_ref, rows_ref, dx_out,
    g_v, n_v, w_v, h_v, du_v, dw_v, rb_v, dns_v, dno_v, dnr_v, ys_v, yo_v, yr_v, dx_v, es_v, out_v,
    ld_sem, w_sem, ss_sem, sr_sem, ps_sem, pr_sem, es_sem, er_sem, out_sem,
):
    ring = Ring(n)
    nz, half, c, z = ring.nz, ring.half, ring.c, ring.z
    slot = slot_of(nz)
    tp, dm = x_ref.shape
    tl = tp // 2
    ff = w_v.shape[1]
    fl = ff // nz
    chunks = ff // FCHUNK

    ring.barrier()
    loads = [
        pltpu.make_async_copy(grad_ref, g_v.at[pl.ds(c * tl, tl)], ld_sem.at[0]),
        pltpu.make_async_copy(gsib_ref, g_v.at[pl.ds((1 - c) * tl, tl)], ld_sem.at[1]),
    ]
    for copy in loads:
        copy.start()
    w_loads = []
    for j in range(chunks):
        at = pl.ds(j * FCHUNK, FCHUNK)
        w_loads.append(pltpu.make_async_copy(ws_ref.at[:, at], w_v.at[:, at], w_sem.at[j]))
        w_loads[-1].start()

    gain = gain_ref[...].astype(F32)

    def norm_rows(b, carry):
        at = pl.ds(pl.multiple_of(b * ROWS, ROWS), ROWS)
        xf = x_ref[at, :].astype(F32)
        inv = lax.rsqrt(jnp.mean(xf * xf, axis=-1, keepdims=True) + EPS)
        n_v[at, :] = (xf * inv * gain).astype(BF16)
        return carry

    lax.fori_loop(0, tp // ROWS, norm_rows, 0)
    for copy in loads:
        copy.wait()

    def chunk(j):
        fs = slice(j * FCHUNK, (j + 1) * FCHUNK)
        w_loads[j].wait()

        def token_block(b, carry):
            at = pl.ds(pl.multiple_of(b * 256, 256), 256)
            u = contract(n_v[at, :], w_v[0, fs, :], 1, 1).astype(BF16).astype(F32)
            dh = contract(g_v[at, :], w_v[1, fs, :], 1, 1)
            t = jnp.tanh(SQRT_2_PI * (u + CUBIC * (u * u * u)))
            cdf = 0.5 * (1.0 + t)
            slope = cdf + u * (0.5 * (1.0 - t * t)) * (SQRT_2_PI * (1.0 + (3.0 * CUBIC) * (u * u)))
            h_v[at, fs] = (u * cdf).astype(BF16)
            du_v[at, fs] = (dh * slope).astype(BF16)
            return carry

        lax.fori_loop(0, tp // 256, token_block, 0)
        dw_v[1, fs, :] = contract(h_v[:, fs], g_v[...], 0, 0)
        dw_v[0, fs, :] = contract(du_v[:, fs], n_v[...], 0, 0)

    orders = scatter_messages(half)
    sends = [[], []]
    for side, sign in enumerate((1, -1)):
        for i, (w, k) in enumerate(orders[side]):
            src = dw_v.at[w, pl.ds(slot[k] * fl, fl)]
            dst = rb_v.at[side, i]
            sends[side].append(remote(src, dst, ss_sem.at[side, i], sr_sem.at[side, i], ring.dev(sign)))

    def scatter(i):
        for side in range(2):
            w, k = orders[side][i]
            at = slice(slot[k] * fl, (slot[k] + 1) * fl)
            if i >= 2:
                sends[side][i - 2].wait_recv()
                dw_v[w, at, :] = dw_v[w, at, :] + rb_v[side, i - 2]
            sends[side][i].start()

    chunk(0)
    scatter(0)
    chunk(1)
    scatter(1)
    for j in range(2, chunks):
        chunk(j)
    scatter(2)

    mine, theirs = c * tl, (1 - c) * tl
    quarter = 128

    def partial_rows(src, w, start, dst):
        def body(b, carry):
            off = pl.multiple_of(b * quarter, quarter)
            dst[pl.ds(off, quarter), :] = jnp.dot(
                src[pl.ds(pl.multiple_of(start + off, quarter), quarter), :], w_v[w], preferred_element_type=F32
            )
            return carry

        lax.fori_loop(0, tl // quarter, body, 0)

    partial_rows(du_v, 0, theirs, dns_v)
    swap_dn = remote(dns_v, dnr_v, ps_sem.at[0], pr_sem.at[0], ring.sibling)
    swap_dn.start()
    partial_rows(du_v, 0, mine, dno_v)
    partial_rows(h_v, 1, theirs, ys_v)
    swap_y = remote(ys_v, yr_v, ps_sem.at[1], pr_sem.at[1], ring.sibling)
    swap_y.start()
    swap_dn.wait_recv()

    def dx_rows(b, carry):
        off = pl.multiple_of(b * ROWS, ROWS)
        loc, at = pl.ds(off, ROWS), pl.ds(pl.multiple_of(mine + off, ROWS), ROWS)
        xf = x_ref[at, :].astype(F32)
        inv = lax.rsqrt(jnp.mean(xf * xf, axis=-1, keepdims=True) + EPS)
        q = (dno_v[loc, :] + dnr_v[loc, :]) * gain
        dot = jnp.mean(xf * q, axis=-1, keepdims=True)
        dxn = inv * q - xf * (inv * inv * inv * dot)
        dx_v[at, :] = (g_v[at, :].astype(F32) + dxn).astype(BF16)
        return carry

    lax.fori_loop(0, tl // ROWS, dx_rows, 0)
    own_rows = dx_v.at[pl.ds(mine, tl)]
    swap_dx = remote(own_rows, own_rows, ps_sem.at[2], pr_sem.at[2], ring.sibling)
    swap_dx.start()
    keep_dx = pltpu.make_async_copy(own_rows, dx_out, out_sem.at[0])
    keep_dx.start()
    partial_rows(h_v, 1, mine, yo_v)
    swap_dx.wait_recv()

    for k in range(nz):
        es_v[k] = jnp.dot(pick_ref[k * CAP:(k + 1) * CAP, :], dx_v[...], preferred_element_type=F32)
    gives = []
    for d in range(1, nz):
        kk = ring.chip(d)
        gives.append(remote(es_v.at[kk], rows_ref.at[z], es_sem.at[d], er_sem.at[d], ring.dev(d)))
        gives[-1].start()
    own_give = pltpu.make_async_copy(es_v.at[z], rows_ref.at[z], out_sem.at[1])
    own_give.start()

    scatter(3)
    swap_y.wait_recv()

    def out_rows(b, carry):
        off = pl.multiple_of(b * ROWS, ROWS)
        loc, at = pl.ds(off, ROWS), pl.ds(pl.multiple_of(mine + off, ROWS), ROWS)
        out_v[loc, :] = (x_ref[at, :].astype(F32) + (yo_v[loc, :] + yr_v[loc, :])).astype(BF16)
        return carry

    lax.fori_loop(0, tl // ROWS, out_rows, 0)
    keep_out = pltpu.make_async_copy(out_v, out_ref, out_sem.at[2])
    keep_out.start()
    last = len(orders[0])
    for i in range(4, last):
        scatter(i)
    for side in range(2):
        for i in (last - 2, last - 1):
            sends[side][i].wait_recv()
    at = slice(slot[0] * fl, (slot[0] + 1) * fl)
    keeps = [keep_dx, own_give, keep_out]
    for w, dst in enumerate((dup_ref, ddown_ref)):
        a, b = (last - 1, last - 2) if w == 0 else (last - 2, last - 1)
        dw_v[w, at, :] = dw_v[w, at, :] + rb_v[0, a] + rb_v[1, b]
        keeps.append(pltpu.make_async_copy(dw_v.at[w, pl.ds(slot[0] * fl, fl)], dst, out_sem.at[3 + w]))
        keeps[-1].start()
    for copy in gives:
        copy.wait_recv()
    for copy in [swap_dn, swap_y, swap_dx] + gives + sends[0] + sends[1]:
        copy.wait_send()
    for copy in keeps:
        copy.wait()


def mlp(n, x, grad, gsib, ws, gain, pick):
    nz = n // 2
    tp, dm = x.shape
    tl = tp // 2
    ff = ws.shape[1]
    fl = ff // nz
    hops = n // 2 - 1
    vmem, hbm = pl.BlockSpec(memory_space=pltpu.VMEM), pl.BlockSpec(memory_space=pl.ANY)
    half_f32 = pltpu.VMEM((tl, dm), F32)
    dma = pltpu.SemaphoreType.DMA
    return pl.pallas_call(
        functools.partial(mlp_kernel, n),
        name='mlp',
        out_shape=(
            jax.ShapeDtypeStruct((tl, dm), BF16),
            jax.ShapeDtypeStruct((fl, dm), F32),
            jax.ShapeDtypeStruct((fl, dm), F32),
            jax.ShapeDtypeStruct((nz, CAP, dm), F32),
            jax.ShapeDtypeStruct((tl, dm), BF16),
        ),
        in_specs=[vmem, hbm, hbm, hbm, vmem, vmem],
        out_specs=(hbm,) * 5,
        scratch_shapes=[
            pltpu.VMEM((tp, dm), BF16),
            pltpu.VMEM((tp, dm), BF16),
            pltpu.VMEM((2, ff, dm), BF16),
            pltpu.VMEM((tp, ff), BF16),
            pltpu.VMEM((tp, ff), BF16),
            pltpu.VMEM((2, ff, dm), F32),
            pltpu.VMEM((2, hops, fl, dm), F32),
            half_f32, half_f32, half_f32, half_f32, half_f32, half_f32,
            pltpu.VMEM((tp, dm), BF16),
            pltpu.VMEM((nz, CAP, dm), F32),
            pltpu.VMEM((tl, dm), BF16),
            dma((2,)), dma((ff // FCHUNK,)), dma((2, hops)), dma((2, hops)),
            dma((3,)), dma((3,)), dma((nz,)), dma((nz,)), dma((5,)),
        ],
        compiler_params=pltpu.CompilerParams(
            collective_id=1, has_side_effects=True, vmem_limit_bytes=VMEM_LIMIT
        ),
    )(x, grad, gsib, ws, gain, pick)


def place_kernel(names_ref, rows_ref, out_ref, hi_v, mid_v, lo_v):
    @pl.when(pl.program_id(0) == 0)
    def _():
        rows = rows_ref[...]
        hi = rows.astype(BF16)
        rest = rows - hi.astype(F32)
        mid = rest.astype(BF16)
        hi_v[...] = hi
        mid_v[...] = mid
        lo_v[...] = (rest - mid.astype(F32)).astype(BF16)

    block = out_ref.shape[0]
    here = (iota((block, 1), 0) + pl.program_id(0) * block).astype(F32) == names_ref[0:1, :]
    hot = jnp.where(here, 1.0, 0.0).astype(BF16)
    out_ref[...] = (
        jnp.dot(hot, hi_v[...], preferred_element_type=F32)
        + jnp.dot(hot, mid_v[...], preferred_element_type=F32)
        + jnp.dot(hot, lo_v[...], preferred_element_type=F32)
    )


def place(vocab, names, rows):
    slots, dm = rows.shape
    block = 512
    whole = lambda i: (0, 0)
    return pl.pallas_call(
        place_kernel,
        name='place',
        grid=(vocab // block,),
        out_shape=jax.ShapeDtypeStruct((vocab, dm), F32),
        in_specs=[pl.BlockSpec((8, slots), whole), pl.BlockSpec((slots, dm), whole)],
        out_specs=pl.BlockSpec((block, dm), lambda i: (i, 0)),
        scratch_shapes=[pltpu.VMEM((slots, dm), BF16)] * 3,
        compiler_params=pltpu.CompilerParams(vmem_limit_bytes=48_000_000),
    )(names, rows)


def swap_kernel(n, src_ref, dst_ref, keep_sem, send_sem, recv_sem):
    me = lax.axis_index('tensor')
    sem = pltpu.get_barrier_semaphore()
    for d in range(1, n):
        pl.semaphore_signal(sem, inc=1, device_id={'tensor': lax.rem(me + d, n)}, device_id_type=MESH)
    pl.semaphore_wait(sem, n - 1)
    keep = pltpu.make_async_copy(src_ref.at[me], dst_ref.at[me], keep_sem)
    keep.start()
    copies = []
    for d in range(1, n):
        to = lax.rem(me + d, n)
        copies.append(remote(src_ref.at[to], dst_ref.at[me], send_sem.at[d], recv_sem.at[d], {'tensor': to}))
        copies[-1].start()
    for copy in copies:
        copy.wait()
    keep.wait()


def swap_blocks(n, blocks, collective_id):
    hbm = pl.BlockSpec(memory_space=pl.ANY)
    return pl.pallas_call(
        functools.partial(swap_kernel, n),
        name='swap_blocks',
        out_shape=jax.ShapeDtypeStruct(blocks.shape, blocks.dtype),
        in_specs=[hbm],
        out_specs=hbm,
        scratch_shapes=[pltpu.SemaphoreType.DMA, pltpu.SemaphoreType.DMA((n,)), pltpu.SemaphoreType.DMA((n,))],
        compiler_params=pltpu.CompilerParams(collective_id=collective_id, has_side_effects=True),
    )(blocks)


def all_blocks(n, block, collective_id):
    return swap_blocks(n, jnp.broadcast_to(block[None], (n,) + block.shape), collective_id)


def dense_lookup(n, ids, emb):
    vocab, dm = emb.shape
    me = lax.axis_index('tensor')
    ids_all = all_blocks(n, jnp.broadcast_to(ids, (8, ids.shape[1])), 2)[:, 0]
    rel = ids_all.reshape(-1, 1) - (me * vocab).astype(F32)
    hot = (iota((rel.shape[0], vocab), 1).astype(F32) == rel).astype(BF16)
    part = jnp.dot(hot, emb, preferred_element_type=F32).astype(BF16)
    parts = swap_blocks(n, part.reshape(n, -1, dm), 3)
    x_own = jnp.sum(parts.astype(F32), axis=0).astype(BF16)
    x_all = all_blocks(n, x_own, 4)
    pair = lax.dynamic_slice_in_dim(x_all, 2 * (me // 2), 2, axis=0)
    return pair.reshape(-1, dm)


def dense_place(n, vocab, ids, dx):
    me = lax.axis_index('tensor')
    ids_all = all_blocks(n, jnp.broadcast_to(ids, (8, ids.shape[1])), 5)[:, 0]
    dx_all = all_blocks(n, dx, 6).reshape(-1, dx.shape[1])
    rel = ids_all.reshape(1, -1) - (me * vocab).astype(F32)
    hot = (iota((vocab, rel.shape[1]), 0).astype(F32) == rel).astype(BF16)
    return jnp.dot(hot, dx_all, preferred_element_type=F32)


def solution(mesh):
    n = mesh.shape['tensor']
    tok_spec = P(('data', 'tensor'))
    row_spec = P(('data', 'tensor'), None)

    def local_step(token_ids, emb_shard, norm_gain, w_up, w_down, grad_out):
        vocab, dm = emb_shard.shape
        ids = token_ids.astype(F32)[None, :]
        x, pick, names, flags, ws, gsib = gather(n, ids, emb_shard, w_up.T, w_down, grad_out)
        crowded = flags[0, LANES - 1] > 0.5
        x = lax.cond(crowded, lambda: dense_lookup(n, ids, emb_shard), lambda: x)
        ws = ws.reshape(2, -1, dm)
        out, d_up, d_down, rows, dx = mlp(n, x, grad_out, gsib, ws, norm_gain[None, :], pick)
        d_emb = lax.cond(
            crowded,
            lambda: dense_place(n, vocab, ids, dx),
            lambda: place(vocab, names, rows.reshape(-1, dm)),
        )
        return out, d_emb, d_up.T, d_down

    return jax.shard_map(
        local_step,
        mesh=mesh,
        in_specs=(tok_spec, P('tensor', None), P(None), P(None, 'tensor'), P('tensor', None), row_spec),
        out_specs=(row_spec, row_spec, P('data', 'tensor'), row_spec),
        check_vma=False,
    )
```

```python
import functools

import jax
import jax.numpy as jnp
from jax import lax
from jax.experimental import pallas as pl
from jax.experimental.pallas import tpu as pltpu
from jax.sharding import PartitionSpec as P

EPS = 1e-6
CAP = 64
LANES = 128
MESH = pl.DeviceIdType.MESH
VMEM_LIMIT = 67_000_000
F32 = jnp.float32
BF16 = jnp.bfloat16
SQRT_2_PI = 0.7978845608028654
CUBIC = 0.044715


def contract(left_op, right_op, left_dim, right_dim):
    dims = (((left_dim,), (right_dim,)), ((), ()))
    return lax.dot_general(left_op, right_op, dims, preferred_element_type=F32)


def iota(shape, dim):
    return lax.broadcasted_iota(jnp.int32, shape, dim)


def gelu_pair(u):
    t = jnp.tanh(SQRT_2_PI * (u + CUBIC * (u * u * u)))
    cdf = 0.5 * (1.0 + t)
    slope = cdf + u * (0.5 * (1.0 - t * t)) * (SQRT_2_PI * (1.0 + (3.0 * CUBIC) * (u * u)))
    return u * cdf, slope


class Ring:
    def __init__(self, n):
        self.n, self.nz, self.half = n, n // 2, n // 4
        self.me = lax.axis_index('tensor')
        self.c = lax.rem(self.me, 2)
        self.z = self.me // 2

    def chip(self, k):
        return lax.rem(self.z + (k + self.nz) % self.nz, self.nz)

    def dev(self, k):
        return {'tensor': 2 * self.chip(k) + self.c}

    @property
    def sibling(self):
        return {'tensor': self.me + 1 - 2 * self.c}

    def barrier(self):
        sem = pltpu.get_barrier_semaphore()
        for k in range(1, self.nz):
            pl.semaphore_signal(sem, inc=1, device_id=self.dev(k), device_id_type=MESH)
        pl.semaphore_signal(sem, inc=1, device_id=self.sibling, device_id_type=MESH)
        pl.semaphore_wait(sem, self.nz)


def slot_of(nz):
    half = nz // 2
    order = [half] + [s * k for k in range(half - 1, 0, -1) for s in (1, -1)] + [0]
    table = {k: i for i, k in enumerate(order)}
    table[-half] = table[half]
    return table


def gather_messages(half):
    right = [(w, k) for k in range(half) for w in (0, 1) if w == 0 or k < half - 1]
    return right, [(1 - w, k) for w, k in right]


def scatter_messages(half):
    right = [(0, half)]
    for k in range(half - 1, 0, -1):
        right += [(1, k), (0, k)]
    return right, [(1 - w, -k) for w, k in right]


def remote(src, dst, send_sem, recv_sem, device):
    return pltpu.make_async_remote_copy(
        src_ref=src, dst_ref=dst, send_sem=send_sem, recv_sem=recv_sem, device_id=device, device_id_type=MESH
    )


class Fold:
    def __init__(self, dm):
        self.dm = dm
        self.lo = dm // LANES * LANES
        self.dp = self.lo + LANES
        assert 2 * (dm - self.lo) == LANES

    def tail(self, value):
        h = value.shape[0] // 2
        return jnp.concatenate([value[:h, self.lo:self.dm], value[h:, self.lo:self.dm]], axis=1)

    def store(self, ref, value):
        h = value.shape[0] // 2
        ref[:, :self.lo] = value[:, :self.lo]
        ref[:h, self.lo:] = self.tail(value)

    def add(self, ref, value):
        h = value.shape[0] // 2
        ref[:, :self.lo] = ref[:, :self.lo] + value[:, :self.lo]
        ref[:h, self.lo:] = ref[:h, self.lo:] + self.tail(value)

    def unfold(self, ref):
        h = ref.shape[0] // 2
        ref[h:, self.lo:self.dm] = ref[:h, self.dm:self.dp]

    def send(self, src, dst, send_sem, recv_sem, device):
        return FoldCopy(self, src, dst, send_sem, recv_sem, device)


class FoldCopy:
    def __init__(self, fold, src, dst, send_sem, recv_sem, device):
        rows = src.shape[0]
        h = rows // 2
        parts = ((pl.ds(0, h), pl.ds(0, fold.dp)), (pl.ds(h, h), pl.ds(0, fold.lo)))
        self.copies = [
            remote(src.at[r, l], dst.at[r, l], send_sem.at[i], recv_sem.at[i], device)
            for i, (r, l) in enumerate(parts)
        ]

    def start(self):
        for copy in self.copies:
            copy.start()

    def wait_recv(self):
        for copy in self.copies:
            copy.wait_recv()

    def wait_send(self):
        for copy in self.copies:
            copy.wait_send()


def step_kernel(
    n, ids_ref, emb_ref, up_ref, down_ref, grad_ref, gain_ref,
    out_ref, dup_ref, ddown_ref, rows_ref, names_ref, flag_ref,
    w_v, g_v, x_v, xq_v, n_v, h_v, du_v, st_v, rb_v, snd_v, own_v, dnr_v, yr_v, dx_v, es_v, er_v, xs_v, xr_v,
    pick_v, tri_v, ids_v, col_v, req_s, req_r, emb_v, out_v, rows_v,
    ld_sem, emb_sem, ws_sem, wr_sem, ps_sem, pr_sem, qs_sem, qr_sem, xs_sem, xr_sem,
    ss_sem, sr_sem, es_sem, er_sem, out_sem,
):
    ring = Ring(n)
    nz, half, c, z = ring.nz, ring.half, ring.c, ring.z
    slot = slot_of(nz)
    dm, vocab = emb_ref.shape
    fl = up_ref.shape[0]
    tl = ids_ref.shape[1]
    tp = 2 * tl
    slots = nz * CAP
    fold = Fold(dm)
    step = emb_v.shape[2]
    sides = ((0, 1), (1, -1))
    sent = []

    load_grad = pltpu.make_async_copy(grad_ref, g_v.at[c], ld_sem.at[0])
    load_grad.start()
    own_ids = pltpu.make_async_copy(ids_ref, ids_v.at[c], ld_sem.at[1])
    own_ids.start()

    def load_emb(i):
        return pltpu.make_async_copy(emb_ref.at[:, pl.ds(i * step, step)], emb_v.at[i % 2], emb_sem.at[i % 2])

    for i in range(2):
        load_emb(i).start()
    mine = slot[0]
    for w, ref in enumerate((up_ref, down_ref)):
        w_v[w, mine, :, :dm] = ref[...]
        w_v[w, mine, :fl // 2, dm:] = ref[fl // 2:, fold.lo:]
    ring.barrier()

    def start(copy):
        copy.start()
        sent.append(copy)
        return copy

    swap_ids = start(remote(ids_ref, ids_v.at[c], ps_sem.at[0], pr_sem.at[0], ring.sibling))

    moves = [[], []]
    for side, sign in sides:
        for i, (w, k) in enumerate(gather_messages(half)[side]):
            src, dst = w_v.at[w, slot[-k * sign]], w_v.at[w, slot[-(k + 1) * sign]]
            moves[side].append(fold.send(src, dst, ws_sem.at[side, i], wr_sem.at[side, i], ring.dev(sign)))
    for i in range(2):
        for side, _ in sides:
            start(moves[side][i])
    swap_grad = start(remote(grad_ref, g_v.at[c], ps_sem.at[1], pr_sem.at[1], ring.sibling))

    def forward(i):
        for side, sign in sides:
            moves[side][i].wait_recv()
            if i + 2 < len(moves[side]):
                start(moves[side][i + 2])
            w, k = gather_messages(half)[side][i]
            fold.unfold(w_v.at[w, slot[-(k + 1) * sign]])

    own_ids.wait()
    swap_ids.wait_recv()
    ids = jnp.concatenate([ids_v[0], ids_v[1]], axis=1)
    ids_t = jnp.transpose(jnp.broadcast_to(ids, (LANES, tp)))
    seen = jnp.zeros((1, tp), F32)
    for i in range(tp // LANES):
        earlier = iota((LANES, tp), 0) + i * LANES < iota((LANES, tp), 1)
        tri_v[i * LANES:(i + 1) * LANES, :] = jnp.where(earlier, 1.0, 0.0).astype(BF16)
        same = ids_t[i * LANES:(i + 1) * LANES, 0:1] == ids
        hit = jnp.where(earlier & same, 1.0, 0.0)
        seen = jnp.maximum(seen, jnp.max(hit, axis=0, keepdims=True))
    row = iota((n, 1), 0)
    owner = jnp.where(row < nz, 2 * row + c, 2 * (row - nz) + 1 - c)
    base = (owner * vocab).astype(F32)
    member = jnp.where((seen < 0.5) & (ids >= base) & (ids < base + vocab), 1.0, 0.0)
    rank = jnp.dot(member.astype(BF16), tri_v[...], preferred_element_type=F32)
    count = jnp.max(jnp.sum(member, axis=1, keepdims=True), axis=0, keepdims=True)
    over = jnp.where(count > CAP, 1.0, 0.0)
    for k in range(nz):
        hit = (rank[k:k + 1, :] == iota((CAP, 1), 0).astype(F32)) & (member[k:k + 1, :] > 0.5)
        col = jnp.max(jnp.where(hit, ids, -1.0), axis=1, keepdims=True)
        col_v[k * CAP:(k + 1) * CAP, :] = jnp.broadcast_to(col, (CAP, LANES))
    cols_t = jnp.transpose(col_v[...])
    lane = iota((8, LANES), 1)
    per = LANES // CAP
    for k in range(nz):
        at = (k // per) * LANES
        tile = cols_t[0:8, at:at + LANES]
        if k % per:
            tile = pltpu.roll(tile, LANES - (k % per) * CAP, 1)
        req_s[k] = jnp.where(lane < CAP, tile, over)
    asks = []
    for d in range(1, nz):
        asks.append(start(remote(req_s.at[ring.chip(d)], req_r.at[z], qs_sem.at[d], qr_sem.at[d], ring.dev(d))))
    req_r[z] = req_s[z]
    forward(0)
    for t in range(2):
        pick_v[t] = jnp.where(col_v[:, 0:1] == ids_v[t], 1.0, 0.0).astype(BF16)

    for copy in asks:
        copy.wait_recv()
    flag = req_r[0]
    for k in range(1, nz):
        flag = jnp.maximum(flag, req_r[k])
    flag_ref[...] = flag
    tiles = []
    for p in range(nz // per):
        tile = req_r[p * per]
        for j in range(1, per):
            tile = jnp.where(lane < j * CAP, tile, pltpu.roll(req_r[p * per + j], j * CAP, 1))
        tiles.append(tile)
    names = jnp.concatenate(tiles, axis=1) - (ring.me * vocab).astype(F32)
    names_ref[...] = jnp.transpose(jnp.broadcast_to(names[0:1, :], (LANES, slots)))
    for i in range(vocab // step):
        load_emb(i).wait()
        hot = jnp.where(names_ref[:, 0:1] == (iota((1, step), 1) + i * step).astype(F32), 1.0, 0.0).astype(BF16)
        found = contract(hot, emb_v[i % 2], 1, 1)
        if i + 2 < vocab // step:
            load_emb(i + 2).start()
        for k in range(nz):
            part = found[k * CAP:(k + 1) * CAP]
            if i == 0:
                es_v[k, :, :dm] = part
            else:
                es_v[k, :, :dm] = es_v[k, :, :dm] + part
    for k in range(nz):
        fold.store(xs_v.at[k], es_v[k, :, :dm].astype(BF16))
    gives = []
    for d in range(1, nz):
        gives.append(start(fold.send(xs_v.at[ring.chip(d)], xr_v.at[z], xs_sem.at[d], xr_sem.at[d], ring.dev(d))))
    xr_v[z] = xs_v[z]
    forward(1)
    forward(2)
    forward(3)

    for copy in gives:
        copy.wait_recv()
    for k in range(nz):
        fold.unfold(xr_v.at[k])
    got = xr_v[...].reshape(slots, fold.dp)[:, :dm]
    for t in range(2):
        x_v[t] = contract(got, pick_v[t], 0, 0).astype(BF16)
    swap_x = remote(x_v, xq_v, ps_sem.at[2], pr_sem.at[2], ring.sibling)
    swap_x.start()
    load_grad.wait()
    swap_grad.wait_recv()
    swap_x.wait_send()
    swap_x.wait_recv()

    def lane_blocks(body):
        for t in range(2):
            lax.fori_loop(0, tl // LANES, functools.partial(body, t), 0)

    def lanes(b):
        return pl.ds(pl.multiple_of(b * LANES, LANES), LANES)

    def norm(t, b, carry):
        at = lanes(b)
        xb = x_v[t, :, at] + xq_v[t, :, at]
        x_v[t, :, at] = xb
        xf = xb.astype(F32)
        inv = lax.rsqrt(jnp.mean(xf * xf, axis=0, keepdims=True) + EPS)
        n_v[t, :, at] = (xf * inv * gain_ref[...]).astype(BF16)
        return carry

    lane_blocks(norm)

    def hidden(k):
        s = slot[k]

        def half_tokens(t, carry):
            u = jnp.dot(w_v[0, s, :, :dm], n_v[t], preferred_element_type=F32).astype(BF16).astype(F32)
            dh = jnp.dot(w_v[1, s, :, :dm], g_v[t], preferred_element_type=F32)
            act, slope = gelu_pair(u)
            h_v[t, s * fl:(s + 1) * fl, :] = act.astype(BF16)
            du_v[t, s * fl:(s + 1) * fl, :] = (dh * slope).astype(BF16)
            return carry

        lax.fori_loop(0, 2, half_tokens, 0)

    def grad_w(w, k):
        s = slice(slot[k] * fl, (slot[k] + 1) * fl)
        left, right = (h_v, g_v) if w else (du_v, n_v)
        return contract(left[0, s, :], right[0], 1, 1) + contract(left[1, s, :], right[1], 1, 1)

    orders = scatter_messages(half)
    sends = [[], []]
    for side, sign in sides:
        for i in range(len(orders[0])):
            src = st_v.at[side, i] if i < 2 else rb_v.at[side, i - 2]
            dst = rb_v.at[side, i]
            sends[side].append(fold.send(src, dst, ss_sem.at[side, i], sr_sem.at[side, i], ring.dev(sign)))

    def scatter(i):
        for side, _ in sides:
            part = grad_w(*orders[side][i])
            if i < 2:
                fold.store(st_v.at[side, i], part)
            else:
                sends[side][i - 2].wait_recv()
                fold.add(rb_v.at[side, i - 2], part)
            start(sends[side][i])

    hidden(0)
    for k in range(1, half):
        hidden(k)
        hidden(-k)
        for i in (2 * k + 2, 2 * k + 3):
            if i < len(moves[0]):
                forward(i)
    hidden(half)
    scatter(0)
    scatter(1)

    blocks = [(a, min(a + 2 * LANES, dm)) for a in range(0, dm, 2 * LANES)]

    def through(w, right, dst):
        for a, b in blocks:
            left = w_v[w, :, :, a:b].reshape(nz * fl, b - a)
            dst[a:b, :] = contract(left, right, 0, 0)

    through(0, du_v[1 - c], snd_v)
    swap_dn = remote(snd_v, dnr_v, ps_sem.at[3], pr_sem.at[3], ring.sibling)
    swap_dn.start()
    through(0, du_v[c], own_v)
    scatter(2)
    swap_dn.wait_send()
    swap_dn.wait_recv()

    def dx_block(b, carry):
        at = lanes(b)
        xf = x_v[c, :, at].astype(F32)
        inv = lax.rsqrt(jnp.mean(xf * xf, axis=0, keepdims=True) + EPS)
        q = (own_v[:, at] + dnr_v[:, at]) * gain_ref[...]
        dot = jnp.mean(xf * q, axis=0, keepdims=True)
        dxn = inv * q - xf * (inv * inv * inv * dot)
        dx_v[c, :, at] = (g_v[c, :, at].astype(F32) + dxn).astype(BF16)
        return carry

    lax.fori_loop(0, tl // LANES, dx_block, 0)
    swap_dx = start(remote(dx_v.at[c], dx_v.at[c], ps_sem.at[4], pr_sem.at[4], ring.sibling))
    through(1, h_v[1 - c], snd_v)
    swap_y = start(remote(snd_v, yr_v, ps_sem.at[5], pr_sem.at[5], ring.sibling))
    swap_dx.wait_recv()
    for k in range(nz):
        rows = slice(k * CAP, (k + 1) * CAP)
        fold.store(es_v.at[k], contract(pick_v[0, rows, :], dx_v[0], 1, 1) + contract(pick_v[1, rows, :], dx_v[1], 1, 1))
    backs = []
    for d in range(1, nz):
        backs.append(start(fold.send(es_v.at[ring.chip(d)], er_v.at[z], es_sem.at[d], er_sem.at[d], ring.dev(d))))
    er_v[z] = es_v[z]
    scatter(3)
    through(1, h_v[c], own_v)
    swap_y.wait_recv()

    def out_block(b, carry):
        at = lanes(b)
        out_v[:, at] = (x_v[c, :, at].astype(F32) + (own_v[:, at] + yr_v[:, at])).astype(BF16)
        return carry

    lax.fori_loop(0, tl // LANES, out_block, 0)
    keeps = [pltpu.make_async_copy(out_v, out_ref, out_sem.at[0])]
    keeps[0].start()
    last = len(orders[0])
    for i in range(4, last):
        scatter(i)

    for copy in backs:
        copy.wait_recv()
    for k in range(nz):
        fold.unfold(er_v.at[k])
        rows = er_v[k, :, :dm]
        at = slice(k * CAP, (k + 1) * CAP)
        for p in range(3):
            piece = rows.astype(BF16)
            rows_v[p, at, :] = piece
            rows = rows - piece.astype(F32)
    keeps.append(pltpu.make_async_copy(rows_v, rows_ref, out_sem.at[1]))
    keeps[1].start()

    for w in range(2):
        a, b = (last - 1, last - 2) if w == 0 else (last - 2, last - 1)
        part = grad_w(w, 0)
        sends[0][a].wait_recv()
        sends[1][b].wait_recv()
        rb_v[0, a] = rb_v[0, a] + rb_v[1, b]
        fold.unfold(rb_v.at[0, a])
        (dup_ref, ddown_ref)[w][...] = rb_v[0, a, :, :dm] + part
    for copy in sent:
        copy.wait_send()
    for copy in keeps:
        copy.wait()


def step(n, ids, emb_t, up, down, grad_t, gain):
    nz = n // 2
    dm, vocab = emb_t.shape
    tl, fl = ids.shape[1], up.shape[0]
    tp = 2 * tl
    dp = Fold(dm).dp
    slots = nz * CAP
    hops = nz - 1
    vmem, hbm = pl.BlockSpec(memory_space=pltpu.VMEM), pl.BlockSpec(memory_space=pl.ANY)
    dma = pltpu.SemaphoreType.DMA
    tokens = pltpu.VMEM((2, dm, tl), BF16)
    partial = pltpu.VMEM((dm, tl), F32)
    return pl.pallas_call(
        functools.partial(step_kernel, n),
        name='step',
        out_shape=(
            jax.ShapeDtypeStruct((dm, tl), BF16),
            jax.ShapeDtypeStruct((fl, dm), F32),
            jax.ShapeDtypeStruct((fl, dm), F32),
            jax.ShapeDtypeStruct((3, slots, dm), BF16),
            jax.ShapeDtypeStruct((slots, LANES), F32),
            jax.ShapeDtypeStruct((8, LANES), F32),
        ),
        in_specs=[vmem, hbm, vmem, vmem, hbm, vmem],
        out_specs=(hbm, vmem, vmem, hbm, vmem, vmem),
        scratch_shapes=[
            pltpu.VMEM((2, nz, fl, dp), BF16),
            tokens, tokens, tokens, tokens,
            pltpu.VMEM((2, nz * fl, tl), BF16),
            pltpu.VMEM((2, nz * fl, tl), BF16),
            pltpu.VMEM((2, 2, fl, dp), F32),
            pltpu.VMEM((2, hops, fl, dp), F32),
            partial, partial, partial, partial,
            tokens,
            pltpu.VMEM((nz, CAP, dp), F32),
            pltpu.VMEM((nz, CAP, dp), F32),
            pltpu.VMEM((nz, CAP, dp), BF16),
            pltpu.VMEM((nz, CAP, dp), BF16),
            pltpu.VMEM((2, slots, tl), BF16),
            pltpu.VMEM((tp, tp), BF16),
            pltpu.VMEM((2, 1, tl), F32),
            pltpu.VMEM((slots, LANES), F32),
            pltpu.VMEM((nz, 8, LANES), F32),
            pltpu.VMEM((nz, 8, LANES), F32),
            pltpu.VMEM((2, dm, 512), BF16),
            pltpu.VMEM((dm, tl), BF16),
            pltpu.VMEM((3, slots, dm), BF16),
            dma((2,)), dma((2,)), dma((2, hops, 2)), dma((2, hops, 2)), dma((6,)), dma((6,)),
            dma((nz,)), dma((nz,)), dma((nz, 2)), dma((nz, 2)),
            dma((2, hops, 2)), dma((2, hops, 2)), dma((nz, 2)), dma((nz, 2)), dma((2,)),
        ],
        compiler_params=pltpu.CompilerParams(
            collective_id=0, has_side_effects=True, vmem_limit_bytes=VMEM_LIMIT
        ),
    )(ids, emb_t, up, down, grad_t, gain)


def place_kernel(names_ref, rows_ref, out_ref):
    block = out_ref.shape[1]
    here = names_ref[:, 0:1] == (iota((1, block), 1) + pl.program_id(0) * block).astype(F32)
    hot = jnp.where(here, 1.0, 0.0).astype(BF16)
    out_ref[...] = contract(rows_ref[0], hot, 0, 0) + contract(rows_ref[1], hot, 0, 0) + contract(rows_ref[2], hot, 0, 0)


def place(vocab, names, rows):
    _, slots, dm = rows.shape
    block = 512
    return pl.pallas_call(
        place_kernel,
        name='place',
        grid=(vocab // block,),
        out_shape=jax.ShapeDtypeStruct((dm, vocab), F32),
        in_specs=[
            pl.BlockSpec((slots, LANES), lambda i: (0, 0)),
            pl.BlockSpec((3, slots, dm), lambda i: (0, 0, 0)),
        ],
        out_specs=pl.BlockSpec((dm, block), lambda i: (0, i)),
        compiler_params=pltpu.CompilerParams(vmem_limit_bytes=48_000_000),
    )(names, rows)


def swap_kernel(n, src_ref, dst_ref, keep_sem, send_sem, recv_sem):
    me = lax.axis_index('tensor')
    sem = pltpu.get_barrier_semaphore()
    for d in range(1, n):
        pl.semaphore_signal(sem, inc=1, device_id={'tensor': lax.rem(me + d, n)}, device_id_type=MESH)
    pl.semaphore_wait(sem, n - 1)
    keep = pltpu.make_async_copy(src_ref.at[me], dst_ref.at[me], keep_sem)
    keep.start()
    copies = []
    for d in range(1, n):
        to = lax.rem(me + d, n)
        copies.append(remote(src_ref.at[to], dst_ref.at[me], send_sem.at[d], recv_sem.at[d], {'tensor': to}))
        copies[-1].start()
    for copy in copies:
        copy.wait()
    keep.wait()


def swap_blocks(n, blocks, collective_id):
    hbm = pl.BlockSpec(memory_space=pl.ANY)
    return pl.pallas_call(
        functools.partial(swap_kernel, n),
        name='swap_blocks',
        out_shape=jax.ShapeDtypeStruct(blocks.shape, blocks.dtype),
        in_specs=[hbm],
        out_specs=hbm,
        scratch_shapes=[pltpu.SemaphoreType.DMA, pltpu.SemaphoreType.DMA((n,)), pltpu.SemaphoreType.DMA((n,))],
        compiler_params=pltpu.CompilerParams(collective_id=collective_id, has_side_effects=True),
    )(blocks)


def all_blocks(n, block, collective_id):
    return swap_blocks(n, jnp.broadcast_to(block[None], (n,) + block.shape), collective_id)


def rms_norm(x_rows, gain_f):
    inv_rms = lax.rsqrt(jnp.mean(x_rows * x_rows, axis=-1, keepdims=True) + EPS)
    return x_rows * inv_rms * gain_f


def dense_step(n, ids, emb, norm_gain, up, down, grad_out):
    vocab, dm = emb.shape
    fl = up.shape[0]
    base = (lax.axis_index('tensor') * vocab).astype(F32)
    ids_all = all_blocks(n, jnp.broadcast_to(ids, (8, ids.shape[1])), 1)[:, 0]
    hot = (iota((ids_all.size, vocab), 1).astype(F32) == ids_all.reshape(-1, 1) - base).astype(BF16)
    part = jnp.dot(hot, emb, preferred_element_type=F32).astype(BF16)
    x_f = jnp.sum(swap_blocks(n, part.reshape(n, -1, dm), 2).astype(F32), axis=0)
    ws = all_blocks(n, jnp.stack([up, down]), 3)
    up_all, down_all = ws[:, 0].reshape(-1, dm), ws[:, 1].reshape(-1, dm)
    normed_f, norm_back = jax.vjp(lambda x_in: rms_norm(x_in, norm_gain.astype(F32)), x_f)
    normed = normed_f.astype(BF16)
    pre_act = contract(normed, up_all, 1, 1).astype(BF16).astype(F32)
    act_f, slope = gelu_pair(pre_act)
    hidden = act_f.astype(BF16)
    d_pre = (contract(grad_out, down_all, 1, 1) * slope).astype(BF16)
    y = jnp.dot(hidden, down_all, preferred_element_type=F32)
    out = (x_f + y).astype(BF16)
    d_norm = jnp.dot(d_pre, up_all, preferred_element_type=F32)
    dx = (grad_out.astype(F32) + norm_back(d_norm)[0]).astype(BF16)
    d_w = jnp.stack([contract(d_pre, normed, 0, 0), contract(hidden, grad_out, 0, 0)]).reshape(2, n, fl, dm)
    d_w = jnp.sum(swap_blocks(n, jnp.moveaxis(d_w, 1, 0), 4), axis=0)
    dx_all = all_blocks(n, dx, 5).reshape(-1, dm)
    hot_t = (iota((vocab, ids_all.size), 0).astype(F32) == ids_all.reshape(1, -1) - base).astype(BF16)
    d_emb = jnp.dot(hot_t, dx_all, preferred_element_type=F32)
    return out.T, d_emb.T, d_w[0], d_w[1]


def solution(mesh):
    n = mesh.shape['tensor']
    tok_spec = P(('data', 'tensor'))
    row_spec = P(('data', 'tensor'), None)

    def local_step(token_ids, emb_shard, norm_gain, w_up, w_down, grad_out):
        vocab, dm = emb_shard.shape
        ids = token_ids.astype(F32)[None, :]
        gain = jnp.broadcast_to(norm_gain.astype(F32)[:, None], (dm, LANES))
        up = w_up.T
        out, d_up, d_down, rows, names, flags = step(n, ids, emb_shard.T, up, w_down, grad_out.T, gain)
        out, d_emb, d_up, d_down = lax.cond(
            flags[0, LANES - 1] > 0.5,
            lambda: dense_step(n, ids, emb_shard, norm_gain, up, w_down, grad_out),
            lambda: (out, place(vocab, names, rows), d_up, d_down),
        )
        return out.T, d_emb.T, d_up.T, d_down

    return jax.shard_map(
        local_step,
        mesh=mesh,
        in_specs=(tok_spec, P('tensor', None), P(None), P(None, 'tensor'), P('tensor', None), row_spec),
        out_specs=(row_spec, row_spec, P('data', 'tensor'), row_spec),
        check_vma=False,
    )
```

```python
import functools

import jax
import jax.numpy as jnp
from jax import lax
from jax.experimental import pallas as pl
from jax.experimental.pallas import tpu as pltpu
from jax.sharding import PartitionSpec as P

EPS = 1e-6
CAP = 64
MULTI = 16
BHEAD = 32
LANES = 128
MESH = pl.DeviceIdType.MESH
VMEM_LIMIT = 67_000_000
F32 = jnp.float32
BF16 = jnp.bfloat16
SQRT_2_PI = 0.7978845608028654
CUBIC = 0.044715


def contract(left_op, right_op, left_dim, right_dim):
    dims = (((left_dim,), (right_dim,)), ((), ()))
    return lax.dot_general(left_op, right_op, dims, preferred_element_type=F32)


def iota(shape, dim):
    return lax.broadcasted_iota(jnp.int32, shape, dim)


def gelu_pair(u):
    t = jnp.tanh(SQRT_2_PI * (u + CUBIC * (u * u * u)))
    cdf = 0.5 * (1.0 + t)
    slope = cdf + u * (0.5 * (1.0 - t * t)) * (SQRT_2_PI * (1.0 + (3.0 * CUBIC) * (u * u)))
    return u * cdf, slope


class Ring:
    def __init__(self, n):
        self.n, self.nz, self.half = n, n // 2, n // 4
        self.me = lax.axis_index('tensor')
        self.c = lax.rem(self.me, 2)
        self.z = self.me // 2

    def chip(self, k):
        return lax.rem(self.z + (k + self.nz) % self.nz, self.nz)

    def dev(self, k):
        return {'tensor': 2 * self.chip(k) + self.c}

    @property
    def sibling(self):
        return {'tensor': self.me + 1 - 2 * self.c}

    def barrier(self):
        sem = pltpu.get_barrier_semaphore()
        for k in range(1, self.nz):
            pl.semaphore_signal(sem, inc=1, device_id=self.dev(k), device_id_type=MESH)
        pl.semaphore_signal(sem, inc=1, device_id=self.sibling, device_id_type=MESH)
        pl.semaphore_wait(sem, self.nz)


def slot_of(nz):
    half = nz // 2
    order = [half] + [s * k for k in range(half - 1, 0, -1) for s in (1, -1)] + [0]
    table = {k: i for i, k in enumerate(order)}
    table[-half] = table[half]
    return table


def gather_messages(half):
    right = [(w, k) for k in range(half) for w in (0, 1) if w == 0 or k < half - 1]
    return right, [(1 - w, k) for w, k in right]


def scatter_messages(half):
    right = [(0, half)]
    for k in range(half - 1, 0, -1):
        right += [(1, k), (0, k)]
    return right, [(1 - w, -k) for w, k in right]


def remote(src, dst, send_sem, recv_sem, device):
    return pltpu.make_async_remote_copy(
        src_ref=src, dst_ref=dst, send_sem=send_sem, recv_sem=recv_sem, device_id=device, device_id_type=MESH
    )


class Fold:
    def __init__(self, dm):
        self.dm = dm
        self.lo = dm // LANES * LANES
        self.dp = self.lo + LANES
        assert 2 * (dm - self.lo) == LANES

    def tail(self, value, h):
        low = value.shape[0] - h
        return jnp.concatenate([value[:low, self.lo:self.dm], value[h:, self.lo:self.dm]], axis=1)

    def store(self, ref, value, h):
        low = value.shape[0] - h
        ref[:, :self.lo] = value[:, :self.lo]
        ref[:low, self.lo:] = self.tail(value, h)
        if low < h:
            ref[low:h, self.lo:self.dm] = value[low:h, self.lo:self.dm]

    def add(self, ref, value, h):
        low = value.shape[0] - h
        ref[:, :self.lo] = ref[:, :self.lo] + value[:, :self.lo]
        ref[:low, self.lo:] = ref[:low, self.lo:] + self.tail(value, h)

    def unfold(self, ref, h):
        low = ref.shape[0] - h
        ref[h:, self.lo:self.dm] = ref[:low, self.dm:self.dp]

    def send(self, src, dst, h, send_sem, recv_sem, device):
        return FoldCopy(self, src, dst, h, send_sem, recv_sem, device)


class FoldCopy:
    def __init__(self, fold, src, dst, h, send_sem, recv_sem, device):
        parts = ((pl.ds(0, h), pl.ds(0, fold.dp)), (pl.ds(h, src.shape[0] - h), pl.ds(0, fold.lo)))
        self.copies = [
            remote(src.at[r, l], dst.at[r, l], send_sem.at[i], recv_sem.at[i], device)
            for i, (r, l) in enumerate(parts)
        ]

    def start(self):
        for copy in self.copies:
            copy.start()

    def wait_recv(self):
        for copy in self.copies:
            copy.wait_recv()

    def wait_send(self):
        for copy in self.copies:
            copy.wait_send()


def step_kernel(
    n, ids_ref, emb_ref, up_ref, down_ref, grad_ref, gain_ref,
    out_ref, dup_ref, ddown_ref, rows_ref, names_ref, flag_ref,
    w_v, gn_v, x_v, xq_v, hd_v, st_v, rb_v, snd_v, own_v, dnr_v, yr_v, dx_v, es_v, er_v, eb_v, eq_v, xs_v, xr_v,
    pick_v, tri_v, ids_v, col_v, name_v, req_s, req_r, emb_v, found_v, out_v, rows_v, row_v, gain_v,
    ld_sem, emb_sem, ws_sem, wr_sem, ps_sem, pr_sem, qs_sem, qr_sem, xs_sem, xr_sem,
    ss_sem, sr_sem, es_sem, er_sem, out_sem,
):
    ring = Ring(n)
    nz, half, c, z = ring.nz, ring.half, ring.c, ring.z
    slot = slot_of(nz)
    dm, vocab = emb_ref.shape
    fl = up_ref.shape[0]
    tl = ids_ref.shape[1]
    tp = 2 * tl
    slots = nz * CAP
    fold = Fold(dm)
    wh, xh, eh, bh = fl // 2, CAP // 2, MULTI // 2, BHEAD
    step = emb_v.shape[2]
    sides = ((0, 1), (1, -1))
    sent = []

    load_grad = pltpu.make_async_copy(grad_ref, gn_v.at[1, c], ld_sem.at[0])
    load_grad.start()
    own_ids = pltpu.make_async_copy(ids_ref, ids_v.at[c], ld_sem.at[1])
    own_ids.start()

    def load_emb(i):
        b = lax.rem(i, 2)
        at = pl.ds(pl.multiple_of(i * step, step), step)
        return pltpu.make_async_copy(emb_ref.at[:, at], emb_v.at[b], emb_sem.at[b])

    for i in range(2):
        load_emb(i).start()
    mine = slot[0]
    for w, ref in enumerate((up_ref, down_ref)):
        w_v[w, mine, :, :dm] = ref[...]
        w_v[w, mine, :wh, dm:] = ref[wh:, fold.lo:]
    row_v[...] = jnp.zeros_like(row_v)
    row_v[:, :dm] = gain_ref[...].astype(F32)
    gain_v[...] = jnp.transpose(jnp.broadcast_to(row_v[...], (LANES, fold.dp)))
    with jax.named_scope('barrier'):
        ring.barrier()

    def start(copy):
        copy.start()
        sent.append(copy)
        return copy

    swap_ids = start(remote(ids_ref, ids_v.at[c], ps_sem.at[0], pr_sem.at[0], ring.sibling))
    moves = [[], []]
    for side, sign in sides:
        for i, (w, k) in enumerate(gather_messages(half)[side]):
            src, dst = w_v.at[w, slot[-k * sign]], w_v.at[w, slot[-(k + 1) * sign]]
            moves[side].append(fold.send(src, dst, wh, ws_sem.at[side, i], wr_sem.at[side, i], ring.dev(sign)))
    for side, _ in sides:
        start(moves[side][0].copies[0])

    def forward(i):
        with jax.named_scope(f'fwd{i}'):
            for side, sign in sides:
                moves[side][i].wait_recv()
                if i + 2 < len(moves[side]):
                    start(moves[side][i + 2])
                w, k = gather_messages(half)[side][i]
                fold.unfold(w_v.at[w, slot[-(k + 1) * sign]], wh)

    own_ids.wait()
    with jax.named_scope('ids_wait'):
        swap_ids.wait_recv()
    ids = jnp.concatenate([ids_v[0], ids_v[1]], axis=1).astype(F32)
    ids_t = jnp.transpose(jnp.broadcast_to(ids, (LANES, tp)))
    seen = jnp.zeros((1, tp), F32)
    total = jnp.zeros((1, tp), F32)
    for i in range(tp // LANES):
        earlier = iota((LANES, tp), 0) + i * LANES < iota((LANES, tp), 1)
        tri = jnp.where(earlier, 1.0, 0.0)
        tri_v[i * LANES:(i + 1) * LANES, :] = tri.astype(BF16)
        same = jnp.where(ids_t[i * LANES:(i + 1) * LANES, 0:1] == ids, 1.0, 0.0)
        seen = jnp.maximum(seen, jnp.max(same * tri, axis=0, keepdims=True))
        total = total + jnp.sum(same, axis=0, keepdims=True)
    row = iota((n, 1), 0)
    owner = jnp.where(row < nz, 2 * row + c, 2 * (row - nz) + 1 - c)
    base = (owner * vocab).astype(F32)
    member = jnp.where((seen < 0.5) & (ids >= base) & (ids < base + vocab), 1.0, 0.0)
    multi = jnp.where(total > 1.5, 1.0, 0.0)
    several, single = member * multi, member * (1.0 - multi)
    both = jnp.concatenate([several, single], axis=0).astype(BF16)
    rank = jnp.dot(both, tri_v[...], preferred_element_type=F32)
    n_several = jnp.sum(several, axis=1, keepdims=True)
    count = n_several + jnp.sum(single, axis=1, keepdims=True)
    rank = jnp.where(several > 0.5, rank[:n], n_several + rank[n:])
    over = jnp.maximum(jnp.where(count > CAP, 1.0, 0.0), jnp.where(n_several > MULTI, 1.0, 0.0))
    over = jnp.max(over, axis=0, keepdims=True)
    for k in range(nz):
        hit = (rank[k:k + 1, :] == iota((CAP, 1), 0).astype(F32)) & (member[k:k + 1, :] > 0.5)
        col = jnp.max(jnp.where(hit, ids, -1.0), axis=1, keepdims=True)
        col_v[k * CAP:(k + 1) * CAP, :] = jnp.broadcast_to(col, (CAP, LANES))
    cols_t = jnp.transpose(col_v[...])
    lane = iota((8, LANES), 1)
    per = LANES // CAP
    for k in range(nz):
        at = (k // per) * LANES
        tile = cols_t[0:8, at:at + LANES]
        if k % per:
            tile = pltpu.roll(tile, LANES - (k % per) * CAP, 1)
        req_s[k] = jnp.where(lane < CAP, tile, over)
    asks = []
    for d in range(1, nz):
        asks.append(start(remote(req_s.at[ring.chip(d)], req_r.at[z], qs_sem.at[d], qr_sem.at[d], ring.dev(d))))
    for side, _ in sides:
        start(moves[side][0].copies[1])
        start(moves[side][1])
    swap_grad = start(remote(grad_ref, gn_v.at[1, c], ps_sem.at[1], pr_sem.at[1], ring.sibling))
    req_r[z] = req_s[z]
    for t in range(2):
        pick_v[t] = jnp.where(col_v[:, 0:1] == ids[:, t * tl:(t + 1) * tl], 1.0, 0.0).astype(BF16)

    with jax.named_scope('asks_wait'):
        for copy in asks:
            copy.wait_recv()
    flag = req_r[0]
    for k in range(1, nz):
        flag = jnp.maximum(flag, req_r[k])
    flag_ref[0, 0] = jnp.max(jnp.where(lane < CAP, 0.0, flag))
    tiles = []
    for p in range(nz // per):
        tile = req_r[p * per]
        for j in range(1, per):
            tile = jnp.where(lane < j * CAP, tile, pltpu.roll(req_r[p * per + j], j * CAP, 1))
        tiles.append(tile)
    names = jnp.concatenate(tiles, axis=1) - (ring.me * vocab).astype(F32)
    name_v[...] = jnp.transpose(jnp.broadcast_to(names[0:1, :], (LANES, slots)))
    found_v[...] = jnp.zeros_like(found_v)

    def find(i, carry):
        load_emb(i).wait()
        hot = jnp.where(name_v[:, 0:1] == (iota((1, step), 1) + i * step).astype(F32), 1.0, 0.0).astype(BF16)
        found_v[...] = found_v[...] + contract(hot, emb_v[lax.rem(i, 2)], 1, 1)

        @pl.when(i + 2 < vocab // step)
        def _():
            load_emb(i + 2).start()

        return carry

    with jax.named_scope('find'):
        lax.fori_loop(0, vocab // step, find, 0)
    for k in range(nz):
        fold.store(xs_v.at[k], found_v[k * CAP:(k + 1) * CAP, :].astype(BF16), xh)
    gives = []
    for d in range(1, nz):
        gives.append(start(fold.send(xs_v.at[ring.chip(d)], xr_v.at[z], xh, xs_sem.at[d], xr_sem.at[d], ring.dev(d))))
    xr_v[z] = xs_v[z]
    forward(0)
    forward(1)

    with jax.named_scope('gives_wait'):
        for copy in gives:
            copy.wait_recv()
    for k in range(nz):
        fold.unfold(xr_v.at[k], xh)
    got = xr_v[...].reshape(slots, fold.dp)[:, :dm]
    for t in range(2):
        x_v[t] = contract(got, pick_v[t], 0, 0).astype(BF16)
    swap_x = remote(x_v, xq_v, ps_sem.at[2], pr_sem.at[2], ring.sibling)
    swap_x.start()
    load_grad.wait()
    swap_grad.wait_recv()
    with jax.named_scope('swapx_wait'):
        swap_x.wait_send()
        swap_x.wait_recv()

    def lanes(b):
        return pl.ds(pl.multiple_of(b * LANES, LANES), LANES)

    def norm(i, carry):
        t, at = i // (tl // LANES), lanes(lax.rem(i, tl // LANES))
        xb = x_v[t, :, at] + xq_v[t, :, at]
        x_v[t, :, at] = xb
        xf = xb.astype(F32)
        inv = lax.rsqrt(jnp.mean(xf * xf, axis=0, keepdims=True) + EPS)
        gn_v[0, t, :, at] = (xf * inv * gain_v[:dm, :]).astype(BF16)
        return carry

    lax.fori_loop(0, tp // LANES, norm, 0)

    def hidden(lo, hi):
        def body(i, carry):
            s, t = lo + i // 2, lax.rem(i, 2)
            u = jnp.dot(w_v[0, s, :, :dm], gn_v[0, t], preferred_element_type=F32).astype(BF16).astype(F32)
            dh = jnp.dot(w_v[1, s, :, :dm], gn_v[1, t], preferred_element_type=F32)
            act, slope = gelu_pair(u)
            at = pl.ds(pl.multiple_of(s * fl, fl), fl)
            hd_v[1, t, at, :] = act.astype(BF16)
            hd_v[0, t, at, :] = (dh * slope).astype(BF16)
            return carry

        with jax.named_scope(f'hid{lo}'):
            lax.fori_loop(0, 2 * (hi - lo), body, 0)

    def grad_w(w, s):
        at = pl.ds(pl.multiple_of(s * fl, fl), fl)
        return contract(hd_v[w, 0, at, :], gn_v[w, 0], 1, 1) + contract(hd_v[w, 1, at, :], gn_v[w, 1], 1, 1)

    orders = scatter_messages(half)
    sends = [[], []]
    for side, sign in sides:
        for i in range(len(orders[0])):
            src = st_v.at[side, i] if i < 2 else rb_v.at[side, i - 2]
            dst = rb_v.at[side, i]
            sends[side].append(fold.send(src, dst, wh, ss_sem.at[side, i], sr_sem.at[side, i], ring.dev(sign)))

    def scatter(i):
        with jax.named_scope(f'scat{i}'):
            (w0, k0), (_, k1) = orders[0][i], orders[1][i]
            if i >= 2:
                for side, _ in sides:
                    sends[side][i - 2].wait_recv()

            def body(side, carry):
                w = w0 + side * (1 - 2 * w0)
                part = grad_w(w, slot[k0] + side * (slot[k1] - slot[k0]))
                if i < 2:
                    fold.store(st_v.at[side, i], part, wh)
                else:
                    fold.add(rb_v.at[side, i - 2], part, wh)
                return carry

            lax.fori_loop(0, 2, body, 0)
            for side, _ in sides:
                start(sends[side][i])

    last = len(moves[0]) - 1
    hidden(nz - 1, nz)
    hidden(nz - 3, nz - 1)
    for k in range(2, half):
        forward(2 * k - 2)
        forward(2 * k - 1)
        hidden(nz - 1 - 2 * k, nz + 1 - 2 * k)
    forward(last)
    hidden(0, 1)
    scatter(0)
    scatter(1)

    wide = 2 * LANES

    def through(w, t, dst):
        def body(b, carry):
            at = pl.ds(pl.multiple_of(b * wide, wide), wide)
            left = w_v[w, :, :, at].reshape(nz * fl, wide)
            dst[at, :] = contract(left, hd_v[w_of_hd[w], t], 0, 0)
            return carry

        lax.fori_loop(0, fold.dp // wide, body, 0)

    w_of_hd = (0, 1)
    with jax.named_scope('thru'):
        through(0, 1 - c, snd_v)
    body_rows = pl.ds(0, dm)
    swap_dn = remote(snd_v.at[body_rows], dnr_v, ps_sem.at[3], pr_sem.at[3], ring.sibling)
    swap_dn.start()
    through(0, c, own_v)
    with jax.named_scope('swapdn_wait'):
        swap_dn.wait_send()
        swap_dn.wait_recv()

    def dx_block(b, carry):
        at = lanes(b)
        xf = x_v[c, :, at].astype(F32)
        inv = lax.rsqrt(jnp.mean(xf * xf, axis=0, keepdims=True) + EPS)
        q = (own_v[:dm, at] + dnr_v[:, at]) * gain_v[:dm, :]
        dot = jnp.mean(xf * q, axis=0, keepdims=True)
        dxn = inv * q - xf * (inv * inv * inv * dot)
        dx_v[c, :, at] = (gn_v[1, c, :, at].astype(F32) + dxn).astype(BF16)
        return carry

    lax.fori_loop(0, tl // LANES, dx_block, 0)
    swap_dx = start(remote(dx_v.at[c], dx_v.at[c], ps_sem.at[4], pr_sem.at[4], ring.sibling))
    through(1, 1 - c, snd_v)
    swap_y = start(remote(snd_v.at[body_rows], yr_v, ps_sem.at[5], pr_sem.at[5], ring.sibling))
    with jax.named_scope('swapdx_wait'):
        swap_dx.wait_recv()

    def pack(k, carry):
        at = pl.ds(pl.multiple_of(k * CAP, CAP), CAP)
        rows = contract(pick_v[0, at, :], dx_v[0], 1, 1) + contract(pick_v[1, at, :], dx_v[1], 1, 1)
        fold.store(es_v.at[k], rows[:MULTI], eh)
        fold.store(eb_v.at[k], rows[MULTI:].astype(BF16), bh)
        return carry

    lax.fori_loop(0, nz, pack, 0)
    backs = []
    for d in range(1, nz):
        kk, to = ring.chip(d), ring.dev(d)
        backs.append(start(fold.send(es_v.at[kk], er_v.at[z], eh, es_sem.at[0, d], er_sem.at[0, d], to)))
        backs.append(start(fold.send(eb_v.at[kk], eq_v.at[z], bh, es_sem.at[1, d], er_sem.at[1, d], to)))
    er_v[z] = es_v[z]
    eq_v[z] = eb_v[z]
    scatter(2)
    through(1, c, own_v)
    scatter(3)
    with jax.named_scope('swapy_wait'):
        swap_y.wait_recv()

    def out_block(b, carry):
        at = lanes(b)
        out_v[:, at] = (x_v[c, :, at].astype(F32) + (own_v[:dm, at] + yr_v[:, at])).astype(BF16)
        return carry

    lax.fori_loop(0, tl // LANES, out_block, 0)
    keeps = [pltpu.make_async_copy(out_v, out_ref, out_sem.at[0])]
    keeps[0].start()
    last = len(orders[0])
    for i in range(4, last):
        scatter(i)

    with jax.named_scope('backs_wait'):
        for copy in backs:
            copy.wait_recv()
    lots, rest = nz * MULTI, CAP - MULTI

    def spread(k, carry):
        fold.unfold(er_v.at[k], eh)
        fold.unfold(eq_v.at[k], bh)
        rows = er_v[k, :, :dm]
        head = name_v[pl.ds(pl.multiple_of(k * CAP, CAP), MULTI), :]
        for p in range(3):
            at = pl.ds(pl.multiple_of(p * lots + k * MULTI, MULTI), MULTI)
            piece = rows.astype(BF16)
            rows_v[at, :] = piece
            names_ref[at, :] = head
            rows = rows - piece.astype(F32)
        at = pl.ds(pl.multiple_of(3 * lots + k * rest, 16), rest)
        rows_v[at, :] = eq_v[k, :, :dm]
        names_ref[at, :] = name_v[pl.ds(pl.multiple_of(k * CAP + MULTI, 16), rest), :]
        return carry

    lax.fori_loop(0, nz, spread, 0)
    keeps.append(pltpu.make_async_copy(rows_v, rows_ref, out_sem.at[1]))
    keeps[1].start()

    for w in range(2):
        a, b = (last - 1, last - 2) if w == 0 else (last - 2, last - 1)
        part = grad_w(w, mine)
        with jax.named_scope(f'fin{w}'):
            sends[0][a].wait_recv()
            sends[1][b].wait_recv()
        rb_v[0, a] = rb_v[0, a] + rb_v[1, b]
        fold.unfold(rb_v.at[0, a], wh)
        (dup_ref, ddown_ref)[w][...] = rb_v[0, a, :, :dm] + part
    for copy in sent:
        copy.wait_send()
    for copy in keeps:
        copy.wait()


def step(n, ids, emb_t, up, down, grad_t, gain):
    nz = n // 2
    dm, vocab = emb_t.shape
    tl, fl = ids.shape[1], up.shape[0]
    tp = 2 * tl
    dp = Fold(dm).dp
    slots = nz * CAP
    parts = slots + 2 * nz * MULTI
    hops = nz - 1
    vmem, hbm = pl.BlockSpec(memory_space=pltpu.VMEM), pl.BlockSpec(memory_space=pl.ANY)
    dma = pltpu.SemaphoreType.DMA
    tokens = pltpu.VMEM((2, dm, tl), BF16)
    return pl.pallas_call(
        functools.partial(step_kernel, n),
        name='step',
        out_shape=(
            jax.ShapeDtypeStruct((dm, tl), BF16),
            jax.ShapeDtypeStruct((fl, dm), F32),
            jax.ShapeDtypeStruct((fl, dm), F32),
            jax.ShapeDtypeStruct((parts, dm), BF16),
            jax.ShapeDtypeStruct((parts, LANES), F32),
            jax.ShapeDtypeStruct((1, 1), F32),
        ),
        in_specs=[vmem, hbm, vmem, vmem, hbm, vmem],
        out_specs=(hbm, vmem, vmem, hbm, vmem, pl.BlockSpec(memory_space=pltpu.SMEM)),
        scratch_shapes=[
            pltpu.VMEM((2, nz, fl, dp), BF16),
            pltpu.VMEM((2, 2, dm, tl), BF16),
            tokens, tokens,
            pltpu.VMEM((2, 2, nz * fl, tl), BF16),
            pltpu.VMEM((2, 2, fl, dp), F32),
            pltpu.VMEM((2, hops, fl, dp), F32),
            pltpu.VMEM((dp, tl), F32),
            pltpu.VMEM((dp, tl), F32),
            pltpu.VMEM((dm, tl), F32),
            pltpu.VMEM((dm, tl), F32),
            tokens,
            pltpu.VMEM((nz, MULTI, dp), F32),
            pltpu.VMEM((nz, MULTI, dp), F32),
            pltpu.VMEM((nz, CAP - MULTI, dp), BF16),
            pltpu.VMEM((nz, CAP - MULTI, dp), BF16),
            pltpu.VMEM((nz, CAP, dp), BF16),
            pltpu.VMEM((nz, CAP, dp), BF16),
            pltpu.VMEM((2, slots, tl), BF16),
            pltpu.VMEM((tp, tp), BF16),
            pltpu.VMEM((2, 1, tl), jnp.int32),
            pltpu.VMEM((slots, LANES), F32),
            pltpu.VMEM((slots, LANES), F32),
            pltpu.VMEM((nz, 8, LANES), F32),
            pltpu.VMEM((nz, 8, LANES), F32),
            pltpu.VMEM((2, dm, 512), BF16),
            pltpu.VMEM((slots, dm), F32),
            pltpu.VMEM((dm, tl), BF16),
            pltpu.VMEM((parts, dm), BF16),
            pltpu.VMEM((1, dp), F32),
            pltpu.VMEM((dp, LANES), F32),
            dma((2,)), dma((2,)), dma((2, hops, 2)), dma((2, hops, 2)), dma((6,)), dma((6,)),
            dma((nz,)), dma((nz,)), dma((nz, 2)), dma((nz, 2)),
            dma((2, hops, 2)), dma((2, hops, 2)), dma((2, nz, 2)), dma((2, nz, 2)), dma((2,)),
        ],
        compiler_params=pltpu.CompilerParams(
            collective_id=0, has_side_effects=True, vmem_limit_bytes=VMEM_LIMIT
        ),
    )(ids, emb_t, up, down, grad_t, gain)


def place_kernel(names_ref, rows_ref, out_ref, up_ref, down_ref, emb_out, out_out, up_out, down_out):
    block = emb_out.shape[1]
    here = names_ref[:, 0:1] == (iota((1, block), 1) + pl.program_id(0) * block).astype(F32)
    hot = jnp.where(here, 1.0, 0.0).astype(BF16)
    emb_out[...] = contract(rows_ref[...], hot, 0, 0)
    out_out[...] = out_ref[...]
    up_out[...] = up_ref[...]
    down_out[...] = down_ref[...]


def place(vocab, names, rows, out, d_up, d_down):
    parts, dm = rows.shape
    grid = 4
    passing = [pl.BlockSpec((a.shape[0] // grid, a.shape[1]), lambda i: (i, 0)) for a in (out, d_up, d_down)]
    return pl.pallas_call(
        place_kernel,
        name='place',
        grid=(grid,),
        out_shape=(jax.ShapeDtypeStruct((dm, vocab), F32),)
        + tuple(jax.ShapeDtypeStruct(a.shape, a.dtype) for a in (out, d_up, d_down)),
        in_specs=[pl.BlockSpec((parts, LANES), lambda i: (0, 0)), pl.BlockSpec((parts, dm), lambda i: (0, 0))] + passing,
        out_specs=(pl.BlockSpec((dm, vocab // grid), lambda i: (0, i)),) + tuple(passing),
        compiler_params=pltpu.CompilerParams(vmem_limit_bytes=48_000_000),
    )(names, rows, out, d_up, d_down)


def swap_kernel(n, src_ref, dst_ref, keep_sem, send_sem, recv_sem):
    me = lax.axis_index('tensor')
    sem = pltpu.get_barrier_semaphore()
    for d in range(1, n):
        pl.semaphore_signal(sem, inc=1, device_id={'tensor': lax.rem(me + d, n)}, device_id_type=MESH)
    pl.semaphore_wait(sem, n - 1)
    keep = pltpu.make_async_copy(src_ref.at[me], dst_ref.at[me], keep_sem)
    keep.start()
    copies = []
    for d in range(1, n):
        to = lax.rem(me + d, n)
        copies.append(remote(src_ref.at[to], dst_ref.at[me], send_sem.at[d], recv_sem.at[d], {'tensor': to}))
        copies[-1].start()
    for copy in copies:
        copy.wait()
    keep.wait()


def swap_blocks(n, blocks, collective_id):
    hbm = pl.BlockSpec(memory_space=pl.ANY)
    return pl.pallas_call(
        functools.partial(swap_kernel, n),
        name='swap_blocks',
        out_shape=jax.ShapeDtypeStruct(blocks.shape, blocks.dtype),
        in_specs=[hbm],
        out_specs=hbm,
        scratch_shapes=[pltpu.SemaphoreType.DMA, pltpu.SemaphoreType.DMA((n,)), pltpu.SemaphoreType.DMA((n,))],
        compiler_params=pltpu.CompilerParams(collective_id=collective_id, has_side_effects=True),
    )(blocks)


def all_blocks(n, block, collective_id):
    return swap_blocks(n, jnp.broadcast_to(block[None], (n,) + block.shape), collective_id)


def rms_norm(x_rows, gain_f):
    inv_rms = lax.rsqrt(jnp.mean(x_rows * x_rows, axis=-1, keepdims=True) + EPS)
    return x_rows * inv_rms * gain_f


def dense_step(n, ids, emb, norm_gain, up, down, grad_out):
    vocab, dm = emb.shape
    fl = up.shape[0]
    base = (lax.axis_index('tensor') * vocab).astype(F32)
    ids_all = all_blocks(n, jnp.broadcast_to(ids.astype(F32), (8, ids.shape[1])), 1)[:, 0]
    hot = (iota((ids_all.size, vocab), 1).astype(F32) == ids_all.reshape(-1, 1) - base).astype(BF16)
    part = jnp.dot(hot, emb, preferred_element_type=F32).astype(BF16)
    x_f = jnp.sum(swap_blocks(n, part.reshape(n, -1, dm), 2).astype(F32), axis=0)
    ws = all_blocks(n, jnp.stack([up, down]), 3)
    up_all, down_all = ws[:, 0].reshape(-1, dm), ws[:, 1].reshape(-1, dm)
    normed_f, norm_back = jax.vjp(lambda x_in: rms_norm(x_in, norm_gain.astype(F32)), x_f)
    normed = normed_f.astype(BF16)
    pre_act = contract(normed, up_all, 1, 1).astype(BF16).astype(F32)
    act_f, slope = gelu_pair(pre_act)
    hidden = act_f.astype(BF16)
    d_pre = (contract(grad_out, down_all, 1, 1) * slope).astype(BF16)
    y = jnp.dot(hidden, down_all, preferred_element_type=F32)
    out = (x_f + y).astype(BF16)
    d_norm = jnp.dot(d_pre, up_all, preferred_element_type=F32)
    dx = (grad_out.astype(F32) + norm_back(d_norm)[0]).astype(BF16)
    d_w = jnp.stack([contract(d_pre, normed, 0, 0), contract(hidden, grad_out, 0, 0)]).reshape(2, n, fl, dm)
    d_w = jnp.sum(swap_blocks(n, jnp.moveaxis(d_w, 1, 0), 4), axis=0)
    dx_all = all_blocks(n, dx, 5).reshape(-1, dm)
    hot_t = (iota((vocab, ids_all.size), 0).astype(F32) == ids_all.reshape(1, -1) - base).astype(BF16)
    d_emb = jnp.dot(hot_t, dx_all, preferred_element_type=F32)
    return d_emb.T, out.T, d_w[0], d_w[1]


def solution(mesh):
    n = mesh.shape['tensor']
    tok_spec = P(('data', 'tensor'))
    row_spec = P(('data', 'tensor'), None)

    def local_step(token_ids, emb_shard, norm_gain, w_up, w_down, grad_out):
        vocab, dm = emb_shard.shape
        ids, gain, up = token_ids[None, :], norm_gain[None, :], w_up.T
        out, d_up, d_down, rows, names, flag = step(n, ids, emb_shard.T, up, w_down, grad_out.T, gain)
        placed = place(vocab, names, rows, out, d_up, d_down)

        def again(state):
            return (jnp.zeros((), F32),) + dense_step(n, ids, emb_shard, norm_gain, up, w_down, grad_out)

        state = lax.while_loop(lambda state: state[0] > 0.5, again, (flag[0, 0],) + tuple(placed))
        _, d_emb, out, d_up, d_down = state
        return out.T, d_emb.T, d_up.T, d_down

    return jax.shard_map(
        local_step,
        mesh=mesh,
        in_specs=(tok_spec, P('tensor', None), P(None), P(None, 'tensor'), P('tensor', None), row_spec),
        out_specs=(row_spec, row_spec, P('data', 'tensor'), row_spec),
        check_vma=False,
    )
```

```python
import functools

import jax
import jax.numpy as jnp
from jax import lax
from jax.experimental import pallas as pl
from jax.experimental.pallas import tpu as pltpu
from jax.sharding import PartitionSpec as P

EPS = 1e-6
CAP = 64
MULTI = 16
BHEAD = 32
LANES = 128
MESH = pl.DeviceIdType.MESH
VMEM_LIMIT = 67_000_000
F32 = jnp.float32
BF16 = jnp.bfloat16
SQRT_2_PI = 0.7978845608028654
CUBIC = 0.044715


def contract(left_op, right_op, left_dim, right_dim):
    dims = (((left_dim,), (right_dim,)), ((), ()))
    return lax.dot_general(left_op, right_op, dims, preferred_element_type=F32)


def iota(shape, dim):
    return lax.broadcasted_iota(jnp.int32, shape, dim)


def gelu_pair(u):
    t = jnp.tanh(SQRT_2_PI * (u + CUBIC * (u * u * u)))
    cdf = 0.5 * (1.0 + t)
    slope = cdf + u * (0.5 * (1.0 - t * t)) * (SQRT_2_PI * (1.0 + (3.0 * CUBIC) * (u * u)))
    return u * cdf, slope


class Ring:
    def __init__(self, n, groups):
        self.n, self.nz, self.half, self.groups = n, n // 2, n // 4, groups
        self.me = lax.axis_index('tensor')
        self.g = lax.axis_index('data')
        self.c = lax.rem(self.me, 2)
        self.z = self.me // 2

    def chip(self, k):
        return lax.rem(self.z + (k + self.nz) % self.nz, self.nz)

    def dev(self, k):
        return {'tensor': 2 * self.chip(k) + self.c}

    def twin(self, e):
        return {'data': lax.rem(self.g + e, self.groups), 'tensor': self.me}

    @property
    def sibling(self):
        return {'tensor': self.me + 1 - 2 * self.c}

    def barrier(self):
        sem = pltpu.get_barrier_semaphore()
        for k in range(1, self.nz):
            pl.semaphore_signal(sem, inc=1, device_id=self.dev(k), device_id_type=MESH)
        pl.semaphore_signal(sem, inc=1, device_id=self.sibling, device_id_type=MESH)
        for e in range(1, self.groups):
            pl.semaphore_signal(sem, inc=1, device_id=self.twin(e), device_id_type=MESH)
        pl.semaphore_wait(sem, self.nz + self.groups - 1)


def slot_of(nz):
    half = nz // 2
    order = [half] + [s * k for k in range(half - 1, 0, -1) for s in (1, -1)] + [0]
    table = {k: i for i, k in enumerate(order)}
    table[-half] = table[half]
    return table


def gather_messages(half):
    right = [(w, k) for k in range(half) for w in (0, 1) if w == 0 or k < half - 1]
    return right, [(1 - w, k) for w, k in right]


BLOCK = 16


def shared_blocks(groups):
    each = max(1, 12 // groups)
    assert groups * each % 2 == 0
    return each, BLOCK * (-(-groups * each // 2))


def scatter_messages(half):
    right = [(0, half)]
    for k in range(half - 1, 0, -1):
        right += [(1, k), (0, k)]
    return right, [(1 - w, -k) for w, k in right]


def remote(src, dst, send_sem, recv_sem, device):
    return pltpu.make_async_remote_copy(
        src_ref=src, dst_ref=dst, send_sem=send_sem, recv_sem=recv_sem, device_id=device, device_id_type=MESH
    )


class Fold:
    def __init__(self, dm):
        self.dm = dm
        self.lo = dm // LANES * LANES
        self.dp = self.lo + LANES
        assert 2 * (dm - self.lo) == LANES

    def tail(self, value, h):
        low = value.shape[0] - h
        return jnp.concatenate([value[:low, self.lo:self.dm], value[h:, self.lo:self.dm]], axis=1)

    def store(self, ref, value, h):
        low = value.shape[0] - h
        ref[:, :self.lo] = value[:, :self.lo]
        ref[:low, self.lo:] = self.tail(value, h)
        if low < h:
            ref[low:h, self.lo:self.dm] = value[low:h, self.lo:self.dm]

    def add(self, ref, value, h):
        low = value.shape[0] - h
        ref[:, :self.lo] = ref[:, :self.lo] + value[:, :self.lo]
        ref[:low, self.lo:] = ref[:low, self.lo:] + self.tail(value, h)

    def unfold(self, ref, h):
        low = ref.shape[0] - h
        ref[h:, self.lo:self.dm] = ref[:low, self.dm:self.dp]

    def send(self, src, dst, h, send_sem, recv_sem, device):
        return FoldCopy(self, src, dst, h, send_sem, recv_sem, device)


class FoldCopy:
    def __init__(self, fold, src, dst, h, send_sem, recv_sem, device):
        parts = ((pl.ds(0, h), pl.ds(0, fold.dp)), (pl.ds(h, src.shape[0] - h), pl.ds(0, fold.lo)))
        self.copies = [
            remote(src.at[r, l], dst.at[r, l], send_sem.at[i], recv_sem.at[i], device)
            for i, (r, l) in enumerate(parts)
        ]

    def start(self):
        for copy in self.copies:
            copy.start()

    def wait_recv(self):
        for copy in self.copies:
            copy.wait_recv()

    def wait_send(self):
        for copy in self.copies:
            copy.wait_send()


def step_kernel(
    n, groups, ids_ref, emb_ref, up_ref, down_ref, grad_ref, gain_ref,
    out_ref, dup_ref, ddown_ref, rows_ref, names_ref, flag_ref,
    w_v, gn_v, x_v, xq_v, hd_v, st_v, rb_v, snd_v, own_v, dnr_v, yr_v, dx_v, es_v, er_v, eb_v, eq_v, xs_v, xr_v,
    pick_v, tri_v, ids_v, col_v, name_v, req_s, req_r, emb_v, found_v, out_v, rows_v, row_v, gain_v,
    ld_sem, emb_sem, ws_sem, wr_sem, bs_sem, br_sem, ts_sem, tr_sem, ps_sem, pr_sem, qs_sem, qr_sem, xs_sem, xr_sem,
    ss_sem, sr_sem, es_sem, er_sem, out_sem,
):
    ring = Ring(n, groups)
    nz, half, c, z = ring.nz, ring.half, ring.c, ring.z
    slot = slot_of(nz)
    each, shared = shared_blocks(groups)
    dm, vocab = emb_ref.shape
    fl = up_ref.shape[0]
    tl = ids_ref.shape[1]
    tp = 2 * tl
    slots = nz * CAP
    fold = Fold(dm)
    wh, xh, eh, bh = fl // 2, CAP // 2, MULTI // 2, BHEAD
    gh = (fl - shared) // 2
    ring_rows = pl.ds(shared, fl - shared)
    step = emb_v.shape[2]
    sides = ((0, 1), (1, -1))
    sent = []

    load_grad = pltpu.make_async_copy(grad_ref, gn_v.at[1, c], ld_sem.at[0])
    load_grad.start()
    own_ids = pltpu.make_async_copy(ids_ref, ids_v.at[c], ld_sem.at[1])
    own_ids.start()

    def load_emb(i):
        b = lax.rem(i, 2)
        at = pl.ds(pl.multiple_of(i * step, step), step)
        return pltpu.make_async_copy(emb_ref.at[:, at], emb_v.at[b], emb_sem.at[b])

    for i in range(2):
        load_emb(i).start()
    mine = slot[0]
    for w, ref in enumerate((up_ref, down_ref)):
        w_v[w, mine, :, :dm] = ref[...]
        w_v[w, mine, shared:shared + gh, dm:] = ref[shared + gh:, fold.lo:]
    row_v[...] = jnp.zeros_like(row_v)
    row_v[:, :dm] = gain_ref[...].astype(F32).reshape(1, dm)
    gain_v[...] = jnp.transpose(jnp.broadcast_to(row_v[...], (LANES, fold.dp)))
    with jax.named_scope('barrier'):
        ring.barrier()

    def start(copy):
        copy.start()
        sent.append(copy)
        return copy

    blocks = []
    for j in range(each):
        b = ring.g * each + j
        blocks.append((lax.rem(b, 2), pl.ds(pl.multiple_of(BLOCK * (b // 2), BLOCK), BLOCK)))

    def hops(k):
        return [
            remote(
                w_v.at[blocks[j][0], slot[-k * sign], blocks[j][1]],
                w_v.at[blocks[j][0], slot[-(k + 1) * sign], blocks[j][1]],
                bs_sem.at[side, j, k], br_sem.at[side, j, k], ring.dev(sign),
            )
            for j in range(each) for side, sign in sides if k < half - 1 or side == j % 2
        ]

    stages = ((nz - 3, nz), (nz - 5, nz - 3), (0, nz - 5))

    def twins(stage):
        lo, hi = stages[stage]
        return [
            remote(
                w_v.at[w, pl.ds(lo, hi - lo), at], w_v.at[w, pl.ds(lo, hi - lo), at],
                ts_sem.at[stage, j, e], tr_sem.at[stage, j, e], ring.twin(e),
            )
            for j, (w, at) in enumerate(blocks) for e in range(1, groups)
        ]

    block_moves = [hops(k) for k in range(half)]
    twin_moves = [twins(stage) for stage in range(len(stages))]

    def relay(k, stage):
        with jax.named_scope(f'relay{k}'):
            for copy in block_moves[k]:
                copy.wait_recv()
            if k + 1 < half:
                for copy in block_moves[k + 1]:
                    start(copy)
            if stage is not None:
                for copy in twin_moves[stage]:
                    start(copy)

    def from_twins(stage):
        with jax.named_scope(f'twins{stage}'):
            for copy in twin_moves[stage]:
                copy.wait_recv()

    for copy in block_moves[0]:
        start(copy)
    swap_ids = start(remote(ids_ref, ids_v.at[c], ps_sem.at[0], pr_sem.at[0], ring.sibling))
    moves = [[], []]
    for side, sign in sides:
        for i, (w, k) in enumerate(gather_messages(half)[side]):
            src, dst = w_v.at[w, slot[-k * sign], ring_rows], w_v.at[w, slot[-(k + 1) * sign], ring_rows]
            moves[side].append(fold.send(src, dst, gh, ws_sem.at[side, i], wr_sem.at[side, i], ring.dev(sign)))
    for side, _ in sides:
        start(moves[side][0].copies[0])

    def forward(i):
        with jax.named_scope(f'fwd{i}'):
            for side, sign in sides:
                moves[side][i].wait_recv()
                if i + 2 < len(moves[side]):
                    start(moves[side][i + 2])
                w, k = gather_messages(half)[side][i]
                fold.unfold(w_v.at[w, slot[-(k + 1) * sign], ring_rows], gh)

    own_ids.wait()
    with jax.named_scope('ids_wait'):
        swap_ids.wait_recv()
    ids = jnp.concatenate([ids_v[0], ids_v[1]], axis=1).astype(F32)
    ids_t = jnp.transpose(jnp.broadcast_to(ids, (LANES, tp)))
    seen = jnp.zeros((1, tp), F32)
    total = jnp.zeros((1, tp), F32)
    for i in range(tp // LANES):
        earlier = iota((LANES, tp), 0) + i * LANES < iota((LANES, tp), 1)
        tri = jnp.where(earlier, 1.0, 0.0)
        tri_v[i * LANES:(i + 1) * LANES, :] = tri.astype(BF16)
        same = jnp.where(ids_t[i * LANES:(i + 1) * LANES, 0:1] == ids, 1.0, 0.0)
        seen = jnp.maximum(seen, jnp.max(same * tri, axis=0, keepdims=True))
        total = total + jnp.sum(same, axis=0, keepdims=True)
    row = iota((n, 1), 0)
    owner = jnp.where(row < nz, 2 * row + c, 2 * (row - nz) + 1 - c)
    base = (owner * vocab).astype(F32)
    member = jnp.where((seen < 0.5) & (ids >= base) & (ids < base + vocab), 1.0, 0.0)
    multi = jnp.where(total > 1.5, 1.0, 0.0)
    several, single = member * multi, member * (1.0 - multi)
    both = jnp.concatenate([several, single], axis=0).astype(BF16)
    rank = jnp.dot(both, tri_v[...], preferred_element_type=F32)
    n_several = jnp.sum(several, axis=1, keepdims=True)
    count = n_several + jnp.sum(single, axis=1, keepdims=True)
    rank = jnp.where(several > 0.5, rank[:n], n_several + rank[n:])
    over = jnp.maximum(jnp.where(count > CAP, 1.0, 0.0), jnp.where(n_several > MULTI, 1.0, 0.0))
    over = jnp.max(over, axis=0, keepdims=True)
    for k in range(nz):
        hit = (rank[k:k + 1, :] == iota((CAP, 1), 0).astype(F32)) & (member[k:k + 1, :] > 0.5)
        col = jnp.max(jnp.where(hit, ids, -1.0), axis=1, keepdims=True)
        col_v[k * CAP:(k + 1) * CAP, :] = jnp.broadcast_to(col, (CAP, LANES))
    cols_t = jnp.transpose(col_v[...])
    lane = iota((8, LANES), 1)
    per = LANES // CAP
    for k in range(nz):
        at = (k // per) * LANES
        tile = cols_t[0:8, at:at + LANES]
        if k % per:
            tile = pltpu.roll(tile, LANES - (k % per) * CAP, 1)
        req_s[k] = jnp.where(lane < CAP, tile, over)
    asks = []
    for d in range(1, nz):
        asks.append(start(remote(req_s.at[ring.chip(d)], req_r.at[z], qs_sem.at[d], qr_sem.at[d], ring.dev(d))))
    relay(0, 0)
    for side, _ in sides:
        start(moves[side][0].copies[1])
        start(moves[side][1])
    swap_grad = start(remote(grad_ref, gn_v.at[1, c], ps_sem.at[1], pr_sem.at[1], ring.sibling))
    req_r[z] = req_s[z]
    for t in range(2):
        pick_v[t] = jnp.where(col_v[:, 0:1] == ids[:, t * tl:(t + 1) * tl], 1.0, 0.0).astype(BF16)

    with jax.named_scope('asks_wait'):
        for copy in asks:
            copy.wait_recv()
    relay(1, 1)
    flag = req_r[0]
    for k in range(1, nz):
        flag = jnp.maximum(flag, req_r[k])
    flag_ref[0, 0] = jnp.max(jnp.where(lane < CAP, 0.0, flag))
    tiles = []
    for p in range(nz // per):
        tile = req_r[p * per]
        for j in range(1, per):
            tile = jnp.where(lane < j * CAP, tile, pltpu.roll(req_r[p * per + j], j * CAP, 1))
        tiles.append(tile)
    names = jnp.concatenate(tiles, axis=1) - (ring.me * vocab).astype(F32)
    name_v[...] = jnp.transpose(jnp.broadcast_to(names[0:1, :], (LANES, slots)))
    found_v[...] = jnp.zeros_like(found_v)

    def find(i, carry):
        load_emb(i).wait()
        hot = jnp.where(name_v[:, 0:1] == (iota((1, step), 1) + i * step).astype(F32), 1.0, 0.0).astype(BF16)
        found_v[...] = found_v[...] + contract(hot, emb_v[lax.rem(i, 2)], 1, 1)

        @pl.when(i + 2 < vocab // step)
        def _():
            load_emb(i + 2).start()

        return carry

    with jax.named_scope('find'):
        lax.fori_loop(0, vocab // step, find, 0)
    for k in range(nz):
        fold.store(xs_v.at[k], found_v[k * CAP:(k + 1) * CAP, :].astype(BF16), xh)
    relay(2, None)
    gives = []
    for d in range(1, nz):
        gives.append(start(fold.send(xs_v.at[ring.chip(d)], xr_v.at[z], xh, xs_sem.at[d], xr_sem.at[d], ring.dev(d))))
    xr_v[z] = xs_v[z]
    forward(0)
    forward(1)
    relay(3, 2)
    forward(2)

    with jax.named_scope('gives_wait'):
        for copy in gives:
            copy.wait_recv()
    forward(3)
    for k in range(nz):
        fold.unfold(xr_v.at[k], xh)
    got = xr_v[...].reshape(slots, fold.dp)[:, :dm]
    swaps = []
    for t in range(2):
        x_v[t] = contract(got, pick_v[t], 0, 0).astype(BF16)
        swaps.append(remote(x_v.at[t], xq_v.at[t], ps_sem.at[2 + t], pr_sem.at[2 + t], ring.sibling))
        swaps[t].start()
    forward(4)
    load_grad.wait()
    swap_grad.wait_recv()

    def lanes(b):
        return pl.ds(pl.multiple_of(b * LANES, LANES), LANES)

    def norm(t, b, carry):
        at = lanes(b)
        xb = x_v[t, :, at] + xq_v[t, :, at]
        x_v[t, :, at] = xb
        xf = xb.astype(F32)
        inv = lax.rsqrt(jnp.mean(xf * xf, axis=0, keepdims=True) + EPS)
        gn_v[0, t, :, at] = (xf * inv * gain_v[:dm, :]).astype(BF16)
        return carry

    for t in range(2):
        with jax.named_scope('swapx_wait'):
            swaps[t].wait_send()
            swaps[t].wait_recv()
        lax.fori_loop(0, tl // LANES, functools.partial(norm, t), 0)

    def hidden(lo, hi):
        def body(i, carry):
            s, t = lo + i // 2, lax.rem(i, 2)
            u = jnp.dot(w_v[0, s, :, :dm], gn_v[0, t], preferred_element_type=F32).astype(BF16).astype(F32)
            dh = jnp.dot(w_v[1, s, :, :dm], gn_v[1, t], preferred_element_type=F32)
            act, slope = gelu_pair(u)
            at = pl.ds(pl.multiple_of(s * fl, fl), fl)
            hd_v[1, t, at, :] = act.astype(BF16)
            hd_v[0, t, at, :] = (dh * slope).astype(BF16)
            return carry

        with jax.named_scope(f'hid{lo}'):
            lax.fori_loop(0, 2 * (hi - lo), body, 0)

    def grad_w(w, s):
        at = pl.ds(pl.multiple_of(s * fl, fl), fl)
        return contract(hd_v[w, 0, at, :], gn_v[w, 0], 1, 1) + contract(hd_v[w, 1, at, :], gn_v[w, 1], 1, 1)

    orders = scatter_messages(half)
    sends = [[], []]
    for side, sign in sides:
        for i in range(len(orders[0])):
            src = st_v.at[side, i] if i < 2 else rb_v.at[side, i - 2]
            dst = rb_v.at[side, i]
            sends[side].append(fold.send(src, dst, wh, ss_sem.at[side, i], sr_sem.at[side, i], ring.dev(sign)))

    def scatter(i):
        with jax.named_scope(f'scat{i}'):
            (w0, k0), (_, k1) = orders[0][i], orders[1][i]
            if i >= 2:
                for side, _ in sides:
                    sends[side][i - 2].wait_recv()

            def body(side, carry):
                w = w0 + side * (1 - 2 * w0)
                part = grad_w(w, slot[k0] + side * (slot[k1] - slot[k0]))
                if i < 2:
                    fold.store(st_v.at[side, i], part, wh)
                else:
                    fold.add(rb_v.at[side, i - 2], part, wh)
                return carry

            lax.fori_loop(0, 2, body, 0)
            for side, _ in sides:
                start(sends[side][i])

    forward(5)
    forward(6)
    for stage in range(len(stages)):
        from_twins(stage)
    hidden(0, 1)
    scatter(0)
    hidden(1, nz - 5)
    scatter(1)
    hidden(nz - 5, nz)

    wide = 2 * LANES

    def through(w, t, dst):
        def body(b, carry):
            at = pl.ds(pl.multiple_of(b * wide, wide), wide)
            left = w_v[w, :, :, at].reshape(nz * fl, wide)
            dst[at, :] = contract(left, hd_v[w_of_hd[w], t], 0, 0)
            return carry

        lax.fori_loop(0, fold.dp // wide, body, 0)

    w_of_hd = (0, 1)
    with jax.named_scope('thru'):
        through(0, 1 - c, snd_v)
    body_rows = pl.ds(0, dm)
    swap_dn = remote(snd_v.at[body_rows], dnr_v, ps_sem.at[4], pr_sem.at[4], ring.sibling)
    swap_dn.start()
    through(0, c, own_v)
    with jax.named_scope('swapdn_wait'):
        swap_dn.wait_send()
        swap_dn.wait_recv()

    def dx_block(b, carry):
        at = lanes(b)
        xf = x_v[c, :, at].astype(F32)
        inv = lax.rsqrt(jnp.mean(xf * xf, axis=0, keepdims=True) + EPS)
        q = (own_v[:dm, at] + dnr_v[:, at]) * gain_v[:dm, :]
        dot = jnp.mean(xf * q, axis=0, keepdims=True)
        dxn = inv * q - xf * (inv * inv * inv * dot)
        dx_v[c, :, at] = (gn_v[1, c, :, at].astype(F32) + dxn).astype(BF16)
        return carry

    lax.fori_loop(0, tl // LANES, dx_block, 0)
    swap_dx = start(remote(dx_v.at[c], dx_v.at[c], ps_sem.at[5], pr_sem.at[5], ring.sibling))
    through(1, 1 - c, snd_v)
    swap_y = start(remote(snd_v.at[body_rows], yr_v, ps_sem.at[6], pr_sem.at[6], ring.sibling))
    with jax.named_scope('swapdx_wait'):
        swap_dx.wait_recv()

    def pack(k, carry):
        at = pl.ds(pl.multiple_of(k * CAP, CAP), CAP)
        rows = contract(pick_v[0, at, :], dx_v[0], 1, 1) + contract(pick_v[1, at, :], dx_v[1], 1, 1)
        fold.store(es_v.at[k], rows[:MULTI], eh)
        fold.store(eb_v.at[k], rows[MULTI:].astype(BF16), bh)
        return carry

    lax.fori_loop(0, nz, pack, 0)
    backs = []
    for d in range(1, nz):
        kk, to = ring.chip(d), ring.dev(d)
        backs.append(start(fold.send(es_v.at[kk], er_v.at[z], eh, es_sem.at[0, d], er_sem.at[0, d], to)))
        backs.append(start(fold.send(eb_v.at[kk], eq_v.at[z], bh, es_sem.at[1, d], er_sem.at[1, d], to)))
    er_v[z] = es_v[z]
    eq_v[z] = eb_v[z]
    scatter(2)
    through(1, c, own_v)
    scatter(3)
    with jax.named_scope('swapy_wait'):
        swap_y.wait_recv()

    def out_block(b, carry):
        at = lanes(b)
        out_v[:, at] = (x_v[c, :, at].astype(F32) + (own_v[:dm, at] + yr_v[:, at])).astype(BF16)
        return carry

    lax.fori_loop(0, tl // LANES, out_block, 0)
    keeps = [pltpu.make_async_copy(out_v, out_ref, out_sem.at[0])]
    keeps[0].start()
    last = len(orders[0])
    for i in range(4, last):
        scatter(i)

    with jax.named_scope('backs_wait'):
        for copy in backs:
            copy.wait_recv()
    lots, rest = nz * MULTI, CAP - MULTI

    def spread(k, carry):
        fold.unfold(er_v.at[k], eh)
        fold.unfold(eq_v.at[k], bh)
        rows = er_v[k, :, :dm]
        head = name_v[pl.ds(pl.multiple_of(k * CAP, CAP), MULTI), :]
        for p in range(3):
            at = pl.ds(pl.multiple_of(p * lots + k * MULTI, MULTI), MULTI)
            piece = rows.astype(BF16)
            rows_v[at, :] = piece
            names_ref[at, :] = head
            rows = rows - piece.astype(F32)
        at = pl.ds(pl.multiple_of(3 * lots + k * rest, 16), rest)
        rows_v[at, :] = eq_v[k, :, :dm]
        names_ref[at, :] = name_v[pl.ds(pl.multiple_of(k * CAP + MULTI, 16), rest), :]
        return carry

    lax.fori_loop(0, nz, spread, 0)
    keeps.append(pltpu.make_async_copy(rows_v, rows_ref, out_sem.at[1]))
    keeps[1].start()

    for w in range(2):
        a, b = (last - 1, last - 2) if w == 0 else (last - 2, last - 1)
        part = grad_w(w, mine)
        with jax.named_scope(f'fin{w}'):
            sends[0][a].wait_recv()
            sends[1][b].wait_recv()
        rb_v[0, a] = rb_v[0, a] + rb_v[1, b]
        fold.unfold(rb_v.at[0, a], wh)
        (dup_ref, ddown_ref)[w][...] = rb_v[0, a, :, :dm] + part
    for copy in sent:
        copy.wait_send()
    for copy in keeps:
        copy.wait()


def step(n, groups, ids, emb_t, up, down, grad_t, gain):
    nz = n // 2
    dm, vocab = emb_t.shape
    tl, fl = ids.shape[1], up.shape[0]
    tp = 2 * tl
    dp = Fold(dm).dp
    slots = nz * CAP
    parts = slots + 2 * nz * MULTI
    hops = nz - 1
    each, _ = shared_blocks(groups)
    vmem, hbm = pl.BlockSpec(memory_space=pltpu.VMEM), pl.BlockSpec(memory_space=pl.ANY)
    dma = pltpu.SemaphoreType.DMA
    tokens = pltpu.VMEM((2, dm, tl), BF16)
    return pl.pallas_call(
        functools.partial(step_kernel, n, groups),
        name='step',
        out_shape=(
            jax.ShapeDtypeStruct((dm, tl), BF16),
            jax.ShapeDtypeStruct((fl, dm), F32),
            jax.ShapeDtypeStruct((fl, dm), F32),
            jax.ShapeDtypeStruct((parts, dm), BF16),
            jax.ShapeDtypeStruct((parts, LANES), F32),
            jax.ShapeDtypeStruct((1, 1), F32),
        ),
        in_specs=[vmem, hbm, vmem, vmem, hbm, vmem],
        out_specs=(hbm, vmem, vmem, hbm, vmem, pl.BlockSpec(memory_space=pltpu.SMEM)),
        scratch_shapes=[
            pltpu.VMEM((2, nz, fl, dp), BF16),
            pltpu.VMEM((2, 2, dm, tl), BF16),
            tokens, tokens,
            pltpu.VMEM((2, 2, nz * fl, tl), BF16),
            pltpu.VMEM((2, 2, fl, dp), F32),
            pltpu.VMEM((2, hops, fl, dp), F32),
            pltpu.VMEM((dp, tl), F32),
            pltpu.VMEM((dp, tl), F32),
            pltpu.VMEM((dm, tl), F32),
            pltpu.VMEM((dm, tl), F32),
            tokens,
            pltpu.VMEM((nz, MULTI, dp), F32),
            pltpu.VMEM((nz, MULTI, dp), F32),
            pltpu.VMEM((nz, CAP - MULTI, dp), BF16),
            pltpu.VMEM((nz, CAP - MULTI, dp), BF16),
            pltpu.VMEM((nz, CAP, dp), BF16),
            pltpu.VMEM((nz, CAP, dp), BF16),
            pltpu.VMEM((2, slots, tl), BF16),
            pltpu.VMEM((tp, tp), BF16),
            pltpu.VMEM((2, 1, tl), jnp.int32),
            pltpu.VMEM((slots, LANES), F32),
            pltpu.VMEM((slots, LANES), F32),
            pltpu.VMEM((nz, 8, LANES), F32),
            pltpu.VMEM((nz, 8, LANES), F32),
            pltpu.VMEM((2, dm, 512), BF16),
            pltpu.VMEM((slots, dm), F32),
            pltpu.VMEM((dm, tl), BF16),
            pltpu.VMEM((parts, dm), BF16),
            pltpu.VMEM((1, dp), F32),
            pltpu.VMEM((dp, LANES), F32),
            dma((2,)), dma((2,)), dma((2, hops, 2)), dma((2, hops, 2)),
            dma((2, each, nz // 2)), dma((2, each, nz // 2)), dma((3, each, groups)), dma((3, each, groups)),
            dma((7,)), dma((7,)),
            dma((nz,)), dma((nz,)), dma((nz, 2)), dma((nz, 2)),
            dma((2, hops, 2)), dma((2, hops, 2)), dma((2, nz, 2)), dma((2, nz, 2)), dma((2,)),
        ],
        compiler_params=pltpu.CompilerParams(
            collective_id=0, has_side_effects=True, vmem_limit_bytes=VMEM_LIMIT
        ),
    )(ids, emb_t, up, down, grad_t, gain)


def place_kernel(names_ref, rows_ref, out_ref, up_ref, down_ref, emb_out, out_out, up_out, down_out):
    block = emb_out.shape[1]
    here = names_ref[:, 0:1] == (iota((1, block), 1) + pl.program_id(0) * block).astype(F32)
    hot = jnp.where(here, 1.0, 0.0).astype(BF16)
    emb_out[...] = contract(rows_ref[...], hot, 0, 0)
    out_out[...] = out_ref[...]
    up_out[...] = up_ref[...]
    down_out[...] = down_ref[...]


def place(vocab, names, rows, out, d_up, d_down):
    parts, dm = rows.shape
    grid = 4
    passing = [pl.BlockSpec((a.shape[0] // grid, a.shape[1]), lambda i: (i, 0)) for a in (out, d_up, d_down)]
    return pl.pallas_call(
        place_kernel,
        name='place',
        grid=(grid,),
        out_shape=(jax.ShapeDtypeStruct((dm, vocab), F32),)
        + tuple(jax.ShapeDtypeStruct(a.shape, a.dtype) for a in (out, d_up, d_down)),
        in_specs=[pl.BlockSpec((parts, LANES), lambda i: (0, 0)), pl.BlockSpec((parts, dm), lambda i: (0, 0))] + passing,
        out_specs=(pl.BlockSpec((dm, vocab // grid), lambda i: (0, i)),) + tuple(passing),
        compiler_params=pltpu.CompilerParams(vmem_limit_bytes=VMEM_LIMIT),
    )(names, rows, out, d_up, d_down)


def swap_kernel(n, src_ref, dst_ref, keep_sem, send_sem, recv_sem):
    me = lax.axis_index('tensor')
    sem = pltpu.get_barrier_semaphore()
    for d in range(1, n):
        pl.semaphore_signal(sem, inc=1, device_id={'tensor': lax.rem(me + d, n)}, device_id_type=MESH)
    pl.semaphore_wait(sem, n - 1)
    keep = pltpu.make_async_copy(src_ref.at[me], dst_ref.at[me], keep_sem)
    keep.start()
    copies = []
    for d in range(1, n):
        to = lax.rem(me + d, n)
        copies.append(remote(src_ref.at[to], dst_ref.at[me], send_sem.at[d], recv_sem.at[d], {'tensor': to}))
        copies[-1].start()
    for copy in copies:
        copy.wait()
    keep.wait()


def swap_blocks(n, blocks, collective_id):
    hbm = pl.BlockSpec(memory_space=pl.ANY)
    return pl.pallas_call(
        functools.partial(swap_kernel, n),
        name='swap_blocks',
        out_shape=jax.ShapeDtypeStruct(blocks.shape, blocks.dtype),
        in_specs=[hbm],
        out_specs=hbm,
        scratch_shapes=[pltpu.SemaphoreType.DMA, pltpu.SemaphoreType.DMA((n,)), pltpu.SemaphoreType.DMA((n,))],
        compiler_params=pltpu.CompilerParams(collective_id=collective_id, has_side_effects=True),
    )(blocks)


def all_blocks(n, block, collective_id):
    return swap_blocks(n, jnp.broadcast_to(block[None], (n,) + block.shape), collective_id)


def rms_norm(x_rows, gain_f):
    inv_rms = lax.rsqrt(jnp.mean(x_rows * x_rows, axis=-1, keepdims=True) + EPS)
    return x_rows * inv_rms * gain_f


def dense_step(n, ids, emb, norm_gain, up, down, grad_out):
    vocab, dm = emb.shape
    fl = up.shape[0]
    base = (lax.axis_index('tensor') * vocab).astype(F32)
    ids_all = all_blocks(n, jnp.broadcast_to(ids.astype(F32), (8, ids.shape[1])), 1)[:, 0]
    hot = (iota((ids_all.size, vocab), 1).astype(F32) == ids_all.reshape(-1, 1) - base).astype(BF16)
    part = jnp.dot(hot, emb, preferred_element_type=F32).astype(BF16)
    x_f = jnp.sum(swap_blocks(n, part.reshape(n, -1, dm), 2).astype(F32), axis=0)
    ws = all_blocks(n, jnp.stack([up, down]), 3)
    up_all, down_all = ws[:, 0].reshape(-1, dm), ws[:, 1].reshape(-1, dm)
    normed_f, norm_back = jax.vjp(lambda x_in: rms_norm(x_in, norm_gain.astype(F32)), x_f)
    normed = normed_f.astype(BF16)
    pre_act = contract(normed, up_all, 1, 1).astype(BF16).astype(F32)
    act_f, slope = gelu_pair(pre_act)
    hidden = act_f.astype(BF16)
    d_pre = (contract(grad_out, down_all, 1, 1) * slope).astype(BF16)
    y = jnp.dot(hidden, down_all, preferred_element_type=F32)
    out = (x_f + y).astype(BF16)
    d_norm = jnp.dot(d_pre, up_all, preferred_element_type=F32)
    dx = (grad_out.astype(F32) + norm_back(d_norm)[0]).astype(BF16)
    d_w = jnp.stack([contract(d_pre, normed, 0, 0), contract(hidden, grad_out, 0, 0)]).reshape(2, n, fl, dm)
    d_w = jnp.sum(swap_blocks(n, jnp.moveaxis(d_w, 1, 0), 4), axis=0)
    dx_all = all_blocks(n, dx, 5).reshape(-1, dm)
    hot_t = (iota((vocab, ids_all.size), 0).astype(F32) == ids_all.reshape(1, -1) - base).astype(BF16)
    d_emb = jnp.dot(hot_t, dx_all, preferred_element_type=F32)
    return d_emb.T, out.T, d_w[0], d_w[1]


def solution(mesh):
    n, groups = mesh.shape['tensor'], mesh.shape['data']
    tok_spec = P(('data', 'tensor'))
    row_spec = P(('data', 'tensor'), None)

    def local_step(token_ids, emb_shard, norm_gain, w_up, w_down, grad_out):
        vocab, dm = emb_shard.shape
        ids, gain, up = token_ids[None, :], norm_gain, w_up.T
        out, d_up, d_down, rows, names, flag = step(n, groups, ids, emb_shard.T, up, w_down, grad_out.T, gain)
        placed = place(vocab, names, rows, out, d_up, d_down)

        def again(state):
            return (jnp.zeros((), F32),) + dense_step(n, ids, emb_shard, norm_gain, up, w_down, grad_out)

        state = lax.while_loop(lambda state: state[0] > 0.5, again, (flag[0, 0],) + tuple(placed))
        _, d_emb, out, d_up, d_down = state
        return out.T, d_emb.T, d_up.T, d_down

    return jax.shard_map(
        local_step,
        mesh=mesh,
        in_specs=(tok_spec, P('tensor', None), P(None), P(None, 'tensor'), P('tensor', None), row_spec),
        out_specs=(row_spec, row_spec, P('data', 'tensor'), row_spec),
        check_vma=False,
    )
```

```python
import functools

import jax
import jax.numpy as jnp
from jax import lax
from jax.experimental import pallas as pl
from jax.experimental.pallas import tpu as pltpu
from jax.sharding import PartitionSpec as P

EPS = 1e-6
CAP = 64
MULTI = 16
PAIR = 2
BHEAD = 32
PLACE_GRID = 6
PLACE_ROWS = 256
LANES = 128
MESH = pl.DeviceIdType.MESH
VMEM_LIMIT = 67_000_000
F32 = jnp.float32
BF16 = jnp.bfloat16
SQRT_2_PI = 0.7978845608028654
CUBIC = 0.044715


def contract(left_op, right_op, left_dim, right_dim):
    dims = (((left_dim,), (right_dim,)), ((), ()))
    return lax.dot_general(left_op, right_op, dims, preferred_element_type=F32)


def first_first(left_op, right_op):
    return contract(left_op, right_op, 0, 0)


def last_last(left_op, right_op):
    return contract(left_op, right_op, 1, 1)


def iota(shape, dim):
    return lax.broadcasted_iota(jnp.int32, shape, dim)


def down(rows, start=0):
    return iota((rows, 1), 0) + start


def across(lanes, start=0):
    return iota((1, lanes), 1) + start


def flags(mask):
    return jnp.where(mask, 1.0, 0.0)


def one_hot(mask):
    return flags(mask).astype(BF16)


def over_rows(reduce, value):
    return reduce(value, axis=0, keepdims=True)


def over_lanes(reduce, value):
    return reduce(value, axis=1, keepdims=True)


def earlier_than(rows, lanes, start):
    return down(rows, start) < across(lanes)


def gelu_pair(u):
    t = jnp.tanh(SQRT_2_PI * (u + CUBIC * (u * u * u)))
    cdf = 0.5 * (1.0 + t)
    slope = cdf + u * (0.5 * (1.0 - t * t)) * (SQRT_2_PI * (1.0 + (3.0 * CUBIC) * (u * u)))
    return u * cdf, slope


def rows_at(i):
    return slice(i * LANES, (i + 1) * LANES)


class Ring:
    def __init__(self, n, groups):
        self.n, self.nz, self.half, self.groups = n, n // 2, n // 4, groups
        self.me = lax.axis_index('tensor')
        self.g = lax.axis_index('data')
        self.c = lax.rem(self.me, 2)
        self.z = self.me // 2

    def chip(self, k):
        return lax.rem(self.z + (k + self.nz) % self.nz, self.nz)

    def dev(self, k):
        return {'tensor': 2 * self.chip(k) + self.c}

    def twin(self, e):
        return {'data': lax.rem(self.g + e, self.groups), 'tensor': self.me}

    @property
    def sibling(self):
        return {'tensor': self.me + 1 - 2 * self.c}

    def greet(self):
        sem = pltpu.get_barrier_semaphore()
        for k in range(1, self.nz):
            pl.semaphore_signal(sem, device_id=self.dev(k), device_id_type=MESH)
        pl.semaphore_signal(sem, device_id=self.sibling, device_id_type=MESH)
        for e in range(1, self.groups):
            pl.semaphore_signal(sem, device_id=self.twin(e), device_id_type=MESH)

    def meet(self):
        pl.semaphore_wait(pltpu.get_barrier_semaphore(), self.nz + self.groups - 1)


def slot_of(nz):
    half = nz // 2
    order = [half] + [s * k for k in range(half - 1, 0, -1) for s in (1, -1)] + [0]
    table = {k: i for i, k in enumerate(order)}
    table[-half] = table[half]
    return table


def gather_messages(half):
    right = [(w, k) for k in range(half) for w in (0, 1) if w == 0 or k < half - 1]
    return right, [(1 - w, k) for w, k in right]


BLOCK = 16


def shared_blocks(fl, groups):
    shared = fl - 2 * BLOCK
    count = 2 if groups * BLOCK <= shared else 1
    height = 2 * shared // (groups * count)
    assert height % BLOCK == 0 and height * groups * count == 2 * shared
    return count, height, shared


def far_first(nz):
    return [(nz // 2 + (-1) ** r * ((r + 1) // 2)) % nz for r in range(nz)]


def scatter_messages(half):
    right = [(0, half)]
    for k in range(half - 1, 0, -1):
        right += [(1, k), (0, k)]
    return right, [(1 - w, -k) for w, k in right]


def remote(src, dst, send_sem, recv_sem, device):
    return pltpu.make_async_remote_copy(
        src_ref=src, dst_ref=dst, send_sem=send_sem, recv_sem=recv_sem, device_id=device, device_id_type=MESH
    )


class Fold:
    def __init__(self, dm):
        self.dm = dm
        self.lo = dm // LANES * LANES
        self.dp = self.lo + LANES
        assert 2 * (dm - self.lo) == LANES

    def tail(self, value, h):
        low = value.shape[0] - h
        return jnp.concatenate([value[:low, self.lo:self.dm], value[h:, self.lo:self.dm]], axis=1)

    def store(self, ref, value, h):
        low = value.shape[0] - h
        ref[:, :self.lo] = value[:, :self.lo]
        ref[:low, self.lo:] = self.tail(value, h)
        if low < h:
            ref[low:h, self.lo:self.dm] = value[low:h, self.lo:self.dm]

    def add(self, ref, value, h):
        low = value.shape[0] - h
        ref[:, :self.lo] = ref[:, :self.lo] + value[:, :self.lo]
        ref[:low, self.lo:] = ref[:low, self.lo:] + self.tail(value, h)

    def unfold(self, ref, h):
        low = ref.shape[0] - h
        ref[h:, self.lo:self.dm] = ref[:low, self.dm:self.dp]

    def send(self, src, dst, h, send_sem, recv_sem, device):
        return FoldCopy(self, src, dst, h, send_sem, recv_sem, device, self.spare[jnp.dtype(src.dtype)])


class FoldCopy:
    def __init__(self, fold, src, dst, h, send_sem, recv_sem, device, spare):
        low = src.shape[0] - h
        parts = ((pl.ds(0, h), pl.ds(0, fold.dp)), (pl.ds(h, low), pl.ds(0, fold.lo)))
        self.copies = [remote(src.at[r, l], dst.at[r, l], send_sem, recv_sem, device) for r, l in parts]
        size = h * fold.dp + low * fold.lo
        tile = 16 if jnp.dtype(spare.dtype) == jnp.dtype(BF16) else 8
        width = next(w for w in range(LANES, spare.shape[1] + 1, LANES)
                     if size % (w * tile) == 0 and size // w <= spare.shape[0])
        whole = spare.at[pl.ds(0, size // width), pl.ds(0, width)]
        self.whole = remote(whole, whole, send_sem, recv_sem, device)

    def start(self):
        for copy in self.copies:
            copy.start()

    def wait_recv(self):
        self.whole.wait_recv()

    def wait_send(self):
        self.whole.wait_send()


def step_kernel(
    n, groups, ids_ref, emb_ref, up_ref, down_ref, grad_ref, gain_ref,
    out_ref, dup_ref, ddown_ref, rows_ref, names_ref, bounds_ref, flag_ref,
    w_v, gn_v, x_v, hd_v, st_v, rb_v, snd_v, own_v, dnr_v, yr_v, dx_v, es_v, er_v, eb_v, eq_v, xs_v, xr_v,
    pick_v, tri_v, ids_v, col_v, name_v, nrow_v, req_s, req_r, emb_v, found_v, out_v, rows_v, row_v, gain_v,
    own_w, line_v, flag_v, names_v, bounds_v, dw_v, xo_v, xf_sem, xg_sem,
    ld_sem, emb_sem, ws_sem, wr_sem, bs_sem, br_sem, ts_sem, tr_sem, ps_sem, pr_sem, qs_sem, qr_sem, xr_sem,
    ss_sem, sr_sem, er_sem, out_sem,
):
    ring = Ring(n, groups)
    nz, half, c, z = ring.nz, ring.half, ring.c, ring.z
    slot = slot_of(nz)
    dm, vocab = emb_ref.shape
    fl = up_ref.shape[0]
    each, height, shared = shared_blocks(fl, groups)
    order = far_first(nz)
    back = [order.index((nz - d) % nz) for d in order]
    tl = ids_ref.shape[1]
    tp = 2 * tl
    slots = nz * CAP
    fold = Fold(dm)
    fold.spare = {jnp.dtype(BF16): gn_v.at[0, 0], jnp.dtype(F32): own_v}
    wh, xh, eh, bh = fl // 2, CAP // 2, MULTI // 2, BHEAD
    gh = (fl - shared) // 2
    ring_rows = pl.ds(shared, fl - shared)
    step = emb_v.shape[2]
    sides = ((0, 1), (1, -1))
    sent = []

    ring.greet()
    own_ids = pltpu.make_async_copy(ids_ref, ids_v.at[c], ld_sem.at[1])
    load_w = [pltpu.make_async_copy(ref, own_w.at[w], ld_sem.at[2 + w]) for w, ref in enumerate((up_ref, down_ref))]
    load_gain = pltpu.make_async_copy(gain_ref, line_v, ld_sem.at[4])
    load_grad = pltpu.make_async_copy(grad_ref, gn_v.at[1, c], ld_sem.at[0])
    for copy in [own_ids, load_gain] + load_w + [load_grad]:
        copy.start()

    def load_emb(i):
        at = pl.ds(pl.multiple_of(i * step, step), step)
        return pltpu.make_async_copy(emb_ref.at[:, at], emb_v.at[i], emb_sem.at[i])

    for i in range(vocab // step):
        load_emb(i).start()
    for i in range(tp // LANES):
        tri_v[rows_at(i), :] = one_hot(earlier_than(LANES, tp, i * LANES))
    mine = slot[0]
    for w in range(PAIR):
        load_w[w].wait()
        w_v[w, mine, :, :dm] = own_w[w]
        w_v[w, mine, shared:shared + gh, dm:] = own_w[w, shared + gh:, fold.lo:]
    row_v[...] = jnp.zeros_like(row_v)
    load_gain.wait()
    row_v[:, :dm] = line_v[...].astype(F32).reshape(1, dm)
    gain_v[...] = jnp.transpose(jnp.broadcast_to(row_v[...], (LANES, fold.dp)))
    own_ids.wait()
    with jax.named_scope('barrier'):
        ring.meet()

    def start(copy, after=None):
        if after is not None:
            after.wait_send()
            sent[:] = [other for other in sent if other is not after]
        copy.start()
        sent.append(copy)
        return copy

    blocks = []
    for j in range(each):
        b = ring.g * each + j
        blocks.append((lax.rem(b, PAIR), pl.ds(pl.multiple_of(height * (b // 2), BLOCK), height)))

    def hops(k):
        return [
            remote(
                w_v.at[blocks[j][0], slot[-k * sign], blocks[j][1]],
                w_v.at[blocks[j][0], slot[-(k + 1) * sign], blocks[j][1]],
                bs_sem.at[side, j, k % 2], br_sem.at[side, j, k], ring.dev(sign),
            )
            for j in range(each) for side, sign in sides if k < half - 1 or side == j % 2
        ]

    def hop_before(k):
        keep = [k < half - 1 or side == j % 2 for j in range(each) for side, _ in sides]
        return [copy for copy, use in zip(block_moves[k - 2], keep) if use]

    stages = ((nz - 3, nz - 1), (nz - 5, nz - 3), (0, nz - 5))

    def twins(stage):
        lo, hi = stages[stage]
        return [
            remote(
                w_v.at[w, pl.ds(lo, hi - lo), at], w_v.at[w, pl.ds(lo, hi - lo), at],
                ts_sem.at[stage % 2, j, e - 1], tr_sem.at[stage, j, e - 1], ring.twin(e),
            )
            for j, (w, at) in enumerate(blocks) for e in range(1, groups)
        ]

    block_moves = [hops(k) for k in range(half)]
    twin_moves = [twins(stage) for stage in range(len(stages))]

    def relay(k, stage):
        with jax.named_scope(f'relay{k}'):
            for copy in block_moves[k]:
                copy.wait_recv()
            if k + 1 < half:
                earlier = hop_before(k + 1) if k >= 1 else [None] * len(block_moves[1])
                for copy, after in zip(block_moves[k + 1], earlier):
                    start(copy, after)
            if stage is not None:
                earlier = twin_moves[stage - 2] if stage >= 2 else [None] * len(twin_moves[stage])
                for copy, after in zip(twin_moves[stage], earlier):
                    start(copy, after)

    def from_twins(stage):
        with jax.named_scope(f'twins{stage}'):
            for copy in twin_moves[stage]:
                copy.wait_recv()

    for copy in block_moves[0]:
        start(copy)
    swap_ids = start(remote(ids_v.at[c], ids_v.at[c], ps_sem.at[0], pr_sem.at[0], ring.sibling))
    moves = [[], []]
    for side, sign in sides:
        for i, (w, k) in enumerate(gather_messages(half)[side]):
            src, dst = w_v.at[w, slot[-k * sign], ring_rows], w_v.at[w, slot[-(k + 1) * sign], ring_rows]
            moves[side].append(fold.send(src, dst, gh, ws_sem.at[side, i % 2], wr_sem.at[side, i], ring.dev(sign)))
    def forward(i):
        with jax.named_scope(f'fwd{i}'):
            for side, sign in sides:
                moves[side][i].wait_recv()
                if i + 2 < len(moves[side]):
                    start(moves[side][i + 2], moves[side][i])
                w, k = gather_messages(half)[side][i]
                fold.unfold(w_v.at[w, slot[-(k + 1) * sign], ring_rows], gh)

    with jax.named_scope('ids_wait'):
        swap_ids.wait_recv()
    ids = jnp.concatenate([ids_v[0], ids_v[1]], axis=1).astype(F32)
    ids_t = jnp.transpose(jnp.broadcast_to(ids, (LANES, tp)))
    seen = jnp.zeros((1, tp), F32)
    total = jnp.zeros((1, tp), F32)
    for i in range(tp // LANES):
        tri = flags(earlier_than(LANES, tp, i * LANES))
        same = flags(ids_t[rows_at(i), :1] == ids)
        seen = jnp.maximum(seen, over_rows(jnp.max, same * tri))
        total = total + over_rows(jnp.sum, same)
    row = down(n)
    place = lax.rem(row, nz)
    chip = lax.rem(z + half + (1 - 2 * lax.rem(place, 2)) * ((place + 1) // 2), nz)
    owner = 2 * chip + jnp.where(row < nz, c, 1 - c)
    base = (owner * vocab).astype(F32)
    member = flags((seen < 0.5) & (ids >= base) & (ids < base + vocab))
    multi = flags(total > 1.5)
    several, single = member * multi, member * (1.0 - multi)
    both = jnp.concatenate([several, single], axis=0).astype(BF16)
    rank = jnp.dot(both, tri_v[...], preferred_element_type=F32)
    n_several = over_lanes(jnp.sum, several)
    count = n_several + over_lanes(jnp.sum, single)
    rank = jnp.where(several > 0.5, rank[:n], n_several + rank[n:])
    over = over_rows(jnp.max, flags((count > CAP) | (n_several > MULTI)))
    for k in range(n):
        hit = (rank[k:k + 1, :] == down(CAP).astype(F32)) & (member[k:k + 1, :] > 0.5)
        col = over_lanes(jnp.max, jnp.where(hit, ids, -1.0))
        col_v[k * CAP:(k + 1) * CAP, :] = jnp.broadcast_to(col, (CAP, LANES))
    cols_t = jnp.transpose(col_v[:slots, :])
    lane = iota((8, LANES), 1)
    per = LANES // CAP
    for k in range(nz):
        at = (k // per) * LANES
        tile = cols_t[0:8, at:at + LANES]
        if k % per:
            tile = pltpu.roll(tile, LANES - (k % per) * CAP, 1)
        req_s[k] = jnp.where(lane < CAP, tile, over)
    asks = []
    for p, d in enumerate(order[:-1]):
        asks.append(start(remote(req_s.at[p], req_r.at[back[p]], qs_sem.at[p], qr_sem.at[p], ring.dev(d))))
    relay(0, 0)
    for i in range(PAIR):
        for side, _ in sides:
            start(moves[side][i])
    swap_grad = start(remote(grad_ref, gn_v.at[1, c], ps_sem.at[1], pr_sem.at[1], ring.sibling))
    req_r[nz - 1] = req_s[nz - 1]
    for q in range(PAIR):
        for t in range(PAIR):
            pick_v[q, t] = one_hot(col_v[q * slots:(q + 1) * slots, :1] == ids[:, t * tl:(t + 1) * tl])

    with jax.named_scope('asks_wait'):
        for copy in asks:
            copy.wait_recv()
    flag = req_r[0]
    for k in range(1, nz):
        flag = jnp.maximum(flag, req_r[k])
    flag_v[...] = over_rows(jnp.max, over_lanes(jnp.max, jnp.where(lane < CAP, 0.0, flag)))
    keeps = [pltpu.make_async_copy(flag_v, flag_ref, out_sem.at[2])]
    keeps[0].start()
    tiles = []
    for p in range(nz // per):
        tile = req_r[p * per]
        for j in range(1, per):
            tile = jnp.where(lane < j * CAP, tile, pltpu.roll(req_r[p * per + j], j * CAP, 1))
        tiles.append(tile)
    names = jnp.concatenate(tiles, axis=1) - (ring.me * vocab).astype(F32)
    nrow_v[...] = names
    name_v[...] = jnp.transpose(jnp.broadcast_to(names[0:1, :], (LANES, slots)))
    gives = []

    def find(part):
        cols = slice(part * slots // 2, (part + 1) * slots // 2)
        found_v[...] = jnp.zeros_like(found_v)

        def body(i, carry):
            if part == 0:
                load_emb(i).wait()
            hot = one_hot(down(step, i * step).astype(F32) == nrow_v[:1, cols])
            found_v[:dm, :] = found_v[:dm, :] + jnp.dot(emb_v[i], hot, preferred_element_type=F32)
            return carry

        with jax.named_scope(f'find{part}'):
            lax.fori_loop(0, vocab // step, body, 0)
        found = jnp.transpose(found_v[...])[:, :dm].astype(BF16)
        for q in range(nz // 2):
            fold.store(xs_v.at[part * nz // 2 + q], found[q * CAP:(q + 1) * CAP, :], xh)

    def hand(p):
        return fold.send(xr_v.at[p], xo_v.at[p], xh, xf_sem.at[p], xg_sem.at[p], ring.sibling)

    def give(part):
        for p in range(part * nz // 2, (part + 1) * nz // 2):
            if order[p]:
                to = ring.dev(order[p])
                give_row = fold.send(xs_v.at[p], xr_v.at[back[p]], xh, qs_sem.at[p], xr_sem.at[p], to)
                gives.append(start(give_row, asks[p]))

    relay(1, 1)
    find(0)
    relay(2, None)
    forward(0)
    give(0)
    find(1)
    forward(1)
    give(1)
    xr_v[nz - 1] = xs_v[nz - 1]
    handed = {nz - 1: start(hand(nz - 1))}
    relay(3, 2)
    forward(2)

    with jax.named_scope('gives_wait'):
        for p in range(nz - 1):
            gives[p].wait_recv()
            handed[back[p]] = start(hand(back[p]))
    forward(3)

    def unpack(rows_of, q):
        for p in range(nz):
            fold.unfold(rows_of.at[p], xh)
        rows = rows_of[...].reshape(slots, fold.dp)[:, :dm]
        return [first_first(rows, pick_v[q, t]).astype(BF16) for t in range(PAIR)]

    for t, part in enumerate(unpack(xr_v, 0)):
        x_v[t] = part
    forward(4)
    load_grad.wait()
    swap_grad.wait_recv()
    with jax.named_scope('sibling_wait'):
        for copy in handed.values():
            copy.wait_recv()
    for t, part in enumerate(unpack(xo_v, 1)):
        x_v[t] = x_v[t] + part

    def lanes(b):
        return pl.ds(pl.multiple_of(b * LANES, LANES), LANES)

    def norm(i, carry):
        t, at = i // (tl // LANES), lanes(lax.rem(i, tl // LANES))
        xf = x_v[t, :, at].astype(F32)
        inv = lax.rsqrt(over_rows(jnp.mean, xf * xf) + EPS)
        gn_v[0, t, :, at] = (xf * inv * gain_v[:dm, :]).astype(BF16)
        return carry

    lax.fori_loop(0, tp // LANES, norm, 0)

    def hidden(lo, hi):
        def body(i, carry):
            s, t = lo + i // 2, lax.rem(i, PAIR)
            u = jnp.dot(w_v[0, s, :, :dm], gn_v[0, t], preferred_element_type=F32).astype(BF16).astype(F32)
            dh = jnp.dot(w_v[1, s, :, :dm], gn_v[1, t], preferred_element_type=F32)
            act, slope = gelu_pair(u)
            at = pl.ds(pl.multiple_of(s * fl, fl), fl)
            hd_v[1, t, at, :] = act.astype(BF16)
            hd_v[0, t, at, :] = (dh * slope).astype(BF16)
            return carry

        with jax.named_scope(f'hid{lo}'):
            lax.fori_loop(0, 2 * (hi - lo), body, 0)

    def grad_w(w, s):
        at = pl.ds(pl.multiple_of(s * fl, fl), fl)
        return last_last(hd_v[w, 0, at, :], gn_v[w, 0]) + last_last(hd_v[w, 1, at, :], gn_v[w, 1])

    orders = scatter_messages(half)
    sends = [[], []]
    for side, sign in sides:
        for i in range(len(orders[0])):
            src = st_v.at[side, i] if i < 2 else rb_v.at[side, i - 2]
            dst = rb_v.at[side, i]
            sends[side].append(fold.send(src, dst, wh, ss_sem.at[side, i % 2], sr_sem.at[side, i], ring.dev(sign)))

    def scatter(i):
        with jax.named_scope(f'scat{i}'):
            (w0, k0), (_, k1) = orders[0][i], orders[1][i]
            if i >= 2:
                for side, _ in sides:
                    sends[side][i - 2].wait_recv()

            def body(side, carry):
                w = w0 + side * (1 - 2 * w0)
                part = grad_w(w, slot[k0] + side * (slot[k1] - slot[k0]))
                if i < 2:
                    fold.store(st_v.at[side, i], part, wh)
                else:
                    fold.add(rb_v.at[side, i - 2], part, wh)
                return carry

            if i:
                lax.fori_loop(0, 2, body, 0)
            for side, _ in sides:
                if i == 0:
                    body(side, 0)
                start(sends[side][i], sends[side][i - 2] if i >= 2 else None)

    forward(5)
    forward(6)
    for stage in range(len(stages)):
        from_twins(stage)
    hidden(0, 1)
    scatter(0)
    hidden(1, nz - 5)
    scatter(1)
    hidden(nz - 5, nz)

    wide = 2 * LANES

    def through(w, t, dst):
        def body(b, carry):
            at = pl.ds(pl.multiple_of(b * wide, wide), wide)
            left = w_v[w, :, :, at].reshape(nz * fl, wide)
            dst[at, :] = first_first(left, hd_v[w_of_hd[w], t])
            return carry

        lax.fori_loop(0, fold.dp // wide, body, 0)

    w_of_hd = (0, 1)
    with jax.named_scope('thru'):
        through(0, 1 - c, snd_v)
    body_rows = pl.ds(0, dm)
    swap_dn = remote(snd_v.at[body_rows], dnr_v, ps_sem.at[2], pr_sem.at[2], ring.sibling)
    swap_dn.start()
    through(0, c, own_v)
    with jax.named_scope('swapdn_wait'):
        swap_dn.wait_send()
        swap_dn.wait_recv()

    def dx_block(b, carry):
        at = lanes(b)
        xf = x_v[c, :, at].astype(F32)
        inv = lax.rsqrt(over_rows(jnp.mean, xf * xf) + EPS)
        q = (own_v[:dm, at] + dnr_v[:, at]) * gain_v[:dm, :]
        dot = over_rows(jnp.mean, xf * q)
        dxn = inv * q - xf * (inv * inv * inv * dot)
        dx_v[c, :, at] = (gn_v[1, c, :, at].astype(F32) + dxn).astype(BF16)
        return carry

    lax.fori_loop(0, tl // LANES, dx_block, 0)
    swap_dx = start(remote(dx_v.at[c], dx_v.at[c], ps_sem.at[3], pr_sem.at[3], ring.sibling))
    through(1, 1 - c, snd_v)
    swap_y = start(remote(snd_v.at[body_rows], yr_v, ps_sem.at[4], pr_sem.at[4], ring.sibling))
    with jax.named_scope('swapdx_wait'):
        swap_dx.wait_recv()

    def pack(k, carry):
        at = pl.ds(pl.multiple_of(k * CAP, CAP), CAP)
        rows = last_last(pick_v[0, 0, at, :], dx_v[0]) + last_last(pick_v[0, 1, at, :], dx_v[1])
        fold.store(es_v.at[k], rows[:MULTI], eh)
        fold.store(eb_v.at[k], rows[MULTI:].astype(BF16), bh)
        return carry

    lax.fori_loop(0, nz, pack, 0)
    backs = []
    for p, d in enumerate(order[:-1]):
        to, q = ring.dev(d), back[p]
        backs.append(start(fold.send(es_v.at[p], er_v.at[q], eh, qs_sem.at[p], er_sem.at[0, p], to), gives[p]))
        backs.append(start(fold.send(eb_v.at[p], eq_v.at[q], bh, xf_sem.at[p], er_sem.at[1, p], to), handed[p]))
    er_v[nz - 1] = es_v[nz - 1]
    eq_v[nz - 1] = eb_v[nz - 1]
    scatter(2)
    through(1, c, own_v)
    scatter(3)
    with jax.named_scope('swapy_wait'):
        swap_y.wait_recv()

    def out_block(b, carry):
        at = lanes(b)
        out_v[:, at] = (x_v[c, :, at].astype(F32) + (own_v[:dm, at] + yr_v[:, at])).astype(BF16)
        return carry

    lax.fori_loop(0, tl // LANES, out_block, 0)
    keeps.append(pltpu.make_async_copy(out_v, out_ref, out_sem.at[0]))
    keeps[-1].start()
    last = len(orders[0])
    for i in range(4, last):
        scatter(i)

    with jax.named_scope('backs_wait'):
        for copy in backs:
            copy.wait_recv()
    lots, rest = nz * MULTI, CAP - MULTI

    def spread(k, carry):
        fold.unfold(er_v.at[k], eh)
        fold.unfold(eq_v.at[k], bh)
        rows = er_v[k, :, :dm]
        head = name_v[pl.ds(pl.multiple_of(k * CAP, CAP), MULTI), :]
        for p in range(3):
            at = pl.ds(pl.multiple_of(p * lots + k * MULTI, MULTI), MULTI)
            piece = rows.astype(BF16)
            rows_v[at, :] = piece
            names_v[at, :] = head
            rows = rows - piece.astype(F32)
        at = pl.ds(pl.multiple_of(3 * lots + k * rest, 16), rest)
        rows_v[at, :] = eq_v[k, :, :dm]
        names_v[at, :] = name_v[pl.ds(pl.multiple_of(k * CAP + MULTI, 16), rest), :]
        return carry

    lax.fori_loop(0, nz, spread, 0)

    parts = rows_v.shape[0]
    key = jnp.where(names_v[...] < 0.0, 2.0 * vocab, names_v[...])
    names_v[...] = key
    key = jnp.transpose(key)[0:1, :]
    rank_row = jnp.zeros((1, parts), F32)
    for i in range(parts // LANES):
        col = names_v[rows_at(i), :1]
        ahead = (col < key) | ((col == key) & earlier_than(LANES, parts, i * LANES))
        rank_row = rank_row + over_rows(jnp.sum, flags(ahead))
    for i in range(parts // LANES):
        hit = down(LANES, i * LANES).astype(F32) == rank_row
        tri_v[rows_at(i), :dm] = jnp.dot(one_hot(hit), rows_v[...], preferred_element_type=F32).astype(BF16)
        name = over_lanes(jnp.sum, jnp.where(hit, key, 0.0))
        names_v[rows_at(i), :] = jnp.broadcast_to(name, (LANES, LANES))
    which = across(LANES)
    bounds = jnp.zeros((1, LANES), F32)
    for b in range(PLACE_GRID + 1):
        before = over_lanes(jnp.sum, flags(key < b * (vocab // PLACE_GRID)))
        bounds = jnp.where(which == b, before, bounds)
    bounds_v[...] = bounds.astype(jnp.int32)
    for j, (src, dst) in enumerate(((tri_v.at[pl.ds(0, parts), pl.ds(0, fold.dp)], rows_ref), (names_v, names_ref), (bounds_v, bounds_ref))):
        keeps.append(pltpu.make_async_copy(src, dst, out_sem.at[3 + j]))
        keeps[-1].start()

    for w in range(PAIR):
        a, b = (last - 1, last - 2) if w == 0 else (last - 2, last - 1)
        part = grad_w(w, mine)
        with jax.named_scope(f'fin{w}'):
            sends[0][a].wait_recv()
            sends[1][b].wait_recv()
        rb_v[0, a] = rb_v[0, a] + rb_v[1, b]
        fold.unfold(rb_v.at[0, a], wh)
        dw_v[w] = rb_v[0, a, :, :dm] + part
        keeps.append(pltpu.make_async_copy(dw_v.at[w], (dup_ref, ddown_ref)[w], out_sem.at[6 + w]))
        keeps[-1].start()
    with jax.named_scope('exit_sends'):
        for copy in sent:
            copy.wait_send()
    with jax.named_scope('exit_keeps'):
        for copy in keeps:
            copy.wait()


def step(n, groups, ids, emb_t, up, down, grad_t, gain):
    nz = n // 2
    dm, vocab = emb_t.shape
    tl, fl = ids.shape[1], up.shape[0]
    tp = 2 * tl
    dp = Fold(dm).dp
    slots = nz * CAP
    parts = slots + 2 * nz * MULTI
    assert max(parts, dp) <= tp
    hops = nz - 1
    each, _, _ = shared_blocks(fl, groups)
    vmem, hbm = pl.BlockSpec(memory_space=pltpu.VMEM), pl.BlockSpec(memory_space=pl.ANY)
    dma = pltpu.SemaphoreType.DMA
    tokens = pltpu.VMEM((PAIR, dm, tl), BF16)
    return pl.pallas_call(
        functools.partial(step_kernel, n, groups),
        name='step',
        out_shape=(
            jax.ShapeDtypeStruct((dm, tl), BF16),
            jax.ShapeDtypeStruct((fl, dm), F32),
            jax.ShapeDtypeStruct((fl, dm), F32),
            jax.ShapeDtypeStruct((parts, dp), BF16),
            jax.ShapeDtypeStruct((parts, LANES), F32),
            jax.ShapeDtypeStruct((1, LANES), jnp.int32),
            jax.ShapeDtypeStruct((1, 1), F32),
        ),
        in_specs=[hbm] * 6,
        out_specs=(hbm,) * 7,
        scratch_shapes=[
            pltpu.VMEM((PAIR, nz, fl, dp), BF16),
            pltpu.VMEM((PAIR, PAIR, dm, tl), BF16),
            tokens,
            pltpu.VMEM((PAIR, PAIR, nz * fl, tl), BF16),
            pltpu.VMEM((PAIR, PAIR, fl, dp), F32),
            pltpu.VMEM((PAIR, hops, fl, dp), F32),
            pltpu.VMEM((dp, tl), F32),
            pltpu.VMEM((dp, tl), F32),
            pltpu.VMEM((dm, tl), F32),
            pltpu.VMEM((dm, tl), F32),
            tokens,
            pltpu.VMEM((nz, MULTI, dp), F32),
            pltpu.VMEM((nz, MULTI, dp), F32),
            pltpu.VMEM((nz, CAP - MULTI, dp), BF16),
            pltpu.VMEM((nz, CAP - MULTI, dp), BF16),
            pltpu.VMEM((nz, CAP, dp), BF16),
            pltpu.VMEM((nz, CAP, dp), BF16),
            pltpu.VMEM((PAIR, PAIR, slots, tl), BF16),
            pltpu.VMEM((tp, tp), BF16),
            pltpu.VMEM((PAIR, 1, tl), jnp.int32),
            pltpu.VMEM((2 * slots, LANES), F32),
            pltpu.VMEM((slots, LANES), F32),
            pltpu.VMEM((8, slots), F32),
            pltpu.VMEM((nz, 8, LANES), F32),
            pltpu.VMEM((nz, 8, LANES), F32),
            pltpu.VMEM((vocab // 512, dm, 512), BF16),
            pltpu.VMEM((dp, slots // 2), F32),
            pltpu.VMEM((dm, tl), BF16),
            pltpu.VMEM((parts, dm), BF16),
            pltpu.VMEM((1, dp), F32),
            pltpu.VMEM((dp, LANES), F32),
            pltpu.VMEM((PAIR, fl, dm), BF16),
            pltpu.VMEM((dm,), BF16),
            pltpu.VMEM((1, 1), F32),
            pltpu.VMEM((parts, LANES), F32),
            pltpu.VMEM((1, LANES), jnp.int32),
            pltpu.VMEM((PAIR, fl, dm), F32),
            pltpu.VMEM((nz, CAP, dp), BF16),
            dma((nz,)), dma((nz,)),
            dma((5,)), dma((vocab // 512,)), dma((PAIR, PAIR)), dma((PAIR, hops)),
            dma((PAIR, each, 2)), dma((PAIR, each, nz // 2)), dma((PAIR, each, groups - 1)), dma((3, each, groups - 1)),
            dma((5,)), dma((5,)), dma((hops,)), dma((hops,)), dma((hops,)),
            dma((PAIR, PAIR)), dma((PAIR, hops)), dma((PAIR, hops)), dma((9,)),
        ],
        compiler_params=pltpu.CompilerParams(
            collective_id=0, has_side_effects=True, vmem_limit_bytes=VMEM_LIMIT
        ),
    )(ids, emb_t, up, down, grad_t, gain)


def place_kernel(
    bounds_ref, names_hbm, rows_hbm, out_ref, up_ref, down_ref, emb_out, out_out, up_out, down_out,
    names_v, rows_v, emb_v, out_v, up_v, down_v, in_sem, emb_sem, out_sem,
):
    def load(i, src, dst):
        copy = pltpu.make_async_copy(src, dst, in_sem.at[i])
        copy.start()
        return copy

    needed = [load(0, names_hbm, names_v), load(1, rows_hbm, rows_v)]
    passing = ((out_ref, out_v, out_out), (up_ref, up_v, up_out), (down_ref, down_v, down_out))
    loads = [load(2 + j, src, via) for j, (src, via, _) in enumerate(passing)]
    dm, vocab = emb_v.shape
    block = vocab // PLACE_GRID
    last = rows_v.shape[0] // PLACE_ROWS - 1
    for copy in needed:
        copy.wait()

    def store(i):
        at = pl.ds(pl.multiple_of(i * block, LANES), block)
        return pltpu.make_async_copy(emb_v.at[:, at], emb_out.at[:, at], emb_sem.at[i])

    def fill(i, carry):
        to = pl.ds(pl.multiple_of(i * block, LANES), block)
        lo = jnp.minimum(bounds_ref[0, i] // PLACE_ROWS, last)
        hi = (bounds_ref[0, i + 1] + PLACE_ROWS - 1) // PLACE_ROWS

        def part(q):
            at = pl.ds(pl.multiple_of(q * PLACE_ROWS, PLACE_ROWS), PLACE_ROWS)
            return first_first(rows_v[at, :dm], one_hot(names_v[at, :1] == across(block, i * block).astype(F32)))

        emb_v[:, to] = part(lo)

        def more(q, inner):
            emb_v[:, to] = emb_v[:, to] + part(q)
            return inner

        lax.fori_loop(lo + 1, hi, more, 0)
        store(i).start()
        return carry

    lax.fori_loop(0, PLACE_GRID, fill, 0)
    keeps = []
    for j, (_, via, dst) in enumerate(passing):
        loads[j].wait()
        keeps.append(pltpu.make_async_copy(via, dst, out_sem.at[j]))
        keeps[-1].start()
    for i in range(PLACE_GRID):
        store(i).wait()
    for copy in keeps:
        copy.wait()


def place(vocab, bounds, names, rows, out, d_up, d_down):
    hbm = pl.BlockSpec(memory_space=pl.ANY)
    emb = jax.ShapeDtypeStruct((out.shape[0], vocab), F32)
    results = (emb,) + tuple(jax.ShapeDtypeStruct(a.shape, a.dtype) for a in (out, d_up, d_down))
    dma = pltpu.SemaphoreType.DMA
    return pl.pallas_call(
        place_kernel,
        name='place',
        out_shape=results,
        in_specs=[pl.BlockSpec(memory_space=pltpu.SMEM)] + [hbm] * 5,
        out_specs=(hbm,) * 4,
        scratch_shapes=[pltpu.VMEM(a.shape, a.dtype) for a in (names, rows) + results]
        + [dma((5,)), dma((PLACE_GRID,)), dma((3,))],
        compiler_params=pltpu.CompilerParams(vmem_limit_bytes=VMEM_LIMIT),
    )(bounds, names, rows, out, d_up, d_down)


def swap_kernel(n, src_ref, dst_ref, keep_sem, send_sem, recv_sem):
    me = lax.axis_index('tensor')
    sem = pltpu.get_barrier_semaphore()
    for d in range(1, n):
        pl.semaphore_signal(sem, device_id={'tensor': lax.rem(me + d, n)}, device_id_type=MESH)
    pl.semaphore_wait(sem, n - 1)
    keep = pltpu.make_async_copy(src_ref.at[me], dst_ref.at[me], keep_sem)
    keep.start()
    copies = []
    for d in range(1, n):
        to = lax.rem(me + d, n)
        copies.append(remote(src_ref.at[to], dst_ref.at[me], send_sem.at[d], recv_sem.at[d], {'tensor': to}))
        copies[-1].start()
    for copy in copies:
        copy.wait()
    keep.wait()


def swap_blocks(n, blocks, collective_id):
    hbm = pl.BlockSpec(memory_space=pl.ANY)
    return pl.pallas_call(
        functools.partial(swap_kernel, n),
        name='swap_blocks',
        out_shape=jax.ShapeDtypeStruct(blocks.shape, blocks.dtype),
        in_specs=[hbm],
        out_specs=hbm,
        scratch_shapes=[pltpu.SemaphoreType.DMA, pltpu.SemaphoreType.DMA((n,)), pltpu.SemaphoreType.DMA((n,))],
        compiler_params=pltpu.CompilerParams(collective_id=collective_id, has_side_effects=True),
    )(blocks)


def all_blocks(n, block, collective_id):
    return swap_blocks(n, jnp.broadcast_to(block[None], (n,) + block.shape), collective_id)


def rms_norm(x_rows, gain_f):
    inv_rms = lax.rsqrt(jnp.mean(x_rows * x_rows, axis=-1, keepdims=True) + EPS)
    return x_rows * inv_rms * gain_f


def dense_step(n, ids, emb, norm_gain, up, down, grad_out):
    vocab, dm = emb.shape
    fl = up.shape[0]
    base = (lax.axis_index('tensor') * vocab).astype(F32)
    ids_all = all_blocks(n, jnp.broadcast_to(ids.astype(F32), (8, ids.shape[1])), 1)[:, 0]
    hot = (iota((ids_all.size, vocab), 1).astype(F32) == ids_all.reshape(-1, 1) - base).astype(BF16)
    part = jnp.dot(hot, emb, preferred_element_type=F32).astype(BF16)
    x_f = jnp.sum(swap_blocks(n, part.reshape(n, -1, dm), 2).astype(F32), axis=0)
    ws = all_blocks(n, jnp.stack([up, down]), 3)
    up_all, down_all = ws[:, 0].reshape(-1, dm), ws[:, 1].reshape(-1, dm)
    normed_f, norm_back = jax.vjp(lambda x_in: rms_norm(x_in, norm_gain.astype(F32)), x_f)
    normed = normed_f.astype(BF16)
    pre_act = last_last(normed, up_all).astype(BF16).astype(F32)
    act_f, slope = gelu_pair(pre_act)
    hidden = act_f.astype(BF16)
    d_pre = (last_last(grad_out, down_all) * slope).astype(BF16)
    y = jnp.dot(hidden, down_all, preferred_element_type=F32)
    out = (x_f + y).astype(BF16)
    d_norm = jnp.dot(d_pre, up_all, preferred_element_type=F32)
    dx = (grad_out.astype(F32) + norm_back(d_norm)[0]).astype(BF16)
    d_w = jnp.stack([first_first(d_pre, normed), first_first(hidden, grad_out)]).reshape(PAIR, n, fl, dm)
    d_w = jnp.sum(swap_blocks(n, jnp.moveaxis(d_w, 1, 0), 4), axis=0)
    dx_all = all_blocks(n, dx, 5).reshape(-1, dm)
    hot_t = (iota((vocab, ids_all.size), 0).astype(F32) == ids_all.reshape(1, -1) - base).astype(BF16)
    d_emb = jnp.dot(hot_t, dx_all, preferred_element_type=F32)
    return d_emb.T, out.T, d_w[0], d_w[1]


def solution(mesh):
    n, groups = mesh.shape['tensor'], mesh.shape['data']
    tok_spec = P(('data', 'tensor'))
    row_spec = P(('data', 'tensor'), None)

    def local_step(token_ids, emb_shard, norm_gain, w_up, w_down, grad_out):
        vocab, dm = emb_shard.shape
        ids, gain, up = token_ids[None, :], norm_gain, w_up.T
        out, d_up, d_down, rows, names, bounds, flag = step(n, groups, ids, emb_shard.T, up, w_down, grad_out.T, gain)
        placed = place(vocab, bounds, names, rows, out, d_up, d_down)

        def again(state):
            return (jnp.zeros((), F32),) + dense_step(n, ids, emb_shard, norm_gain, up, w_down, grad_out)

        state = lax.while_loop(lambda state: state[0] > 0.5, again, (flag[0, 0],) + tuple(placed))
        _, d_emb, out, d_up, d_down = state
        return out.T, d_emb.T, d_up.T, d_down

    return jax.shard_map(
        local_step,
        mesh=mesh,
        in_specs=(tok_spec, P('tensor', None), P(None), P(None, 'tensor'), P('tensor', None), row_spec),
        out_specs=(row_spec, row_spec, P('data', 'tensor'), row_spec),
        check_vma=False,
    )
```

```python
import functools
import math

import jax
import jax.numpy as jnp
from jax import lax
from jax.experimental import pallas as pl
from jax.experimental.pallas import tpu as pltpu
from jax.sharding import PartitionSpec as P

EPS = 1e-6
CAP = 64
MULTI = 16
PAIR = 2
BHEAD = 32
PLACE_GRID = 6
PLACE_ROWS = 256
LANES = 128
MESH = pl.DeviceIdType.MESH
VMEM_LIMIT = 67_000_000
F32 = jnp.float32
BF16 = jnp.bfloat16
SQRT_2_PI = 0.7978845608028654
CUBIC = 0.044715


def contract(left_op, right_op, left_dim, right_dim):
    dims = (((left_dim,), (right_dim,)), ((), ()))
    return lax.dot_general(left_op, right_op, dims, preferred_element_type=F32)


def first_first(left_op, right_op):
    return contract(left_op, right_op, 0, 0)


def last_last(left_op, right_op):
    return contract(left_op, right_op, 1, 1)


def iota(shape, dim):
    return lax.broadcasted_iota(jnp.int32, shape, dim)


def down(rows, start=0):
    return iota((rows, 1), 0) + start


def across(lanes, start=0):
    return iota((1, lanes), 1) + start


def flags(mask):
    return jnp.where(mask, 1.0, 0.0)


def one_hot(mask):
    return flags(mask).astype(BF16)


def over_rows(reduce, value):
    return reduce(value, axis=0, keepdims=True)


def over_lanes(reduce, value):
    return reduce(value, axis=1, keepdims=True)


def earlier_than(rows, lanes, start):
    return down(rows, start) < across(lanes)


def gelu_pair(u):
    t = jnp.tanh(SQRT_2_PI * (u + CUBIC * (u * u * u)))
    cdf = 0.5 * (1.0 + t)
    slope = cdf + u * (0.5 * (1.0 - t * t)) * (SQRT_2_PI * (1.0 + (3.0 * CUBIC) * (u * u)))
    return u * cdf, slope


def rows_at(i):
    return slice(i * LANES, (i + 1) * LANES)


class Ring:
    def __init__(self, n, groups):
        self.n, self.nz, self.half, self.groups = n, n // 2, n // 4, groups
        self.me = lax.axis_index('tensor')
        self.g = lax.axis_index('data')
        self.c = lax.rem(self.me, 2)
        self.z = self.me // 2

    def chip(self, k):
        return lax.rem(self.z + (k + self.nz) % self.nz, self.nz)

    def dev(self, k):
        return {'tensor': 2 * self.chip(k) + self.c}

    def twin(self, e):
        return {'data': lax.rem(self.g + e, self.groups), 'tensor': self.me}

    @property
    def sibling(self):
        return {'tensor': self.me + 1 - 2 * self.c}

    def greet(self):
        sem = pltpu.get_barrier_semaphore()
        for k in range(1, self.nz):
            pl.semaphore_signal(sem, device_id=self.dev(k), device_id_type=MESH)
        pl.semaphore_signal(sem, device_id=self.sibling, device_id_type=MESH)
        for e in range(1, self.groups):
            pl.semaphore_signal(sem, device_id=self.twin(e), device_id_type=MESH)

    def meet(self):
        pl.semaphore_wait(pltpu.get_barrier_semaphore(), self.nz + self.groups - 1)


def slot_of(nz):
    half = nz // 2
    order = [half] + [s * k for k in range(half - 1, 0, -1) for s in (1, -1)] + [0]
    table = {k: i for i, k in enumerate(order)}
    table[-half] = table[half]
    return table


def gather_messages(half):
    right = [(w, k) for k in range(half) for w in (0, 1) if w == 0 or k < half - 1]
    return right, [(1 - w, k) for w, k in right]


BLOCK = 16


def shared_blocks(fl, groups):
    shared = fl - 2 * BLOCK
    count = 2 if groups * BLOCK <= shared else 1
    height = 2 * shared // (groups * count)
    assert height % BLOCK == 0 and height * groups * count == 2 * shared
    return count, height, shared


def far_first(nz):
    half = nz // 2
    far = [half] + [half + s * k for k in range(1, half) for s in (-1, 1)]
    return far[:half - 1] + [0] + far[half - 1:]


def scatter_messages(half):
    right = [(0, half)]
    for k in range(half - 1, 0, -1):
        right += [(1, k), (0, k)]
    return right, [(1 - w, -k) for w, k in right]


def remote(src, dst, send_sem, recv_sem, device):
    return pltpu.make_async_remote_copy(
        src_ref=src, dst_ref=dst, send_sem=send_sem, recv_sem=recv_sem, device_id=device, device_id_type=MESH
    )


class Fold:
    def __init__(self, dm):
        self.dm = dm
        self.lo = dm // LANES * LANES
        self.dp = self.lo + LANES
        assert 2 * (dm - self.lo) == LANES

    def tail(self, value, h):
        low = value.shape[0] - h
        return jnp.concatenate([value[:low, self.lo:self.dm], value[h:, self.lo:self.dm]], axis=1)

    def store(self, ref, value, h):
        low = value.shape[0] - h
        ref[:, :self.lo] = value[:, :self.lo]
        ref[:low, self.lo:] = self.tail(value, h)
        if low < h:
            ref[low:h, self.lo:self.dm] = value[low:h, self.lo:self.dm]

    def add(self, ref, value, h):
        low = value.shape[0] - h
        ref[:, :self.lo] = ref[:, :self.lo] + value[:, :self.lo]
        ref[:low, self.lo:] = ref[:low, self.lo:] + self.tail(value, h)

    def unfold(self, ref, h):
        low = ref.shape[0] - h
        ref[h:, self.lo:self.dm] = ref[:low, self.dm:self.dp]

    def parts(self, src, dst, h, device):
        low = src.shape[0] - h
        areas = ((pl.ds(0, h), pl.ds(0, self.dp)), (pl.ds(h, low), pl.ds(0, self.lo)))
        return [(src.at[area], dst.at[area], device) for area in areas]

    def send(self, src, dst, h, send_sem, recv_sem, device):
        return Batch(self.parts(src, dst, h, device), self.spare, send_sem, recv_sem)


class Batch:
    def __init__(self, parts, spare, send_sem, recv_sem):
        self.copies = [remote(src, dst, send_sem, recv_sem, device) for src, dst, device in parts]
        dtype = jnp.dtype(parts[0][0].dtype)
        size = sum(math.prod(src.shape) for src, _, _ in parts)
        ref = spare[dtype]
        tile = 8 * 4 // dtype.itemsize
        width = next(w for w in range(LANES, ref.shape[1] + 1, LANES)
                     if size % (w * tile) == 0 and size // w <= ref.shape[0])
        whole = ref.at[pl.ds(0, size // width), pl.ds(0, width)]
        self.whole = remote(whole, whole, send_sem, recv_sem, parts[0][2])

    def start(self):
        for copy in self.copies:
            copy.start()

    def wait_recv(self):
        self.whole.wait_recv()

    def wait_send(self):
        self.whole.wait_send()


def step_kernel(
    n, groups, ids_ref, emb_ref, up_ref, down_ref, grad_ref, gain_ref,
    out_ref, dup_ref, ddown_ref, rows_ref, names_ref, bounds_ref, flag_ref,
    w_v, gn_v, x_v, hd_v, st_v, rb_v, snd_v, own_v, dnr_v, yr_v, dx_v, es_v, er_v, eb_v, eq_v, xs_v, xr_v,
    pick_v, tri_v, ids_v, col_v, name_v, nrow_v, req_s, req_r, emb_v, found_v, out_v, rows_v, row_v, gain_v,
    own_w, line_v, flag_v, names_v, bounds_v, dw_v, xo_v, xf_sem, xg_sem,
    ld_sem, emb_sem, ws_sem, wr_sem, bs_sem, br_sem, ts_sem, tr_sem, ps_sem, pr_sem, qs_sem, gs_sem, xr_sem,
    ss_sem, sr_sem, es_sem, er_sem, out_sem,
):
    ring = Ring(n, groups)
    nz, half, c, z = ring.nz, ring.half, ring.c, ring.z
    slot = slot_of(nz)
    dm, vocab = emb_ref.shape
    fl = up_ref.shape[0]
    each, height, shared = shared_blocks(fl, groups)
    order = far_first(nz)
    back = [order.index((nz - d) % nz) for d in order]
    own = order.index(0)
    others = [(p, d) for p, d in enumerate(order) if d]
    part_of = nz // 2
    tl = ids_ref.shape[1]
    tp = 2 * tl
    slots = nz * CAP
    fold = Fold(dm)
    fold.spare = {jnp.dtype(BF16): tri_v, jnp.dtype(F32): own_v}
    wh, xh, eh, bh = fl // 2, CAP // 2, MULTI // 2, BHEAD
    gh = (fl - shared) // 2
    ring_rows = pl.ds(shared, fl - shared)
    step = emb_v.shape[2]
    sides = ((0, 1), (1, -1))
    sent = []

    ring.greet()
    own_ids = pltpu.make_async_copy(ids_ref, ids_v.at[c], ld_sem.at[1])
    load_w = [pltpu.make_async_copy(ref, own_w.at[w], ld_sem.at[2 + w]) for w, ref in enumerate((up_ref, down_ref))]
    load_gain = pltpu.make_async_copy(gain_ref, line_v, ld_sem.at[4])
    load_grad = pltpu.make_async_copy(grad_ref, gn_v.at[1, c], ld_sem.at[0])
    for copy in [own_ids, load_gain] + load_w + [load_grad]:
        copy.start()

    def load_emb(i):
        at = pl.ds(pl.multiple_of(i * step, step), step)
        return pltpu.make_async_copy(emb_ref.at[:, at], emb_v.at[i], emb_sem.at[i])

    for i in range(vocab // step):
        load_emb(i).start()
    mine = slot[0]
    for w in range(PAIR):
        load_w[w].wait()
        w_v[w, mine, :, :dm] = own_w[w]
        w_v[w, mine, shared:shared + gh, dm:] = own_w[w, shared + gh:, fold.lo:]
    own_ids.wait()
    with jax.named_scope('barrier'):
        ring.meet()

    def start(copy, after=None):
        if after is not None:
            after.wait_send()
            sent[:] = [other for other in sent if other is not after]
        copy.start()
        sent.append(copy)
        return copy

    blocks = []
    for j in range(each):
        b = ring.g * each + j
        blocks.append((lax.rem(b, PAIR), pl.ds(pl.multiple_of(height * (b // 2), BLOCK), height)))

    def hops(k):
        parts = [
            (w_v.at[w, slot[-k * sign], at], w_v.at[w, slot[-(k + 1) * sign], at], ring.dev(sign))
            for j, (w, at) in enumerate(blocks) for side, sign in sides if k < half - 1 or side == j % 2
        ]
        return Batch(parts, fold.spare, bs_sem.at[k % 2], br_sem.at[k])

    stages = ((nz - 3, nz - 1), (nz - 5, nz - 3), (0, nz - 5))

    def twins(stage):
        lo, hi = stages[stage]
        refs = [w_v.at[w, pl.ds(lo, hi - lo), at] for w, at in blocks]
        parts = [(ref, ref, ring.twin(e)) for ref in refs for e in range(1, groups)]
        return Batch(parts, fold.spare, ts_sem.at[stage % 2], tr_sem.at[stage])

    block_moves = [hops(k) for k in range(half)]
    twin_moves = [twins(stage) for stage in range(len(stages))]

    def relay(k, stage):
        with jax.named_scope(f'relay{k}'):
            block_moves[k].wait_recv()
            if k + 1 < half:
                start(block_moves[k + 1], block_moves[k - 1] if k >= 1 else None)
            if stage is not None:
                start(twin_moves[stage], twin_moves[stage - 2] if stage >= 2 else None)

    def from_twins(stage):
        with jax.named_scope(f'twins{stage}'):
            twin_moves[stage].wait_recv()

    start(block_moves[0])
    swap_ids = start(remote(ids_v.at[c], ids_v.at[c], ps_sem.at[0], pr_sem.at[0], ring.sibling))
    moves = [[], []]
    for side, sign in sides:
        for i, (w, k) in enumerate(gather_messages(half)[side]):
            src, dst = w_v.at[w, slot[-k * sign], ring_rows], w_v.at[w, slot[-(k + 1) * sign], ring_rows]
            moves[side].append(fold.send(src, dst, gh, ws_sem.at[side, i % 2], wr_sem.at[side, i], ring.dev(sign)))

    def forward(i):
        with jax.named_scope(f'fwd{i}'):
            for side, sign in sides:
                moves[side][i].wait_recv()
                if i + 2 < len(moves[side]):
                    start(moves[side][i + 2], moves[side][i])
                w, k = gather_messages(half)[side][i]
                fold.unfold(w_v.at[w, slot[-(k + 1) * sign], ring_rows], gh)

    with jax.named_scope('ids_wait'):
        swap_ids.wait_recv()
    ids = jnp.concatenate([ids_v[0], ids_v[1]], axis=1).astype(F32)
    ids_t = jnp.transpose(jnp.broadcast_to(ids, (LANES, tp)))
    seen = jnp.zeros((1, tp), F32)
    total = jnp.zeros((1, tp), F32)
    for i in range(tp // LANES):
        tri = flags(earlier_than(LANES, tp, i * LANES))
        same = flags(ids_t[rows_at(i), :1] == ids)
        seen = jnp.maximum(seen, over_rows(jnp.max, same * tri))
        total = total + over_rows(jnp.sum, same)
    row = down(n)
    place = lax.rem(row, nz)
    chip = lax.rem(z + sum(jnp.where(place == p, d, 0) for p, d in others), nz)
    owner = 2 * chip + jnp.where(row < nz, c, 1 - c)
    base = (owner * vocab).astype(F32)
    member = flags((seen < 0.5) & (ids >= base) & (ids < base + vocab))
    multi = flags(total > 1.5)
    several, single = member * multi, member * (1.0 - multi)
    both = jnp.concatenate([several, single], axis=0)
    tri = one_hot(earlier_than(LANES, LANES, 0))
    before = jnp.zeros((2 * n, 1), F32)
    ranks = []
    for i in range(tp // LANES):
        some = both[:, rows_at(i)]
        ranks.append(before + jnp.dot(some.astype(BF16), tri, preferred_element_type=F32))
        before = before + over_lanes(jnp.sum, some)
    rank = jnp.concatenate(ranks, axis=1)
    n_several, count = before[:n], before[:n] + before[n:]
    rank = jnp.where(several > 0.5, rank[:n], n_several + rank[n:])
    over = over_rows(jnp.max, flags((count > CAP) | (n_several > MULTI)))
    for k in range(n):
        hit = (rank[k:k + 1, :] == down(CAP).astype(F32)) & (member[k:k + 1, :] > 0.5)
        col = over_lanes(jnp.max, jnp.where(hit, ids, -1.0))
        col_v[k * CAP:(k + 1) * CAP, :] = jnp.broadcast_to(col, (CAP, LANES))
    cols_t = jnp.transpose(col_v[:slots, :])
    lane = iota((8, LANES), 1)
    per = LANES // CAP
    for k in range(nz):
        at = (k // per) * LANES
        tile = cols_t[0:8, at:at + LANES]
        if k % per:
            tile = pltpu.roll(tile, LANES - (k % per) * CAP, 1)
        req_s[k] = jnp.where(lane < CAP, tile, over)
    parts = [(req_s.at[p], req_r.at[back[p]], ring.dev(d)) for p, d in others]
    asks = start(Batch(parts, fold.spare, qs_sem.at[0], qs_sem.at[1]))
    relay(0, 0)
    for i in range(PAIR):
        for side, _ in sides:
            start(moves[side][i])
    swap_grad = start(remote(grad_ref, gn_v.at[1, c], ps_sem.at[1], pr_sem.at[1], ring.sibling))
    req_r[own] = req_s[own]
    for q in range(PAIR):
        for t in range(PAIR):
            pick_v[q, t] = one_hot(col_v[q * slots:(q + 1) * slots, :1] == ids[:, t * tl:(t + 1) * tl])

    with jax.named_scope('asks_wait'):
        asks.wait_recv()
    flag = req_r[0]
    for k in range(1, nz):
        flag = jnp.maximum(flag, req_r[k])
    flag_v[...] = over_rows(jnp.max, over_lanes(jnp.max, jnp.where(lane < CAP, 0.0, flag)))
    keeps = [pltpu.make_async_copy(flag_v, flag_ref, out_sem.at[2])]
    keeps[0].start()
    tiles = []
    for p in range(nz // per):
        tile = req_r[p * per]
        for j in range(1, per):
            tile = jnp.where(lane < j * CAP, tile, pltpu.roll(req_r[p * per + j], j * CAP, 1))
        tiles.append(tile)
    names = jnp.concatenate(tiles, axis=1) - (ring.me * vocab).astype(F32)
    nrow_v[...] = names
    name_v[...] = jnp.transpose(jnp.broadcast_to(names[0:1, :], (LANES, slots)))
    gives = {}
    handed = []

    def find(part):
        cols = slice(part * slots // 2, (part + 1) * slots // 2)
        found_v[...] = jnp.zeros_like(found_v)

        def body(i, carry):
            if part == 0:
                load_emb(i).wait()
            hot = one_hot(down(step, i * step).astype(F32) == nrow_v[:1, cols])
            found_v[:dm, :] = found_v[:dm, :] + jnp.dot(emb_v[i], hot, preferred_element_type=F32)
            return carry

        with jax.named_scope(f'find{part}'):
            lax.fori_loop(0, vocab // step, body, 0)
        found = jnp.transpose(found_v[...])[:, :dm].astype(BF16)
        for q in range(nz // 2):
            fold.store(xs_v.at[part * nz // 2 + q], found[q * CAP:(q + 1) * CAP, :], xh)

    def give(part):
        at = range(part * part_of, (part + 1) * part_of)
        parts = [area for p in at for area in fold.parts(xr_v.at[p], xo_v.at[p], xh, ring.sibling)]
        handed.append(Batch(parts, fold.spare, xf_sem.at[part], xg_sem.at[part]))
        sent.append(handed[part])
        for p in at:
            if order[p]:
                to = ring.dev(order[p])
                gives[p] = start(fold.send(xs_v.at[p], xr_v.at[back[p]], xh, gs_sem.at[p], xr_sem.at[p], to))
            else:
                xr_v[p] = xs_v[p]
                hand(p)

    def hand(p):
        for copy in handed[p // part_of].copies[2 * (p % part_of):2 * (p % part_of) + 2]:
            copy.start()

    relay(1, 1)
    find(0)
    relay(2, None)
    forward(0)
    give(0)
    find(1)
    forward(1)
    give(1)
    row_v[...] = jnp.zeros_like(row_v)
    load_gain.wait()
    row_v[:, :dm] = line_v[...].astype(F32).reshape(1, dm)
    gain_v[...] = jnp.transpose(jnp.broadcast_to(row_v[...], (LANES, fold.dp)))
    relay(3, 2)
    forward(2)

    def arrived(part):
        with jax.named_scope(f'gives_wait{part}'):
            for p in range(part * part_of, (part + 1) * part_of):
                if order[p]:
                    gives[p].wait_recv()
                    hand(back[p])

    def unpack(rows_of, q, part):
        at = slice(part * part_of, (part + 1) * part_of)
        for p in range(part * part_of, (part + 1) * part_of):
            fold.unfold(rows_of.at[p], xh)
        rows = rows_of[at].reshape(part_of * CAP, fold.dp)[:, :dm]
        picks = slice(part * part_of * CAP, (part + 1) * part_of * CAP)
        for t in range(PAIR):
            value = first_first(rows, pick_v[q, t, picks]).astype(BF16)
            x_v[t] = x_v[t] + value if q or part else value

    def from_sibling(part):
        with jax.named_scope(f'sibling_wait{part}'):
            handed[part].wait_recv()
        unpack(xo_v, 1, part)

    arrived(0)
    unpack(xr_v, 0, 0)
    from_sibling(0)
    arrived(1)
    forward(3)
    unpack(xr_v, 0, 1)
    forward(4)
    load_grad.wait()
    swap_grad.wait_recv()
    from_sibling(1)

    def lanes(b):
        return pl.ds(pl.multiple_of(b * LANES, LANES), LANES)

    def norm(i, carry):
        t, at = i // (tl // LANES), lanes(lax.rem(i, tl // LANES))
        xf = x_v[t, :, at].astype(F32)
        inv = lax.rsqrt(over_rows(jnp.mean, xf * xf) + EPS)
        gn_v[0, t, :, at] = (xf * inv * gain_v[:dm, :]).astype(BF16)
        return carry

    lax.fori_loop(0, tp // LANES, norm, 0)

    def hidden(lo, hi):
        def body(i, carry):
            s, t = lo + i // 2, lax.rem(i, PAIR)
            u = jnp.dot(w_v[0, s, :, :dm], gn_v[0, t], preferred_element_type=F32).astype(BF16).astype(F32)
            dh = jnp.dot(w_v[1, s, :, :dm], gn_v[1, t], preferred_element_type=F32)
            act, slope = gelu_pair(u)
            at = pl.ds(pl.multiple_of(s * fl, fl), fl)
            hd_v[1, t, at, :] = act.astype(BF16)
            hd_v[0, t, at, :] = (dh * slope).astype(BF16)
            return carry

        with jax.named_scope(f'hid{lo}'):
            lax.fori_loop(0, 2 * (hi - lo), body, 0)

    def grad_w(w, s):
        at = pl.ds(pl.multiple_of(s * fl, fl), fl)
        return last_last(hd_v[w, 0, at, :], gn_v[w, 0]) + last_last(hd_v[w, 1, at, :], gn_v[w, 1])

    orders = scatter_messages(half)
    sends = [[], []]
    for side, sign in sides:
        for i in range(len(orders[0])):
            src = st_v.at[side, i] if i < 2 else rb_v.at[side, i - 2]
            dst = rb_v.at[side, i]
            sends[side].append(fold.send(src, dst, wh, ss_sem.at[side, i % 2], sr_sem.at[side, i], ring.dev(sign)))

    def scatter(i):
        with jax.named_scope(f'scat{i}'):
            (w0, k0), (_, k1) = orders[0][i], orders[1][i]
            if i >= 2:
                for side, _ in sides:
                    sends[side][i - 2].wait_recv()

            def body(side, carry):
                w = w0 + side * (1 - 2 * w0)
                part = grad_w(w, slot[k0] + side * (slot[k1] - slot[k0]))
                if i < 2:
                    fold.store(st_v.at[side, i], part, wh)
                else:
                    fold.add(rb_v.at[side, i - 2], part, wh)
                return carry

            if i:
                lax.fori_loop(0, 2, body, 0)
            for side, _ in sides:
                if i == 0:
                    body(side, 0)
                start(sends[side][i], sends[side][i - 2] if i >= 2 else None)

    forward(5)
    forward(6)
    for stage in range(len(stages)):
        from_twins(stage)
    hidden(0, 1)
    scatter(0)
    hidden(1, nz - 5)
    scatter(1)
    hidden(nz - 5, nz)

    wide = 2 * LANES

    def through(w, t, dst):
        def body(b, carry):
            at = pl.ds(pl.multiple_of(b * wide, wide), wide)
            left = w_v[w, :, :, at].reshape(nz * fl, wide)
            dst[at, :] = first_first(left, hd_v[w_of_hd[w], t])
            return carry

        lax.fori_loop(0, fold.dp // wide, body, 0)

    w_of_hd = (0, 1)
    with jax.named_scope('thru'):
        through(0, 1 - c, snd_v)
    body_rows = pl.ds(0, dm)
    swap_dn = remote(snd_v.at[body_rows], dnr_v, ps_sem.at[2], pr_sem.at[2], ring.sibling)
    swap_dn.start()
    through(0, c, own_v)
    scatter(2)
    with jax.named_scope('swapdn_wait'):
        swap_dn.wait_send()
        swap_dn.wait_recv()

    def dx_block(b, carry):
        at = lanes(b)
        xf = x_v[c, :, at].astype(F32)
        inv = lax.rsqrt(over_rows(jnp.mean, xf * xf) + EPS)
        q = (own_v[:dm, at] + dnr_v[:, at]) * gain_v[:dm, :]
        dot = over_rows(jnp.mean, xf * q)
        dxn = inv * q - xf * (inv * inv * inv * dot)
        dx_v[c, :, at] = (gn_v[1, c, :, at].astype(F32) + dxn).astype(BF16)
        return carry

    lax.fori_loop(0, tl // LANES, dx_block, 0)
    swap_dx = start(remote(dx_v.at[c], dx_v.at[c], ps_sem.at[3], pr_sem.at[3], ring.sibling))
    through(1, 1 - c, snd_v)
    swap_y = start(remote(snd_v.at[body_rows], yr_v, ps_sem.at[4], pr_sem.at[4], ring.sibling))
    with jax.named_scope('swapdx_wait'):
        swap_dx.wait_recv()

    def pack(k, carry):
        at = pl.ds(pl.multiple_of(k * CAP, CAP), CAP)
        rows = last_last(pick_v[0, 0, at, :], dx_v[0]) + last_last(pick_v[0, 1, at, :], dx_v[1])
        fold.store(es_v.at[k], rows[:MULTI], eh)
        fold.store(eb_v.at[k], rows[MULTI:].astype(BF16), bh)
        return carry

    lax.fori_loop(0, nz, pack, 0)
    backs = []
    for kind, (src, dst, h) in enumerate(((es_v, er_v, eh), (eb_v, eq_v, bh))):
        parts = [area for p, d in others for area in fold.parts(src.at[p], dst.at[back[p]], h, ring.dev(d))]
        backs.append(start(Batch(parts, fold.spare, es_sem.at[kind], er_sem.at[kind])))
    er_v[own] = es_v[own]
    eq_v[own] = eb_v[own]
    through(1, c, own_v)
    scatter(3)
    with jax.named_scope('swapy_wait'):
        swap_y.wait_recv()

    def out_block(b, carry):
        at = lanes(b)
        out_v[:, at] = (x_v[c, :, at].astype(F32) + (own_v[:dm, at] + yr_v[:, at])).astype(BF16)
        return carry

    lax.fori_loop(0, tl // LANES, out_block, 0)
    keeps.append(pltpu.make_async_copy(out_v, out_ref, out_sem.at[0]))
    keeps[-1].start()
    last = len(orders[0])
    for i in range(4, last):
        scatter(i)

    with jax.named_scope('backs_wait'):
        for copy in backs:
            copy.wait_recv()
    lots, rest = nz * MULTI, CAP - MULTI

    def spread(k, carry):
        fold.unfold(er_v.at[k], eh)
        fold.unfold(eq_v.at[k], bh)
        rows = er_v[k, :, :dm]
        head = name_v[pl.ds(pl.multiple_of(k * CAP, CAP), MULTI), :]
        for p in range(3):
            at = pl.ds(pl.multiple_of(p * lots + k * MULTI, MULTI), MULTI)
            piece = rows.astype(BF16)
            rows_v[at, :] = piece
            names_v[at, :] = head
            rows = rows - piece.astype(F32)
        at = pl.ds(pl.multiple_of(3 * lots + k * rest, 16), rest)
        rows_v[at, :] = eq_v[k, :, :dm]
        names_v[at, :] = name_v[pl.ds(pl.multiple_of(k * CAP + MULTI, 16), rest), :]
        return carry

    lax.fori_loop(0, nz, spread, 0)

    parts = rows_v.shape[0]
    key = jnp.where(names_v[...] < 0.0, 2.0 * vocab, names_v[...])
    names_v[...] = key
    key = jnp.transpose(key)[0:1, :]
    rank_row = jnp.zeros((1, parts), F32)
    for i in range(parts // LANES):
        col = names_v[rows_at(i), :1]
        ahead = (col < key) | ((col == key) & earlier_than(LANES, parts, i * LANES))
        rank_row = rank_row + over_rows(jnp.sum, flags(ahead))
    for i in range(parts // LANES):
        hit = down(LANES, i * LANES).astype(F32) == rank_row
        tri_v[rows_at(i), :dm] = jnp.dot(one_hot(hit), rows_v[...], preferred_element_type=F32).astype(BF16)
        name = over_lanes(jnp.sum, jnp.where(hit, key, 0.0))
        names_v[rows_at(i), :] = jnp.broadcast_to(name, (LANES, LANES))
    which = across(LANES)
    bounds = jnp.zeros((1, LANES), F32)
    for b in range(PLACE_GRID + 1):
        before = over_lanes(jnp.sum, flags(key < b * (vocab // PLACE_GRID)))
        bounds = jnp.where(which == b, before, bounds)
    bounds_v[...] = bounds.astype(jnp.int32)
    for j, (src, dst) in enumerate(((tri_v.at[pl.ds(0, parts), pl.ds(0, fold.dp)], rows_ref), (names_v, names_ref), (bounds_v, bounds_ref))):
        keeps.append(pltpu.make_async_copy(src, dst, out_sem.at[3 + j]))
        keeps[-1].start()

    for w in range(PAIR):
        a, b = (last - 1, last - 2) if w == 0 else (last - 2, last - 1)
        part = grad_w(w, mine)
        with jax.named_scope(f'fin{w}'):
            sends[0][a].wait_recv()
            sends[1][b].wait_recv()
        rb_v[0, a] = rb_v[0, a] + rb_v[1, b]
        fold.unfold(rb_v.at[0, a], wh)
        dw_v[w] = rb_v[0, a, :, :dm] + part
        keeps.append(pltpu.make_async_copy(dw_v.at[w], (dup_ref, ddown_ref)[w], out_sem.at[6 + w]))
        keeps[-1].start()
    with jax.named_scope('exit_sends'):
        for copy in sent:
            copy.wait_send()
    with jax.named_scope('exit_keeps'):
        for copy in keeps:
            copy.wait()


def step(n, groups, ids, emb_t, up, down, grad_t, gain):
    nz = n // 2
    dm, vocab = emb_t.shape
    tl, fl = ids.shape[1], up.shape[0]
    tp = 2 * tl
    dp = Fold(dm).dp
    slots = nz * CAP
    parts = slots + 2 * nz * MULTI
    assert max(parts, dp) <= tp
    hops = nz - 1
    hbm = pl.BlockSpec(memory_space=pl.ANY)
    dma = pltpu.SemaphoreType.DMA
    tokens = pltpu.VMEM((PAIR, dm, tl), BF16)
    return pl.pallas_call(
        functools.partial(step_kernel, n, groups),
        name='step',
        out_shape=(
            jax.ShapeDtypeStruct((dm, tl), BF16),
            jax.ShapeDtypeStruct((fl, dm), F32),
            jax.ShapeDtypeStruct((fl, dm), F32),
            jax.ShapeDtypeStruct((parts, dp), BF16),
            jax.ShapeDtypeStruct((parts, LANES), F32),
            jax.ShapeDtypeStruct((1, LANES), jnp.int32),
            jax.ShapeDtypeStruct((1, 1), F32),
        ),
        in_specs=[hbm] * 6,
        out_specs=(hbm,) * 7,
        scratch_shapes=[
            pltpu.VMEM((PAIR, nz, fl, dp), BF16),
            pltpu.VMEM((PAIR, PAIR, dm, tl), BF16),
            tokens,
            pltpu.VMEM((PAIR, PAIR, nz * fl, tl), BF16),
            pltpu.VMEM((PAIR, PAIR, fl, dp), F32),
            pltpu.VMEM((PAIR, hops, fl, dp), F32),
            pltpu.VMEM((dp, tl), F32),
            pltpu.VMEM((dp, tl), F32),
            pltpu.VMEM((dm, tl), F32),
            pltpu.VMEM((dm, tl), F32),
            tokens,
            pltpu.VMEM((nz, MULTI, dp), F32),
            pltpu.VMEM((nz, MULTI, dp), F32),
            pltpu.VMEM((nz, CAP - MULTI, dp), BF16),
            pltpu.VMEM((nz, CAP - MULTI, dp), BF16),
            pltpu.VMEM((nz, CAP, dp), BF16),
            pltpu.VMEM((nz, CAP, dp), BF16),
            pltpu.VMEM((PAIR, PAIR, slots, tl), BF16),
            pltpu.VMEM((tp, tp), BF16),
            pltpu.VMEM((PAIR, 1, tl), jnp.int32),
            pltpu.VMEM((2 * slots, LANES), F32),
            pltpu.VMEM((slots, LANES), F32),
            pltpu.VMEM((8, slots), F32),
            pltpu.VMEM((nz, 8, LANES), F32),
            pltpu.VMEM((nz, 8, LANES), F32),
            pltpu.VMEM((vocab // 512, dm, 512), BF16),
            pltpu.VMEM((dp, slots // 2), F32),
            pltpu.VMEM((dm, tl), BF16),
            pltpu.VMEM((parts, dm), BF16),
            pltpu.VMEM((1, dp), F32),
            pltpu.VMEM((dp, LANES), F32),
            pltpu.VMEM((PAIR, fl, dm), BF16),
            pltpu.VMEM((dm,), BF16),
            pltpu.VMEM((1, 1), F32),
            pltpu.VMEM((parts, LANES), F32),
            pltpu.VMEM((1, LANES), jnp.int32),
            pltpu.VMEM((PAIR, fl, dm), F32),
            pltpu.VMEM((nz, CAP, dp), BF16),
            dma((PAIR,)), dma((PAIR,)),
            dma((5,)), dma((vocab // 512,)), dma((PAIR, PAIR)), dma((PAIR, hops)),
            dma((PAIR,)), dma((nz // 2,)), dma((PAIR,)), dma((3,)),
            dma((5,)), dma((5,)), dma((PAIR,)), dma((nz,)), dma((nz,)),
            dma((PAIR, PAIR)), dma((PAIR, hops)), dma((PAIR,)), dma((PAIR,)), dma((9,)),
        ],
        compiler_params=pltpu.CompilerParams(
            collective_id=0, has_side_effects=True, vmem_limit_bytes=VMEM_LIMIT
        ),
    )(ids, emb_t, up, down, grad_t, gain)


def place_kernel(
    bounds_ref, names_hbm, rows_hbm, out_ref, up_ref, down_ref, emb_out, out_out, up_out, down_out,
    names_v, rows_v, emb_v, out_v, up_v, down_v, in_sem, emb_sem, out_sem,
):
    def load(i, src, dst):
        copy = pltpu.make_async_copy(src, dst, in_sem.at[i])
        copy.start()
        return copy

    parts = names_hbm.shape[0]
    real = pl.ds(0, parts)
    needed = [load(0, names_hbm, names_v.at[real]), load(1, rows_hbm, rows_v.at[real])]
    passing = ((out_ref, out_v, out_out), (up_ref, up_v, up_out), (down_ref, down_v, down_out))
    loads = [load(2 + j, src, via) for j, (src, via, _) in enumerate(passing)]
    dm, vocab = emb_v.shape
    block = vocab // PLACE_GRID
    names_v[parts:] = jnp.full((PLACE_ROWS, LANES), -1.0)
    rows_v[parts:] = jnp.zeros((PLACE_ROWS, rows_v.shape[1]), BF16)
    for copy in needed:
        copy.wait()

    def store(i):
        at = pl.ds(pl.multiple_of(i * block, LANES), block)
        return pltpu.make_async_copy(emb_v.at[:, at], emb_out.at[:, at], emb_sem.at[i])

    def fill(i, carry):
        to = pl.ds(pl.multiple_of(i * block, LANES), block)
        lo = bounds_ref[0, i] // BLOCK * BLOCK

        def part(q):
            at = pl.ds(pl.multiple_of(lo + q * PLACE_ROWS, BLOCK), PLACE_ROWS)
            return first_first(rows_v[at, :dm], one_hot(names_v[at, :1] == across(block, i * block).astype(F32)))

        emb_v[:, to] = part(0)

        def more(q, inner):
            emb_v[:, to] = emb_v[:, to] + part(q)
            return inner

        lax.fori_loop(1, (bounds_ref[0, i + 1] - lo + PLACE_ROWS - 1) // PLACE_ROWS, more, 0)
        store(i).start()
        return carry

    lax.fori_loop(0, PLACE_GRID, fill, 0)
    keeps = []
    for j, (_, via, dst) in enumerate(passing):
        loads[j].wait()
        keeps.append(pltpu.make_async_copy(via, dst, out_sem.at[j]))
        keeps[-1].start()
    for i in range(PLACE_GRID):
        store(i).wait()
    for copy in keeps:
        copy.wait()


def place(vocab, bounds, names, rows, out, d_up, d_down):
    hbm = pl.BlockSpec(memory_space=pl.ANY)
    emb = jax.ShapeDtypeStruct((out.shape[0], vocab), F32)
    results = (emb,) + tuple(jax.ShapeDtypeStruct(a.shape, a.dtype) for a in (out, d_up, d_down))
    dma = pltpu.SemaphoreType.DMA
    return pl.pallas_call(
        place_kernel,
        name='place',
        out_shape=results,
        in_specs=[pl.BlockSpec(memory_space=pltpu.SMEM)] + [hbm] * 5,
        out_specs=(hbm,) * 4,
        scratch_shapes=[pltpu.VMEM((a.shape[0] + PLACE_ROWS, a.shape[1]), a.dtype) for a in (names, rows)]
        + [pltpu.VMEM(a.shape, a.dtype) for a in results]
        + [dma((5,)), dma((PLACE_GRID,)), dma((3,))],
        compiler_params=pltpu.CompilerParams(vmem_limit_bytes=VMEM_LIMIT),
    )(bounds, names, rows, out, d_up, d_down)


def swap_kernel(n, src_ref, dst_ref, keep_sem, send_sem, recv_sem):
    me = lax.axis_index('tensor')
    sem = pltpu.get_barrier_semaphore()
    for d in range(1, n):
        pl.semaphore_signal(sem, device_id={'tensor': lax.rem(me + d, n)}, device_id_type=MESH)
    pl.semaphore_wait(sem, n - 1)
    keep = pltpu.make_async_copy(src_ref.at[me], dst_ref.at[me], keep_sem)
    keep.start()
    copies = []
    for d in range(1, n):
        to = lax.rem(me + d, n)
        copies.append(remote(src_ref.at[to], dst_ref.at[me], send_sem.at[d], recv_sem.at[d], {'tensor': to}))
        copies[-1].start()
    for copy in copies:
        copy.wait()
    keep.wait()


def swap_blocks(n, blocks, collective_id):
    hbm = pl.BlockSpec(memory_space=pl.ANY)
    return pl.pallas_call(
        functools.partial(swap_kernel, n),
        name='swap_blocks',
        out_shape=jax.ShapeDtypeStruct(blocks.shape, blocks.dtype),
        in_specs=[hbm],
        out_specs=hbm,
        scratch_shapes=[pltpu.SemaphoreType.DMA, pltpu.SemaphoreType.DMA((n,)), pltpu.SemaphoreType.DMA((n,))],
        compiler_params=pltpu.CompilerParams(collective_id=collective_id, has_side_effects=True),
    )(blocks)


def all_blocks(n, block, collective_id):
    return swap_blocks(n, jnp.broadcast_to(block[None], (n,) + block.shape), collective_id)


def rms_norm(x_rows, gain_f):
    inv_rms = lax.rsqrt(jnp.mean(x_rows * x_rows, axis=-1, keepdims=True) + EPS)
    return x_rows * inv_rms * gain_f


def dense_step(n, ids, emb, norm_gain, up, down, grad_out):
    vocab, dm = emb.shape
    fl = up.shape[0]
    base = (lax.axis_index('tensor') * vocab).astype(F32)
    ids_all = all_blocks(n, jnp.broadcast_to(ids.astype(F32), (8, ids.shape[1])), 1)[:, 0]
    hot = (iota((ids_all.size, vocab), 1).astype(F32) == ids_all.reshape(-1, 1) - base).astype(BF16)
    part = jnp.dot(hot, emb, preferred_element_type=F32).astype(BF16)
    x_f = jnp.sum(swap_blocks(n, part.reshape(n, -1, dm), 2).astype(F32), axis=0)
    ws = all_blocks(n, jnp.stack([up, down]), 3)
    up_all, down_all = ws[:, 0].reshape(-1, dm), ws[:, 1].reshape(-1, dm)
    normed_f, norm_back = jax.vjp(lambda x_in: rms_norm(x_in, norm_gain.astype(F32)), x_f)
    normed = normed_f.astype(BF16)
    pre_act = last_last(normed, up_all).astype(BF16).astype(F32)
    act_f, slope = gelu_pair(pre_act)
    hidden = act_f.astype(BF16)
    d_pre = (last_last(grad_out, down_all) * slope).astype(BF16)
    y = jnp.dot(hidden, down_all, preferred_element_type=F32)
    out = (x_f + y).astype(BF16)
    d_norm = jnp.dot(d_pre, up_all, preferred_element_type=F32)
    dx = (grad_out.astype(F32) + norm_back(d_norm)[0]).astype(BF16)
    d_w = jnp.stack([first_first(d_pre, normed), first_first(hidden, grad_out)]).reshape(PAIR, n, fl, dm)
    d_w = jnp.sum(swap_blocks(n, jnp.moveaxis(d_w, 1, 0), 4), axis=0)
    dx_all = all_blocks(n, dx, 5).reshape(-1, dm)
    hot_t = (iota((vocab, ids_all.size), 0).astype(F32) == ids_all.reshape(1, -1) - base).astype(BF16)
    d_emb = jnp.dot(hot_t, dx_all, preferred_element_type=F32)
    return d_emb.T, out.T, d_w[0], d_w[1]


def solution(mesh):
    n, groups = mesh.shape['tensor'], mesh.shape['data']
    tok_spec = P(('data', 'tensor'))
    row_spec = P(('data', 'tensor'), None)

    def local_step(token_ids, emb_shard, norm_gain, w_up, w_down, grad_out):
        vocab, dm = emb_shard.shape
        ids, gain, up = token_ids[None, :], norm_gain, w_up.T
        out, d_up, d_down, rows, names, bounds, flag = step(n, groups, ids, emb_shard.T, up, w_down, grad_out.T, gain)
        placed = place(vocab, bounds, names, rows, out, d_up, d_down)

        def again(state):
            return (jnp.zeros((), F32),) + dense_step(n, ids, emb_shard, norm_gain, up, w_down, grad_out)

        state = lax.while_loop(lambda state: state[0] > 0.5, again, (flag[0, 0],) + tuple(placed))
        _, d_emb, out, d_up, d_down = state
        return out.T, d_emb.T, d_up.T, d_down

    return jax.shard_map(
        local_step,
        mesh=mesh,
        in_specs=(tok_spec, P('tensor', None), P(None), P(None, 'tensor'), P('tensor', None), row_spec),
        out_specs=(row_spec, row_spec, P('data', 'tensor'), row_spec),
        check_vma=False,
    )
```

```python
import functools
import math

import jax
import jax.numpy as jnp
from jax import lax
from jax.experimental import pallas as pl
from jax.experimental.pallas import tpu as pltpu
from jax.sharding import PartitionSpec as P

EPS = 1e-6
CAP = 64
MULTI = 16
PAIR = 2
BHEAD = 32
PLACE_GRID = 6
PLACE_ROWS = 256
LANES = 128
MESH = pl.DeviceIdType.MESH
VMEM_LIMIT = 67_000_000
F32 = jnp.float32
BF16 = jnp.bfloat16
SQRT_2_PI = 0.7978845608028654
CUBIC = 0.044715


def contract(left_op, right_op, left_dim, right_dim):
    dims = (((left_dim,), (right_dim,)), ((), ()))
    return lax.dot_general(left_op, right_op, dims, preferred_element_type=F32)


def first_first(left_op, right_op):
    return contract(left_op, right_op, 0, 0)


def last_last(left_op, right_op):
    return contract(left_op, right_op, 1, 1)


def iota(shape, dim):
    return lax.broadcasted_iota(jnp.int32, shape, dim)


def down(rows, start=0):
    return iota((rows, 1), 0) + start


def across(lanes, start=0):
    return iota((1, lanes), 1) + start


def flags(mask):
    return jnp.where(mask, 1.0, 0.0)


def one_hot(mask):
    return flags(mask).astype(BF16)


def over_rows(reduce, value):
    return reduce(value, axis=0, keepdims=True)


def over_lanes(reduce, value):
    return reduce(value, axis=1, keepdims=True)


def earlier_than(rows, lanes, start):
    return down(rows, start) < across(lanes)


def gelu_pair(u):
    t = jnp.tanh(SQRT_2_PI * (u + CUBIC * (u * u * u)))
    cdf = 0.5 * (1.0 + t)
    slope = cdf + u * (0.5 * (1.0 - t * t)) * (SQRT_2_PI * (1.0 + (3.0 * CUBIC) * (u * u)))
    return u * cdf, slope


def rows_at(i):
    return slice(i * LANES, (i + 1) * LANES)


class Ring:
    def __init__(self, n, groups):
        self.n, self.nz, self.half, self.groups = n, n // 2, n // 4, groups
        self.me = lax.axis_index('tensor')
        self.g = lax.axis_index('data')
        self.c = lax.rem(self.me, 2)
        self.z = self.me // 2

    def chip(self, k):
        return lax.rem(self.z + (k + self.nz) % self.nz, self.nz)

    def dev(self, k):
        return {'tensor': 2 * self.chip(k) + self.c}

    def twin(self, e):
        return {'data': lax.rem(self.g + e, self.groups), 'tensor': self.me}

    @property
    def sibling(self):
        return {'tensor': self.me + 1 - 2 * self.c}

    def greet(self):
        sem = pltpu.get_barrier_semaphore()
        for k in range(1, self.nz):
            pl.semaphore_signal(sem, device_id=self.dev(k), device_id_type=MESH)
        pl.semaphore_signal(sem, device_id=self.sibling, device_id_type=MESH)
        for e in range(1, self.groups):
            pl.semaphore_signal(sem, device_id=self.twin(e), device_id_type=MESH)

    def meet(self):
        pl.semaphore_wait(pltpu.get_barrier_semaphore(), self.nz + self.groups - 1)


def slot_of(nz):
    half = nz // 2
    order = [half] + [s * k for k in range(half - 1, 0, -1) for s in (1, -1)] + [0]
    table = {k: i for i, k in enumerate(order)}
    table[-half] = table[half]
    return table


def gather_messages(half):
    right = [(w, k) for k in range(half) for w in (0, 1) if w == 0 or k < half - 1]
    return right, [(1 - w, k) for w, k in right]


BLOCK = 16


def shared_blocks(fl, groups):
    shared = fl - 2 * BLOCK
    count = 2 if groups * BLOCK <= shared else 1
    height = 2 * shared // (groups * count)
    assert height % BLOCK == 0 and height * groups * count == 2 * shared
    return count, height, shared


def far_first(nz):
    half = nz // 2
    far = [half] + [half + s * k for k in range(1, half) for s in (-1, 1)]
    return far[:half - 1] + [0] + far[half - 1:]


def scatter_messages(half):
    right = [(0, half)]
    for k in range(half - 1, 0, -1):
        right += [(1, k), (0, k)]
    return right, [(1 - w, -k) for w, k in right]


def remote(src, dst, send_sem, recv_sem, device):
    return pltpu.make_async_remote_copy(
        src_ref=src, dst_ref=dst, send_sem=send_sem, recv_sem=recv_sem, device_id=device, device_id_type=MESH
    )


class Fold:
    def __init__(self, dm):
        self.dm = dm
        self.lo = dm // LANES * LANES
        self.dp = self.lo + LANES
        assert 2 * (dm - self.lo) == LANES

    def tail(self, value, h):
        low = value.shape[0] - h
        return jnp.concatenate([value[:low, self.lo:self.dm], value[h:, self.lo:self.dm]], axis=1)

    def store(self, ref, value, h):
        low = value.shape[0] - h
        ref[:, :self.lo] = value[:, :self.lo]
        ref[:low, self.lo:] = self.tail(value, h)
        if low < h:
            ref[low:h, self.lo:self.dm] = value[low:h, self.lo:self.dm]

    def add(self, ref, value, h):
        low = value.shape[0] - h
        ref[:, :self.lo] = ref[:, :self.lo] + value[:, :self.lo]
        ref[:low, self.lo:] = ref[:low, self.lo:] + self.tail(value, h)

    def unfold(self, ref, h):
        low = ref.shape[0] - h
        ref[h:, self.lo:self.dm] = ref[:low, self.dm:self.dp]

    def parts(self, src, dst, h, device):
        low = src.shape[0] - h
        areas = ((pl.ds(0, h), pl.ds(0, self.dp)), (pl.ds(h, low), pl.ds(0, self.lo)))
        return [(src.at[area], dst.at[area], device) for area in areas]

    def send(self, src, dst, h, send_sem, recv_sem, device):
        return Batch(self.parts(src, dst, h, device), self.spare, send_sem, recv_sem)


class Batch:
    def __init__(self, parts, spare, send_sem, recv_sem):
        self.copies = [remote(src, dst, send_sem, recv_sem, device) for src, dst, device in parts]
        dtype = jnp.dtype(parts[0][0].dtype)
        size = sum(math.prod(src.shape) for src, _, _ in parts)
        ref = spare[dtype]
        tile = 8 * 4 // dtype.itemsize
        width = next(w for w in range(LANES, ref.shape[1] + 1, LANES)
                     if size % (w * tile) == 0 and size // w <= ref.shape[0])
        whole = ref.at[pl.ds(0, size // width), pl.ds(0, width)]
        self.whole = remote(whole, whole, send_sem, recv_sem, parts[0][2])

    def start(self):
        for copy in self.copies:
            copy.start()

    def wait_recv(self):
        self.whole.wait_recv()

    def wait_send(self):
        self.whole.wait_send()


def step_kernel(
    n, groups, ids_ref, emb_ref, up_ref, down_ref, grad_ref, gain_ref,
    out_ref, dup_ref, ddown_ref, rows_ref, names_ref, bounds_ref, flag_ref,
    w_v, gn_v, x_v, hd_v, st_v, rb_v, snd_v, own_v, dnr_v, yr_v, dx_v, es_v, er_v, eb_v, eq_v, xs_v, xr_v,
    pick_v, tri_v, ids_v, col_v, name_v, nrow_v, req_s, req_r, emb_v, found_v, out_v, rows_v, row_v, gain_v,
    own_w, line_v, flag_v, names_v, bounds_v, dw_v, xo_v, xf_sem, xg_sem,
    ld_sem, emb_sem, ws_sem, wr_sem, bs_sem, br_sem, ts_sem, tr_sem, ps_sem, pr_sem, qs_sem, gs_sem, xr_sem,
    ss_sem, sr_sem, es_sem, er_sem, out_sem,
):
    ring = Ring(n, groups)
    nz, half, c, z = ring.nz, ring.half, ring.c, ring.z
    slot = slot_of(nz)
    dm, vocab = emb_ref.shape
    fl = up_ref.shape[0]
    each, height, shared = shared_blocks(fl, groups)
    order = far_first(nz)
    back = [order.index((nz - d) % nz) for d in order]
    own = order.index(0)
    others = [(p, d) for p, d in enumerate(order) if d]
    part_of = nz // 2
    tl = ids_ref.shape[1]
    tp = 2 * tl
    slots = nz * CAP
    fold = Fold(dm)
    fold.spare = {jnp.dtype(BF16): tri_v, jnp.dtype(F32): own_v}
    wh, xh, eh, bh = fl // 2, CAP // 2, MULTI // 2, BHEAD
    gh = (fl - shared) // 2
    ring_rows = pl.ds(shared, fl - shared)
    step = emb_v.shape[2]
    sides = ((0, 1), (1, -1))
    sent = []

    ring.greet()
    own_ids = pltpu.make_async_copy(ids_ref, ids_v.at[c], ld_sem.at[1])
    load_w = [pltpu.make_async_copy(ref, own_w.at[w], ld_sem.at[2 + w]) for w, ref in enumerate((up_ref, down_ref))]
    load_gain = pltpu.make_async_copy(gain_ref, line_v, ld_sem.at[4])
    load_grad = pltpu.make_async_copy(grad_ref, gn_v.at[1, c], ld_sem.at[0])
    for copy in [own_ids, load_gain] + load_w + [load_grad]:
        copy.start()

    def load_emb(i):
        at = pl.ds(pl.multiple_of(i * step, step), step)
        return pltpu.make_async_copy(emb_ref.at[:, at], emb_v.at[i], emb_sem.at[i])

    for i in range(vocab // step):
        load_emb(i).start()
    mine = slot[0]
    for w in range(PAIR):
        load_w[w].wait()
        w_v[w, mine, :, :dm] = own_w[w]
        w_v[w, mine, shared:shared + gh, dm:] = own_w[w, shared + gh:, fold.lo:]
    own_ids.wait()
    with jax.named_scope('barrier'):
        ring.meet()

    def start(copy, after=None):
        if after is not None:
            after.wait_send()
            sent[:] = [other for other in sent if other is not after]
        copy.start()
        sent.append(copy)
        return copy

    blocks = []
    for j in range(each):
        b = ring.g * each + j
        blocks.append((lax.rem(b, PAIR), pl.ds(pl.multiple_of(height * (b // 2), BLOCK), height)))

    def hops(k):
        parts = [
            (w_v.at[w, slot[-k * sign], at], w_v.at[w, slot[-(k + 1) * sign], at], ring.dev(sign))
            for j, (w, at) in enumerate(blocks) for side, sign in sides if k < half - 1 or side == j % 2
        ]
        return Batch(parts, fold.spare, bs_sem.at[k % 2], br_sem.at[k])

    stages = ((nz - 3, nz - 1), (nz - 5, nz - 3), (0, nz - 5))

    def twins(stage):
        lo, hi = stages[stage]
        refs = [w_v.at[w, pl.ds(lo, hi - lo), at] for w, at in blocks]
        parts = [(ref, ref, ring.twin(e)) for ref in refs for e in range(1, groups)]
        return Batch(parts, fold.spare, ts_sem.at[stage % 2], tr_sem.at[stage])

    block_moves = [hops(k) for k in range(half)]
    twin_moves = [twins(stage) for stage in range(len(stages))]

    def relay(k, stage):
        with jax.named_scope(f'relay{k}'):
            block_moves[k].wait_recv()
            if k + 1 < half:
                start(block_moves[k + 1], block_moves[k - 1] if k >= 1 else None)
            if stage is not None:
                start(twin_moves[stage], twin_moves[stage - 2] if stage >= 2 else None)

    def from_twins(stage):
        with jax.named_scope(f'twins{stage}'):
            twin_moves[stage].wait_recv()

    start(block_moves[0])
    swap_ids = start(remote(ids_v.at[c], ids_v.at[c], ps_sem.at[0], pr_sem.at[0], ring.sibling))
    moves = [[], []]
    for side, sign in sides:
        for i, (w, k) in enumerate(gather_messages(half)[side]):
            src, dst = w_v.at[w, slot[-k * sign], ring_rows], w_v.at[w, slot[-(k + 1) * sign], ring_rows]
            moves[side].append(fold.send(src, dst, gh, ws_sem.at[side, i % 2], wr_sem.at[side, i], ring.dev(sign)))

    def forward(i):
        with jax.named_scope(f'fwd{i}'):
            for side, sign in sides:
                moves[side][i].wait_recv()
                if i + 2 < len(moves[side]):
                    start(moves[side][i + 2], moves[side][i])
                w, k = gather_messages(half)[side][i]
                fold.unfold(w_v.at[w, slot[-(k + 1) * sign], ring_rows], gh)

    with jax.named_scope('ids_wait'):
        swap_ids.wait_recv()
    ids = jnp.concatenate([ids_v[0], ids_v[1]], axis=1).astype(F32)
    ids_t = jnp.transpose(jnp.broadcast_to(ids, (LANES, tp)))
    seen = jnp.zeros((1, tp), F32)
    total = jnp.zeros((1, tp), F32)
    for i in range(tp // LANES):
        tri = flags(earlier_than(LANES, tp, i * LANES))
        same = flags(ids_t[rows_at(i), :1] == ids)
        seen = jnp.maximum(seen, over_rows(jnp.max, same * tri))
        total = total + over_rows(jnp.sum, same)
    row = down(n)
    place = lax.rem(row, nz)
    chip = lax.rem(z + sum(jnp.where(place == p, d, 0) for p, d in others), nz)
    owner = 2 * chip + jnp.where(row < nz, c, 1 - c)
    base = (owner * vocab).astype(F32)
    member = flags((seen < 0.5) & (ids >= base) & (ids < base + vocab))
    multi = flags(total > 1.5)
    several, single = member * multi, member * (1.0 - multi)
    both = jnp.concatenate([several, single], axis=0)
    tri = one_hot(earlier_than(LANES, LANES, 0))
    before = jnp.zeros((2 * n, 1), F32)
    ranks = []
    for i in range(tp // LANES):
        some = both[:, rows_at(i)]
        ranks.append(before + jnp.dot(some.astype(BF16), tri, preferred_element_type=F32))
        before = before + over_lanes(jnp.sum, some)
    rank = jnp.concatenate(ranks, axis=1)
    n_several, count = before[:n], before[:n] + before[n:]
    rank = jnp.where(several > 0.5, rank[:n], n_several + rank[n:])
    over = over_rows(jnp.max, flags((count > CAP) | (n_several > MULTI)))
    for k in range(n):
        hit = (rank[k:k + 1, :] == down(CAP).astype(F32)) & (member[k:k + 1, :] > 0.5)
        col = over_lanes(jnp.max, jnp.where(hit, ids, -1.0))
        col_v[k * CAP:(k + 1) * CAP, :] = jnp.broadcast_to(col, (CAP, LANES))
    cols_t = jnp.transpose(col_v[:slots, :])
    lane = iota((8, LANES), 1)
    per = LANES // CAP
    for k in range(nz):
        at = (k // per) * LANES
        tile = cols_t[0:8, at:at + LANES]
        if k % per:
            tile = pltpu.roll(tile, LANES - (k % per) * CAP, 1)
        req_s[k] = jnp.where(lane < CAP, tile, over)
    parts = [(req_s.at[p], req_r.at[back[p]], ring.dev(d)) for p, d in others]
    asks = start(Batch(parts, fold.spare, qs_sem.at[0], qs_sem.at[1]))
    relay(0, 0)
    for i in range(PAIR):
        for side, _ in sides:
            start(moves[side][i])
    swap_grad = start(remote(grad_ref, gn_v.at[1, c], ps_sem.at[1], pr_sem.at[1], ring.sibling))
    req_r[own] = req_s[own]
    for q in range(PAIR):
        for t in range(PAIR):
            pick_v[q, t] = one_hot(col_v[q * slots:(q + 1) * slots, :1] == ids[:, t * tl:(t + 1) * tl])

    with jax.named_scope('asks_wait'):
        asks.wait_recv()
    flag = req_r[0]
    for k in range(1, nz):
        flag = jnp.maximum(flag, req_r[k])
    flag_v[...] = over_rows(jnp.max, over_lanes(jnp.max, jnp.where(lane < CAP, 0.0, flag)))
    keeps = [pltpu.make_async_copy(flag_v, flag_ref, out_sem.at[2])]
    keeps[0].start()
    tiles = []
    for p in range(nz // per):
        tile = req_r[p * per]
        for j in range(1, per):
            tile = jnp.where(lane < j * CAP, tile, pltpu.roll(req_r[p * per + j], j * CAP, 1))
        tiles.append(tile)
    names = jnp.concatenate(tiles, axis=1) - (ring.me * vocab).astype(F32)
    nrow_v[...] = names
    name_v[...] = jnp.transpose(jnp.broadcast_to(names[0:1, :], (LANES, slots)))
    gives = {}
    handed = []

    def find(part):
        cols = slice(part * slots // 2, (part + 1) * slots // 2)
        found_v[...] = jnp.zeros_like(found_v)

        def body(i, carry):
            if part == 0:
                load_emb(i).wait()
            hot = one_hot(down(step, i * step).astype(F32) == nrow_v[:1, cols])
            found_v[:dm, :] = found_v[:dm, :] + jnp.dot(emb_v[i], hot, preferred_element_type=F32)
            return carry

        with jax.named_scope(f'find{part}'):
            lax.fori_loop(0, vocab // step, body, 0)
        found = jnp.transpose(found_v[...])[:, :dm].astype(BF16)
        for q in range(nz // 2):
            fold.store(xs_v.at[part * nz // 2 + q], found[q * CAP:(q + 1) * CAP, :], xh)

    def give(part):
        at = range(part * part_of, (part + 1) * part_of)
        parts = [area for p in at for area in fold.parts(xr_v.at[p], xo_v.at[p], xh, ring.sibling)]
        handed.append(Batch(parts, fold.spare, xf_sem.at[part], xg_sem.at[part]))
        sent.append(handed[part])
        for p in at:
            if order[p]:
                to = ring.dev(order[p])
                gives[p] = start(fold.send(xs_v.at[p], xr_v.at[back[p]], xh, gs_sem.at[p], xr_sem.at[p], to))
            else:
                xr_v[p] = xs_v[p]
                hand(p)

    def hand(p):
        for copy in handed[p // part_of].copies[2 * (p % part_of):2 * (p % part_of) + 2]:
            copy.start()

    relay(1, 1)
    find(0)
    relay(2, None)
    forward(0)
    give(0)
    find(1)
    forward(1)
    give(1)
    row_v[...] = jnp.zeros_like(row_v)
    load_gain.wait()
    row_v[:, :dm] = line_v[...].astype(F32).reshape(1, dm)
    gain_v[...] = jnp.transpose(jnp.broadcast_to(row_v[...], (LANES, fold.dp)))
    relay(3, 2)
    forward(2)

    def arrived(part):
        with jax.named_scope(f'gives_wait{part}'):
            for p in range(part * part_of, (part + 1) * part_of):
                if order[p]:
                    gives[p].wait_recv()
                    hand(back[p])

    def unpack(rows_of, q, part):
        at = slice(part * part_of, (part + 1) * part_of)
        for p in range(part * part_of, (part + 1) * part_of):
            fold.unfold(rows_of.at[p], xh)
        rows = rows_of[at].reshape(part_of * CAP, fold.dp)[:, :dm]
        picks = slice(part * part_of * CAP, (part + 1) * part_of * CAP)
        for t in range(PAIR):
            value = first_first(rows, pick_v[q, t, picks]).astype(BF16)
            x_v[t] = x_v[t] + value if q or part else value

    def from_sibling(part):
        with jax.named_scope(f'sibling_wait{part}'):
            handed[part].wait_recv()
        unpack(xo_v, 1, part)

    arrived(0)
    unpack(xr_v, 0, 0)
    from_sibling(0)
    arrived(1)
    forward(3)
    unpack(xr_v, 0, 1)
    forward(4)
    load_grad.wait()
    swap_grad.wait_recv()
    from_sibling(1)

    def lanes(b):
        return pl.ds(pl.multiple_of(b * LANES, LANES), LANES)

    def norm(i, carry):
        t, at = i // (tl // LANES), lanes(lax.rem(i, tl // LANES))
        xf = x_v[t, :, at].astype(F32)
        inv = lax.rsqrt(over_rows(jnp.mean, xf * xf) + EPS)
        gn_v[0, t, :, at] = (xf * inv * gain_v[:dm, :]).astype(BF16)
        return carry

    lax.fori_loop(0, tp // LANES, norm, 0)

    def hidden(lo, hi):
        def body(i, carry):
            s, t = lo + i // 2, lax.rem(i, PAIR)
            u = jnp.dot(w_v[0, s, :, :dm], gn_v[0, t], preferred_element_type=F32).astype(BF16).astype(F32)
            dh = jnp.dot(w_v[1, s, :, :dm], gn_v[1, t], preferred_element_type=F32)
            act, slope = gelu_pair(u)
            at = pl.ds(pl.multiple_of(s * fl, fl), fl)
            hd_v[1, t, at, :] = act.astype(BF16)
            hd_v[0, t, at, :] = (dh * slope).astype(BF16)
            return carry

        with jax.named_scope(f'hid{lo}'):
            lax.fori_loop(0, 2 * (hi - lo), body, 0)

    def grad_w(w, s):
        at = pl.ds(pl.multiple_of(s * fl, fl), fl)
        return last_last(hd_v[w, 0, at, :], gn_v[w, 0]) + last_last(hd_v[w, 1, at, :], gn_v[w, 1])

    orders = scatter_messages(half)
    sends = [[], []]
    for side, sign in sides:
        for i in range(len(orders[0])):
            src = st_v.at[side, i] if i < 2 else rb_v.at[side, i - 2]
            dst = rb_v.at[side, i]
            sends[side].append(fold.send(src, dst, wh, ss_sem.at[side, i % 2], sr_sem.at[side, i], ring.dev(sign)))

    def scatter(i):
        with jax.named_scope(f'scat{i}'):
            (w0, k0), (_, k1) = orders[0][i], orders[1][i]
            if i >= 2:
                for side, _ in sides:
                    sends[side][i - 2].wait_recv()

            def body(side, carry):
                w = w0 + side * (1 - 2 * w0)
                part = grad_w(w, slot[k0] + side * (slot[k1] - slot[k0]))
                if i < 2:
                    fold.store(st_v.at[side, i], part, wh)
                else:
                    fold.add(rb_v.at[side, i - 2], part, wh)
                return carry

            if i:
                lax.fori_loop(0, 2, body, 0)
            for side, _ in sides:
                if i == 0:
                    body(side, 0)
                start(sends[side][i], sends[side][i - 2] if i >= 2 else None)

    forward(5)
    forward(6)
    for stage in range(len(stages)):
        from_twins(stage)
    hidden(0, 1)
    scatter(0)
    hidden(1, nz - 5)
    scatter(1)
    hidden(nz - 5, nz)

    wide = 2 * LANES

    def through(w, t, dst):
        def body(b, carry):
            at = pl.ds(pl.multiple_of(b * wide, wide), wide)
            left = w_v[w, :, :, at].reshape(nz * fl, wide)
            dst[at, :] = first_first(left, hd_v[w_of_hd[w], t])
            return carry

        lax.fori_loop(0, fold.dp // wide, body, 0)

    w_of_hd = (0, 1)
    with jax.named_scope('thru'):
        through(0, 1 - c, snd_v)
    body_rows = pl.ds(0, dm)
    swap_dn = remote(snd_v.at[body_rows], dnr_v, ps_sem.at[2], pr_sem.at[2], ring.sibling)
    swap_dn.start()
    through(0, c, own_v)
    scatter(2)
    with jax.named_scope('swapdn_wait'):
        swap_dn.wait_send()
        swap_dn.wait_recv()

    def dx_block(b, carry):
        at = lanes(b)
        xf = x_v[c, :, at].astype(F32)
        inv = lax.rsqrt(over_rows(jnp.mean, xf * xf) + EPS)
        q = (own_v[:dm, at] + dnr_v[:, at]) * gain_v[:dm, :]
        dot = over_rows(jnp.mean, xf * q)
        dxn = inv * q - xf * (inv * inv * inv * dot)
        dx_v[c, :, at] = (gn_v[1, c, :, at].astype(F32) + dxn).astype(BF16)
        return carry

    lax.fori_loop(0, tl // LANES, dx_block, 0)
    swap_dx = start(remote(dx_v.at[c], dx_v.at[c], ps_sem.at[3], pr_sem.at[3], ring.sibling))
    through(1, 1 - c, snd_v)
    swap_y = start(remote(snd_v.at[body_rows], yr_v, ps_sem.at[4], pr_sem.at[4], ring.sibling))
    with jax.named_scope('swapdx_wait'):
        swap_dx.wait_recv()

    def pack(k, carry):
        at = pl.ds(pl.multiple_of(k * CAP, CAP), CAP)
        rows = last_last(pick_v[0, 0, at, :], dx_v[0]) + last_last(pick_v[0, 1, at, :], dx_v[1])
        fold.store(es_v.at[k], rows[:MULTI], eh)
        fold.store(eb_v.at[k], rows[MULTI:].astype(BF16), bh)
        return carry

    lax.fori_loop(0, nz, pack, 0)
    backs = []
    for kind, (src, dst, h) in enumerate(((es_v, er_v, eh), (eb_v, eq_v, bh))):
        parts = [area for p, d in others for area in fold.parts(src.at[p], dst.at[back[p]], h, ring.dev(d))]
        backs.append(start(Batch(parts, fold.spare, es_sem.at[kind], er_sem.at[kind])))
    er_v[own] = es_v[own]
    eq_v[own] = eb_v[own]
    through(1, c, own_v)
    scatter(3)
    with jax.named_scope('swapy_wait'):
        swap_y.wait_recv()

    def out_block(b, carry):
        at = lanes(b)
        out_v[:, at] = (x_v[c, :, at].astype(F32) + (own_v[:dm, at] + yr_v[:, at])).astype(BF16)
        return carry

    lax.fori_loop(0, tl // LANES, out_block, 0)
    keeps.append(pltpu.make_async_copy(out_v, out_ref, out_sem.at[0]))
    keeps[-1].start()
    last = len(orders[0])
    for i in range(4, last):
        scatter(i)

    with jax.named_scope('backs_wait'):
        for copy in backs:
            copy.wait_recv()
    lots, rest = nz * MULTI, CAP - MULTI

    def spread(k, carry):
        fold.unfold(er_v.at[k], eh)
        fold.unfold(eq_v.at[k], bh)
        rows = er_v[k, :, :dm]
        head = name_v[pl.ds(pl.multiple_of(k * CAP, CAP), MULTI), :]
        for p in range(3):
            at = pl.ds(pl.multiple_of(p * lots + k * MULTI, MULTI), MULTI)
            piece = rows.astype(BF16)
            rows_v[at, :] = piece
            names_v[at, :] = head
            rows = rows - piece.astype(F32)
        at = pl.ds(pl.multiple_of(3 * lots + k * rest, 16), rest)
        rows_v[at, :] = eq_v[k, :, :dm]
        names_v[at, :] = name_v[pl.ds(pl.multiple_of(k * CAP + MULTI, 16), rest), :]
        return carry

    lax.fori_loop(0, nz, spread, 0)

    parts = rows_v.shape[0]
    key = jnp.where(names_v[...] < 0.0, 2.0 * vocab, names_v[...])
    names_v[...] = key
    key = jnp.transpose(key)[0:1, :]
    rank_row = jnp.zeros((1, parts), F32)
    for i in range(parts // LANES):
        col = names_v[rows_at(i), :1]
        ahead = (col < key) | ((col == key) & earlier_than(LANES, parts, i * LANES))
        rank_row = rank_row + over_rows(jnp.sum, flags(ahead))
    for i in range(parts // LANES):
        hit = down(LANES, i * LANES).astype(F32) == rank_row
        tri_v[rows_at(i), :dm] = jnp.dot(one_hot(hit), rows_v[...], preferred_element_type=F32).astype(BF16)
        name = over_lanes(jnp.sum, jnp.where(hit, key, 0.0))
        names_v[rows_at(i), :] = jnp.broadcast_to(name, (LANES, LANES))
    which = across(LANES)
    bounds = jnp.zeros((1, LANES), F32)
    for b in range(PLACE_GRID + 1):
        before = over_lanes(jnp.sum, flags(key < b * (vocab // PLACE_GRID)))
        bounds = jnp.where(which == b, before, bounds)
    bounds_v[...] = bounds.astype(jnp.int32)
    for j, (src, dst) in enumerate(((tri_v.at[pl.ds(0, parts), pl.ds(0, fold.dp)], rows_ref), (names_v, names_ref), (bounds_v, bounds_ref))):
        keeps.append(pltpu.make_async_copy(src, dst, out_sem.at[3 + j]))
        keeps[-1].start()

    for w in range(PAIR):
        dw_v[w] = grad_w(w, mine)
    for w in range(PAIR):
        a, b = (last - 1, last - 2) if w == 0 else (last - 2, last - 1)
        with jax.named_scope(f'fin{w}'):
            sends[0][a].wait_recv()
            sends[1][b].wait_recv()
        rb_v[0, a] = rb_v[0, a] + rb_v[1, b]
        fold.unfold(rb_v.at[0, a], wh)
        dw_v[w] = rb_v[0, a, :, :dm] + dw_v[w]
        keeps.append(pltpu.make_async_copy(dw_v.at[w], (dup_ref, ddown_ref)[w], out_sem.at[6 + w]))
        keeps[-1].start()
    with jax.named_scope('exit_sends'):
        for copy in sent:
            copy.wait_send()
    with jax.named_scope('exit_keeps'):
        for copy in keeps:
            copy.wait()


def step(n, groups, ids, emb_t, up, down, grad_t, gain):
    nz = n // 2
    dm, vocab = emb_t.shape
    tl, fl = ids.shape[1], up.shape[0]
    tp = 2 * tl
    dp = Fold(dm).dp
    slots = nz * CAP
    parts = slots + 2 * nz * MULTI
    assert max(parts, dp) <= tp
    hops = nz - 1
    hbm = pl.BlockSpec(memory_space=pl.ANY)
    dma = pltpu.SemaphoreType.DMA
    tokens = pltpu.VMEM((PAIR, dm, tl), BF16)
    return pl.pallas_call(
        functools.partial(step_kernel, n, groups),
        name='step',
        out_shape=(
            jax.ShapeDtypeStruct((dm, tl), BF16),
            jax.ShapeDtypeStruct((fl, dm), F32),
            jax.ShapeDtypeStruct((fl, dm), F32),
            jax.ShapeDtypeStruct((parts, dp), BF16),
            jax.ShapeDtypeStruct((parts, LANES), F32),
            jax.ShapeDtypeStruct((1, LANES), jnp.int32),
            jax.ShapeDtypeStruct((1, 1), F32),
        ),
        in_specs=[hbm] * 6,
        out_specs=(hbm,) * 7,
        scratch_shapes=[
            pltpu.VMEM((PAIR, nz, fl, dp), BF16),
            pltpu.VMEM((PAIR, PAIR, dm, tl), BF16),
            tokens,
            pltpu.VMEM((PAIR, PAIR, nz * fl, tl), BF16),
            pltpu.VMEM((PAIR, PAIR, fl, dp), F32),
            pltpu.VMEM((PAIR, hops, fl, dp), F32),
            pltpu.VMEM((dp, tl), F32),
            pltpu.VMEM((dp, tl), F32),
            pltpu.VMEM((dm, tl), F32),
            pltpu.VMEM((dm, tl), F32),
            tokens,
            pltpu.VMEM((nz, MULTI, dp), F32),
            pltpu.VMEM((nz, MULTI, dp), F32),
            pltpu.VMEM((nz, CAP - MULTI, dp), BF16),
            pltpu.VMEM((nz, CAP - MULTI, dp), BF16),
            pltpu.VMEM((nz, CAP, dp), BF16),
            pltpu.VMEM((nz, CAP, dp), BF16),
            pltpu.VMEM((PAIR, PAIR, slots, tl), BF16),
            pltpu.VMEM((tp, tp), BF16),
            pltpu.VMEM((PAIR, 1, tl), jnp.int32),
            pltpu.VMEM((2 * slots, LANES), F32),
            pltpu.VMEM((slots, LANES), F32),
            pltpu.VMEM((8, slots), F32),
            pltpu.VMEM((nz, 8, LANES), F32),
            pltpu.VMEM((nz, 8, LANES), F32),
            pltpu.VMEM((vocab // 512, dm, 512), BF16),
            pltpu.VMEM((dp, slots // 2), F32),
            pltpu.VMEM((dm, tl), BF16),
            pltpu.VMEM((parts, dm), BF16),
            pltpu.VMEM((1, dp), F32),
            pltpu.VMEM((dp, LANES), F32),
            pltpu.VMEM((PAIR, fl, dm), BF16),
            pltpu.VMEM((dm,), BF16),
            pltpu.VMEM((1, 1), F32),
            pltpu.VMEM((parts, LANES), F32),
            pltpu.VMEM((1, LANES), jnp.int32),
            pltpu.VMEM((PAIR, fl, dm), F32),
            pltpu.VMEM((nz, CAP, dp), BF16),
            dma((PAIR,)), dma((PAIR,)),
            dma((5,)), dma((vocab // 512,)), dma((PAIR, PAIR)), dma((PAIR, hops)),
            dma((PAIR,)), dma((nz // 2,)), dma((PAIR,)), dma((3,)),
            dma((5,)), dma((5,)), dma((PAIR,)), dma((nz,)), dma((nz,)),
            dma((PAIR, PAIR)), dma((PAIR, hops)), dma((PAIR,)), dma((PAIR,)), dma((9,)),
        ],
        compiler_params=pltpu.CompilerParams(
            collective_id=0, has_side_effects=True, vmem_limit_bytes=VMEM_LIMIT
        ),
    )(ids, emb_t, up, down, grad_t, gain)


def place_kernel(
    bounds_ref, names_hbm, rows_hbm, out_ref, up_ref, down_ref, emb_out, out_out, up_out, down_out,
    names_v, rows_v, emb_v, out_v, up_v, down_v, in_sem, emb_sem, out_sem,
):
    def load(i, src, dst):
        copy = pltpu.make_async_copy(src, dst, in_sem.at[i])
        copy.start()
        return copy

    parts = names_hbm.shape[0]
    real = pl.ds(0, parts)
    needed = [load(0, names_hbm, names_v.at[real]), load(1, rows_hbm, rows_v.at[real])]
    passing = ((out_ref, out_v, out_out), (up_ref, up_v, up_out), (down_ref, down_v, down_out))
    loads = [load(2 + j, src, via) for j, (src, via, _) in enumerate(passing)]
    dm, vocab = emb_v.shape
    block = vocab // PLACE_GRID
    names_v[parts:] = jnp.full((PLACE_ROWS, LANES), -1.0)
    rows_v[parts:] = jnp.zeros((PLACE_ROWS, rows_v.shape[1]), BF16)
    for copy in needed:
        copy.wait()

    def store(i):
        at = pl.ds(pl.multiple_of(i * block, LANES), block)
        return pltpu.make_async_copy(emb_v.at[:, at], emb_out.at[:, at], emb_sem.at[i])

    def fill(i, carry):
        to = pl.ds(pl.multiple_of(i * block, LANES), block)
        lo = bounds_ref[0, i] // BLOCK * BLOCK

        def part(q):
            at = pl.ds(pl.multiple_of(lo + q * PLACE_ROWS, BLOCK), PLACE_ROWS)
            return first_first(rows_v[at, :dm], one_hot(names_v[at, :1] == across(block, i * block).astype(F32)))

        emb_v[:, to] = part(0)

        def more(q, inner):
            emb_v[:, to] = emb_v[:, to] + part(q)
            return inner

        lax.fori_loop(1, (bounds_ref[0, i + 1] - lo + PLACE_ROWS - 1) // PLACE_ROWS, more, 0)
        store(i).start()
        return carry

    lax.fori_loop(0, PLACE_GRID, fill, 0)
    keeps = []
    for j, (_, via, dst) in enumerate(passing):
        loads[j].wait()
        keeps.append(pltpu.make_async_copy(via, dst, out_sem.at[j]))
        keeps[-1].start()
    for i in range(PLACE_GRID):
        store(i).wait()
    for copy in keeps:
        copy.wait()


def place(vocab, bounds, names, rows, out, d_up, d_down):
    hbm = pl.BlockSpec(memory_space=pl.ANY)
    emb = jax.ShapeDtypeStruct((out.shape[0], vocab), F32)
    results = (emb,) + tuple(jax.ShapeDtypeStruct(a.shape, a.dtype) for a in (out, d_up, d_down))
    dma = pltpu.SemaphoreType.DMA
    return pl.pallas_call(
        place_kernel,
        name='place',
        out_shape=results,
        in_specs=[pl.BlockSpec(memory_space=pltpu.SMEM)] + [hbm] * 5,
        out_specs=(hbm,) * 4,
        scratch_shapes=[pltpu.VMEM((a.shape[0] + PLACE_ROWS, a.shape[1]), a.dtype) for a in (names, rows)]
        + [pltpu.VMEM(a.shape, a.dtype) for a in results]
        + [dma((5,)), dma((PLACE_GRID,)), dma((3,))],
        compiler_params=pltpu.CompilerParams(vmem_limit_bytes=VMEM_LIMIT),
    )(bounds, names, rows, out, d_up, d_down)


def swap_kernel(n, src_ref, dst_ref, keep_sem, send_sem, recv_sem):
    me = lax.axis_index('tensor')
    sem = pltpu.get_barrier_semaphore()
    for d in range(1, n):
        pl.semaphore_signal(sem, device_id={'tensor': lax.rem(me + d, n)}, device_id_type=MESH)
    pl.semaphore_wait(sem, n - 1)
    keep = pltpu.make_async_copy(src_ref.at[me], dst_ref.at[me], keep_sem)
    keep.start()
    copies = []
    for d in range(1, n):
        to = lax.rem(me + d, n)
        copies.append(remote(src_ref.at[to], dst_ref.at[me], send_sem.at[d], recv_sem.at[d], {'tensor': to}))
        copies[-1].start()
    for copy in copies:
        copy.wait()
    keep.wait()


def swap_blocks(n, blocks, collective_id):
    hbm = pl.BlockSpec(memory_space=pl.ANY)
    return pl.pallas_call(
        functools.partial(swap_kernel, n),
        name='swap_blocks',
        out_shape=jax.ShapeDtypeStruct(blocks.shape, blocks.dtype),
        in_specs=[hbm],
        out_specs=hbm,
        scratch_shapes=[pltpu.SemaphoreType.DMA, pltpu.SemaphoreType.DMA((n,)), pltpu.SemaphoreType.DMA((n,))],
        compiler_params=pltpu.CompilerParams(collective_id=collective_id, has_side_effects=True),
    )(blocks)


def all_blocks(n, block, collective_id):
    return swap_blocks(n, jnp.broadcast_to(block[None], (n,) + block.shape), collective_id)


def rms_norm(x_rows, gain_f):
    inv_rms = lax.rsqrt(jnp.mean(x_rows * x_rows, axis=-1, keepdims=True) + EPS)
    return x_rows * inv_rms * gain_f


def dense_step(n, ids, emb, norm_gain, up, down, grad_out):
    vocab, dm = emb.shape
    fl = up.shape[0]
    base = (lax.axis_index('tensor') * vocab).astype(F32)
    ids_all = all_blocks(n, jnp.broadcast_to(ids.astype(F32), (8, ids.shape[1])), 1)[:, 0]
    hot = (iota((ids_all.size, vocab), 1).astype(F32) == ids_all.reshape(-1, 1) - base).astype(BF16)
    part = jnp.dot(hot, emb, preferred_element_type=F32).astype(BF16)
    x_f = jnp.sum(swap_blocks(n, part.reshape(n, -1, dm), 2).astype(F32), axis=0)
    ws = all_blocks(n, jnp.stack([up, down]), 3)
    up_all, down_all = ws[:, 0].reshape(-1, dm), ws[:, 1].reshape(-1, dm)
    normed_f, norm_back = jax.vjp(lambda x_in: rms_norm(x_in, norm_gain.astype(F32)), x_f)
    normed = normed_f.astype(BF16)
    pre_act = last_last(normed, up_all).astype(BF16).astype(F32)
    act_f, slope = gelu_pair(pre_act)
    hidden = act_f.astype(BF16)
    d_pre = (last_last(grad_out, down_all) * slope).astype(BF16)
    y = jnp.dot(hidden, down_all, preferred_element_type=F32)
    out = (x_f + y).astype(BF16)
    d_norm = jnp.dot(d_pre, up_all, preferred_element_type=F32)
    dx = (grad_out.astype(F32) + norm_back(d_norm)[0]).astype(BF16)
    d_w = jnp.stack([first_first(d_pre, normed), first_first(hidden, grad_out)]).reshape(PAIR, n, fl, dm)
    d_w = jnp.sum(swap_blocks(n, jnp.moveaxis(d_w, 1, 0), 4), axis=0)
    dx_all = all_blocks(n, dx, 5).reshape(-1, dm)
    hot_t = (iota((vocab, ids_all.size), 0).astype(F32) == ids_all.reshape(1, -1) - base).astype(BF16)
    d_emb = jnp.dot(hot_t, dx_all, preferred_element_type=F32)
    return d_emb.T, out.T, d_w[0], d_w[1]


def solution(mesh):
    n, groups = mesh.shape['tensor'], mesh.shape['data']
    tok_spec = P(('data', 'tensor'))
    row_spec = P(('data', 'tensor'), None)

    def local_step(token_ids, emb_shard, norm_gain, w_up, w_down, grad_out):
        vocab, dm = emb_shard.shape
        ids, gain, up = token_ids[None, :], norm_gain, w_up.T
        out, d_up, d_down, rows, names, bounds, flag = step(n, groups, ids, emb_shard.T, up, w_down, grad_out.T, gain)
        placed = place(vocab, bounds, names, rows, out, d_up, d_down)

        def again(state):
            return (jnp.zeros((), F32),) + dense_step(n, ids, emb_shard, norm_gain, up, w_down, grad_out)

        state = lax.while_loop(lambda state: state[0] > 0.5, again, (flag[0, 0],) + tuple(placed))
        _, d_emb, out, d_up, d_down = state
        return out.T, d_emb.T, d_up.T, d_down

    return jax.shard_map(
        local_step,
        mesh=mesh,
        in_specs=(tok_spec, P('tensor', None), P(None), P(None, 'tensor'), P('tensor', None), row_spec),
        out_specs=(row_spec, row_spec, P('data', 'tensor'), row_spec),
        check_vma=False,
    )
```
